128 devices in a mesh: gx: 32 (over x, y, core), gy: 4 (over z).
Axes of the slice: x: 4, y: 4, z: 4, core: 2. Of those that a mesh axis runs over, the one named last changes fastest.
Arguments:
- layer_early: bfloat16 [4096, 8192], P(None, ('gx', 'gy')), may hold values from -48 to 48
- layer_late: bfloat16 [4096, 8192], P(('gx', 'gy')), may hold values from -48 to 48
Outputs:
- similarity: float32 [], replicated
- token_share: float32 [4096], P(('gx', 'gy'))
- early_rows: bfloat16 [4096, 8192], P(('gx', 'gy'))
- late_rows: bfloat16 [4096, 8192], P(('gx', 'gy'))
The draws below stay inside these ranges and needn't reach their ends.
All inputs are finite; a program needn't handle non-finite values.
Results may differ from the reference program's by a relative error of at most 0.0015.
Values may be sent and summed in bfloat16 or wider, within the bound.
A program may use at most 128 MiB of HBM per device.

```python
import math
import jax
import jax.numpy as jnp
from jax import lax

D = 8192
TOKENS = 4096


def draw_layer(key, salt):
    order = jax.random.permutation(jax.random.fold_in(key, 5), D)
    spectrum = 6.0 * jnp.power(order.astype(jnp.float32) + 1.0, -0.5)
    jitter = jnp.exp(jax.random.uniform(jax.random.fold_in(key, salt + 3), (D,), jnp.float32, minval=math.log(0.5), maxval=math.log(2.0)))
    column_scale = jnp.sqrt(spectrum * jitter)
    shared = jax.random.normal(jax.random.fold_in(key, 7), (TOKENS, D), jnp.float32)
    own_part = jax.random.normal(jax.random.fold_in(key, salt + 1), (TOKENS, D), jnp.float32)
    offsets = jax.random.uniform(jax.random.fold_in(key, salt + 2), (D,), jnp.float32, minval=-8.0, maxval=8.0)
    signal = (0.9 * shared + 0.436 * own_part) * column_scale
    return jnp.clip(signal + offsets, -48.0, 48.0)


def draw_layer_early(key, part):
    return draw_layer(key, 11).astype(jnp.bfloat16)


def draw_layer_late(key, part):
    return draw_layer(key, 23).astype(jnp.bfloat16)


def setup_inputs(seed: int = 0) -> dict:
    splits = jax.random.split(jax.random.key(seed), 3)
    layer_early = draw_layer_early(jax.random.fold_in(splits[2], 71), 0)
    layer_late = draw_layer_late(jax.random.fold_in(splits[2], 71), 0)
    return {"layer_early": layer_early, "layer_late": layer_late}


def reference(layer_early, layer_late):
    early_values = layer_early.astype(jnp.float32)
    late_values = layer_late.astype(jnp.float32)
    early_rows = (early_values - lax.optimization_barrier(jnp.mean(early_values, axis=0))).astype(jnp.bfloat16)
    late_rows = (late_values - lax.optimization_barrier(jnp.mean(late_values, axis=0))).astype(jnp.bfloat16)
    gram_early = jnp.dot(early_rows, early_rows.T, preferred_element_type=jnp.float32)
    gram_late = jnp.dot(late_rows, late_rows.T, preferred_element_type=jnp.float32)
    row_align = lax.optimization_barrier(jnp.sum(gram_early * gram_late, axis=1))
    hsic_kl = jnp.sum(row_align)
    hsic_kk = jnp.sum(gram_early * gram_early)
    hsic_ll = jnp.sum(gram_late * gram_late)
    scale_norm = jnp.sqrt(hsic_kk * hsic_ll)
    similarity = hsic_kl / scale_norm
    token_share = TOKENS * row_align / scale_norm
    return (similarity, token_share, early_rows, late_rows)
```

```python
import jax
import jax.numpy as jnp
from jax import lax
from jax.experimental import pallas as pl
from jax.experimental.pallas import tpu as pltpu
from jax.sharding import PartitionSpec as P

MESH = pl.DeviceIdType.MESH
F32 = jnp.float32
BF16 = jnp.bfloat16

SLOTS = ((0, 0), (1, 0), (0, 1), (1, 1), (1, 3), (3, 1))
TILES = (
    (0, 0, False),
    (1, 0, True),
    (2, 0, True),
    (1, 2, True),
    (4, 2, True),
    (5, 1, True),
    (4, 5, False),
    (3, 0, True),
    (3, 5, False),
    (4, 3, False),
)
K_CORE = 1
L_CORE = 0
PIECES = 8


def send(src, dst, send_sem, recv_sem, gx, gy):
    pltpu.make_async_remote_copy(
        src_ref=src,
        dst_ref=dst,
        send_sem=send_sem,
        recv_sem=recv_sem,
        device_id=(gx, gy),
        device_id_type=MESH,
    ).start()


def kernel(
    xt_hbm,
    late_hbm,
    share_ref,
    sim_ref,
    eout_hbm,
    lout_hbm,
    xt,
    late,
    cen,
    rt,
    blocks,
    gram,
    stage,
    parts,
    parts0,
    own_sum,
    plane_sums,
    mean_out,
    means,
    early_pieces,
    early_out,
    late_out,
    acc,
    row_cols,
    col_acc,
    msg,
    msg_in,
    total,
    total_in,
    load_sem,
    out_sem,
    late_send,
    late_recv,
    early_send,
    early_recv,
    pair_send,
    sums_send,
    sums_recv,
    mean_send,
    mean_recv,
    gather_send,
    gather_recv,
    rows_send,
    rows_recv,
    part_send,
    part_recv,
    part0_send,
    part0_recv,
    msg_send,
    msg_recv,
    total_send,
    total_recv,
):
    gx = lax.axis_index("gx")
    z = lax.axis_index("gy")
    core = lax.rem(gx, 2)
    chip = gx // 2
    x = chip // 4
    y = lax.rem(chip, 4)
    partner = gx + 1 - 2 * core
    k_dev = 2 * chip + K_CORE
    l_dev = 2 * chip + L_CORE
    is_k = core == K_CORE
    is_l = core == L_CORE

    def arrived(ref, sem):
        pltpu.make_async_remote_copy(
            src_ref=ref, dst_ref=ref, send_sem=sem, recv_sem=sem, device_id=(partner, z), device_id_type=MESH
        ).wait_recv()

    def left(ref, sem):
        pltpu.make_async_remote_copy(
            src_ref=ref, dst_ref=ref, send_sem=sem, recv_sem=sem, device_id=(partner, z), device_id_type=MESH
        ).wait_send()

    def chip_at(dx, dy):
        return lax.rem(x + dx, 4) * 4 + lax.rem(y + dy, 4)

    def level(dz):
        return lax.rem(z + dz, 4)

    barrier = pltpu.get_barrier_semaphore()

    @pl.loop(1, 16)
    def _(r):
        other = lax.rem(chip + r, 16)
        pl.semaphore_signal(barrier, inc=1, device_id=(2 * other, z), device_id_type=MESH)
        pl.semaphore_signal(barrier, inc=1, device_id=(2 * other + 1, z), device_id_type=MESH)

    for dz in (1, 2, 3):
        pl.semaphore_signal(barrier, inc=1, device_id=(2 * chip, level(dz)), device_id_type=MESH)
        pl.semaphore_signal(barrier, inc=1, device_id=(2 * chip + 1, level(dz)), device_id_type=MESH)
    pl.semaphore_signal(barrier, inc=1, device_id=(partner, z), device_id_type=MESH)

    load_x = pltpu.make_async_copy(xt_hbm, xt, load_sem.at[0])
    load_y = pltpu.make_async_copy(late_hbm, late, load_sem.at[1])
    load_x.start()
    load_y.start()
    load_x.wait()

    sums = jnp.zeros((64, 256), F32)
    for u in range(16):
        sums = sums + xt[:, 256 * u : 256 * (u + 1)].astype(F32)
    col_mean = jnp.sum(sums, axis=1, keepdims=True) / 4096.0
    for u in range(16):
        cen[u] = (xt[:, 256 * u : 256 * (u + 1)].astype(F32) - col_mean).astype(BF16)
    load_y.wait()

    pl.semaphore_wait(barrier, 37)

    my_rows = pl.ds(pl.multiple_of(32 * (4 * core + z), 32), 32)
    for dz in (1, 2, 3):
        to = level(dz)
        send(
            late.at[:, pl.ds(pl.multiple_of(2048 * to, 2048), 2048)],
            blocks.at[0, my_rows, :],
            late_send,
            late_recv,
            l_dev,
            to,
        )
    own_cols = pl.ds(pl.multiple_of(2048 * z, 2048), 2048)

    @pl.loop(1, 16)
    def _(r):
        other = lax.rem(chip + r, 16)
        send(cen.at[other], rt.at[gx], early_send, early_recv, 2 * other + K_CORE, z)

    @pl.when(is_k)
    def _():
        send(late.at[:, own_cols], blocks.at[0, my_rows, :], pair_send.at[0], late_recv, l_dev, z)
        rt[gx] = cen[chip]
        arrived(rt.at[0:31], early_recv)

        @pl.loop(0, 16)
        def _(u):
            cols = jnp.concatenate([rt[2 * u].astype(F32), rt[2 * u + 1].astype(F32)], axis=0)
            at = pl.ds(pl.multiple_of(128 * u, 128), 128)
            blocks[0, :, at] = cols.T.astype(BF16)

    @pl.when(is_l)
    def _():
        send(cen.at[chip], rt.at[gx], pair_send.at[0], early_recv, k_dev, z)
        blocks[0, my_rows, :] = late[:, own_cols]
        arrived(blocks.at[0, 0:224, :], late_recv)
        for c in range(4):
            at = slice(512 * c, 512 * (c + 1))
            part = jnp.zeros((32, 512), F32)
            for r in range(8):
                part = part + blocks[0, 32 * r : 32 * (r + 1), at].astype(F32)
            own_sum[:, at] = jnp.sum(part, axis=0, keepdims=True)
        plane_sums[chip] = own_sum[...]

        @pl.loop(1, 16)
        def _(r):
            other = lax.rem(chip + r, 16)
            send(own_sum, plane_sums.at[chip], sums_send, sums_recv, 2 * other + L_CORE, z)

        arrived(plane_sums.at[0:15], sums_recv)
        mean = plane_sums[0]
        for u in range(1, 16):
            mean = mean + plane_sums[u]
        mean_out[...] = mean / 4096.0
        means[z] = mean_out[...]
        for c in range(4):
            at = slice(512 * c, 512 * (c + 1))
            m = mean_out[:, at]
            for r in range(8):
                rows = slice(32 * r, 32 * (r + 1))
                blocks[0, rows, at] = (blocks[0, rows, at].astype(F32) - m).astype(BF16)

    def forward(src, dst, piece, ex, ey):
        rows = pl.ds(32 * piece, 32)
        to = 2 * chip_at(4 - ex, 4 - ey) + core
        send(blocks.at[src, rows, :], blocks.at[dst, rows, :], gather_send, gather_recv.at[dst - 1, piece], to, z)

    for i in range(PIECES):
        forward(0, 1, i, 1, 0)
        forward(0, 2, i, 0, 1)

    @pl.when(is_l)
    def _():
        send(mean_out, means.at[z], pair_send.at[1], mean_recv, k_dev, z)
        for dz in (1, 2, 3):
            send(mean_out, means.at[z], mean_send, mean_recv, k_dev, level(dz))
            send(mean_out, means.at[z], mean_send, mean_recv, l_dev, level(dz))

    @pl.when(is_k)
    def _():
        for dz in (1, 2, 3):
            for q in (0, 1):
                rows = pl.ds(pl.multiple_of(32 * (4 * q + level(dz)), 32), 32)
                send(blocks.at[0, rows, :], early_pieces.at[z], rows_send, rows_recv, 2 * chip + q, level(dz))
        rows = pl.ds(pl.multiple_of(32 * (4 * L_CORE + z), 32), 32)
        send(blocks.at[0, rows, :], early_pieces.at[z], pair_send.at[1], rows_recv, l_dev, z)
        early_pieces[z] = blocks[0, my_rows, :]

    dims = (((1,), (1,)), ((), ()))

    def product(t):
        a, b, _ = TILES[t]
        gram[t] = lax.dot_general(blocks[a], blocks[b], dims, preferred_element_type=F32)
        if t > 0:
            stage[t - 1] = gram[t].astype(BF16)
        for dz in (1, 2, 3):
            to = level(dz)
            rows = pl.ds(pl.multiple_of(64 * to, 64), 64)
            slot = dz - 1 + 4 * (1 - core)
            if t == 0:
                send(gram.at[0, rows, :], parts0.at[slot], part0_send, part0_recv, k_dev, to)
            else:
                send(stage.at[t - 1, rows, :], parts.at[t - 1, slot], part_send, part_recv.at[t - 1], k_dev, to)

        @pl.when(is_l)
        def _():
            rows = pl.ds(pl.multiple_of(64 * z, 64), 64)
            if t == 0:
                send(gram.at[0, rows, :], parts0.at[3], pair_send.at[2], part0_recv, k_dev, z)
            else:
                send(stage.at[t - 1, rows, :], parts.at[t - 1, 3], pair_send.at[3], part_recv.at[t - 1], k_dev, z)

    lane = lax.broadcasted_iota(jnp.int32, (64, 128), 1)

    def settle(t):
        _, b, both = TILES[t]
        rows = pl.ds(pl.multiple_of(64 * z, 64), 64)
        if t == 0:
            arrived(parts0, part0_recv)
            get = lambda s: parts0[s]
        else:
            arrived(parts.at[t - 1], part_recv.at[t - 1])
            get = lambda s: parts[t - 1, s].astype(F32)
        k = gram[t, rows, :] + ((get(0) + get(1)) + get(2))
        l = (get(3) + get(4)) + (get(5) + get(6))
        h = k * l
        row_cols[...] += jnp.where(lane == t, jnp.sum(h, axis=1, keepdims=True), 0.0)
        weight = 1.0
        if both:
            weight = 2.0
            col_acc[b : b + 1, :] += jnp.sum(h, axis=0, keepdims=True)
        acc[0] += weight * (k * k)
        acc[1] += weight * (l * l)
        acc[2] += weight * h

    product(0)

    @pl.when(is_k)
    def _():
        acc[...] = jnp.zeros_like(acc)
        row_cols[...] = jnp.zeros_like(row_cols)
        col_acc[...] = jnp.zeros_like(col_acc)

    for i in range(PIECES):
        rows = slice(32 * i, 32 * (i + 1))
        arrived(blocks.at[1, rows, :], gather_recv.at[0, i])
        forward(1, 4, i, 0, 3)
        arrived(blocks.at[2, rows, :], gather_recv.at[1, i])
        forward(2, 5, i, 3, 0)
        rows = pl.ds(32 * i, 32)
        to = 2 * chip_at(4 - (1 - core), 4 - core) + core
        send(blocks.at[2 - core, rows, :], blocks.at[3, rows, :], gather_send, gather_recv.at[2, i], to, z)

    for t in (1, 2, 3):
        product(t)

    @pl.when(is_k)
    def _():
        arrived(means, mean_recv)
        arrived(early_pieces.at[0:3], rows_recv)

    @pl.when(is_l)
    def _():
        arrived(means.at[0:3], mean_recv)
        arrived(early_pieces, rows_recv)

    for c in range(4):
        at = slice(2048 * c, 2048 * (c + 1))
        late_out[:, at] = (late[:, at].astype(F32) - means[c]).astype(BF16)
    low = lax.broadcasted_iota(jnp.int32, (32, 128), 1) < 64
    for u in range(16):
        p = [early_pieces[c, :, 128 * u : 128 * (u + 1)].astype(F32) for c in range(4)]
        turned = [pltpu.roll(v, 64, 1) for v in p]
        for j in range(2):
            first = jnp.where(low, p[2 * j], turned[2 * j + 1])
            second = jnp.where(low, turned[2 * j], p[2 * j + 1])
            early_out[:, 128 * (4 * u + j) : 128 * (4 * u + j + 1)] = first.astype(BF16)
            early_out[:, 128 * (4 * u + 2 + j) : 128 * (4 * u + 3 + j)] = second.astype(BF16)
    put_e = pltpu.make_async_copy(early_out, eout_hbm, out_sem.at[0])
    put_l = pltpu.make_async_copy(late_out, lout_hbm, out_sem.at[1])
    put_e.start()
    put_l.start()

    for i in range(PIECES):
        arrived(blocks.at[4, 32 * i : 32 * (i + 1), :], gather_recv.at[3, i])
    product(4)
    for i in range(PIECES):
        arrived(blocks.at[5, 32 * i : 32 * (i + 1), :], gather_recv.at[4, i])
    product(5)
    product(6)

    @pl.when(is_k)
    def _():
        for t in (0, 1, 2, 3):
            settle(t)

    for i in range(PIECES):
        arrived(blocks.at[3, 32 * i : 32 * (i + 1), :], gather_recv.at[2, i])
    for t in (7, 8, 9):
        product(t)

    @pl.when(is_k)
    def _():
        for t in (4, 5, 6, 7, 8, 9):
            settle(t)
        sides = row_cols[...]
        turned = jnp.concatenate([sides] * 4, axis=0).T
        mine = lax.broadcasted_iota(jnp.int32, (1, 256), 1) // 64 == z
        scal_lane = lax.broadcasted_iota(jnp.int32, (1, 128), 1)
        scal = jnp.zeros((1, 128), F32)
        for j in range(3):
            s = jnp.sum(jnp.sum(acc[j], axis=0, keepdims=True), axis=1, keepdims=True)
            scal = jnp.where(scal_lane == j, s, scal)
        for dx in range(4):
            for dy in range(4):
                r = 4 * dx + dy
                if (dx, dy) in SLOTS:
                    slot = SLOTS.index((dx, dy))
                    row = jnp.zeros((1, 256), F32)
                    for t, (a, _, _) in enumerate(TILES):
                        if a == slot:
                            row = row + turned[t : t + 1, :]
                    msg[r, :, 0:256] = col_acc[slot : slot + 1, :] + jnp.where(mine, row, 0.0)
                else:
                    msg[r, :, 0:256] = jnp.zeros((1, 256), F32)
                msg[r, :, 256:384] = scal
        for dx in range(4):
            for dy in range(4):
                r = 4 * dx + dy
                if r:
                    send(msg.at[r], msg_in.at[r], msg_send, msg_recv, 2 * chip_at(dx, dy) + K_CORE, z)
        msg_in[0] = msg[0]
        arrived(msg_in.at[0:15], msg_recv)
        s = msg_in[0]
        for r in range(1, 16):
            s = s + msg_in[r]
        total[...] = s
        for dz in (1, 2, 3):
            send(total, total_in.at[dz - 1], total_send, total_recv, k_dev, level(dz))
            send(total, total_in.at[dz - 1], total_send, total_recv, l_dev, level(dz))
        send(total, total_in.at[3], pair_send.at[2], total_recv, l_dev, z)
        total_in[3] = total[...]
        arrived(total_in.at[0:3], total_recv)

    @pl.when(is_l)
    def _():
        arrived(total_in, total_recv)

    final = (total_in[0] + total_in[1]) + (total_in[2] + total_in[3])
    scal_lane = lax.broadcasted_iota(jnp.int32, (1, 128), 1)
    scal = final[:, 256:384]
    kk, ll, kl = (jnp.sum(jnp.where(scal_lane == j, scal, 0.0), axis=1, keepdims=True) for j in range(3))
    norm = jnp.sqrt(kk * ll)
    sim_ref[...] = jnp.broadcast_to(kl / norm, (1, 128))
    half = jnp.where(core == 0, final[:, 0:128], final[:, 128:256])
    tokens = half
    for j in (1, 2, 3):
        tokens = jnp.where(z == j, pltpu.roll(half, 128 - 32 * j, 1), tokens)
    share_ref[...] = 4096.0 * tokens / norm

    put_e.wait()
    put_l.wait()
    left(late.at[:, 0:6144], late_send)
    left(cen.at[0:15], early_send)
    left(blocks.at[1:6], gather_send)
    left(parts.at[:, 0:3], part_send)
    left(parts0.at[0:3], part0_send)

    @pl.when(is_k)
    def _():
        left(late.at[:, 0:2048], pair_send.at[0])
        left(early_pieces.at[0], pair_send.at[1])
        left(total, pair_send.at[2])
        left(blocks.at[0, 0:192, :], rows_send)
        left(msg.at[0:15], msg_send)
        left(msg.at[0:6], total_send)

    @pl.when(is_l)
    def _():
        left(cen.at[0], pair_send.at[0])
        left(mean_out, pair_send.at[1])
        left(parts0.at[0], pair_send.at[2])
        left(parts.at[:, 0], pair_send.at[3])
        left(plane_sums.at[0:15], sums_send)
        left(plane_sums.at[0:6], mean_send)


def body(layer_early, layer_late):
    vm = pltpu.VMEM
    dma = pltpu.SemaphoreType.DMA
    hbm = pl.BlockSpec(memory_space=pltpu.HBM)
    whole = pl.BlockSpec(memory_space=pltpu.VMEM)
    share, sim, early_rows, late_rows = pl.pallas_call(
        kernel,
        out_shape=(
            jax.ShapeDtypeStruct((1, 128), F32),
            jax.ShapeDtypeStruct((1, 128), F32),
            jax.ShapeDtypeStruct((32, 8192), BF16),
            jax.ShapeDtypeStruct((32, 8192), BF16),
        ),
        in_specs=[hbm, hbm],
        out_specs=(whole, whole, hbm, hbm),
        scratch_shapes=[
            vm((64, 4096), BF16),
            vm((32, 8192), BF16),
            vm((16, 64, 256), BF16),
            vm((32, 64, 256), BF16),
            vm((6, 256, 2048), BF16),
            vm((10, 256, 256), F32),
            vm((9, 256, 256), BF16),
            vm((9, 7, 64, 256), BF16),
            vm((7, 64, 256), F32),
            vm((1, 2048), F32),
            vm((16, 1, 2048), F32),
            vm((1, 2048), F32),
            vm((4, 1, 2048), F32),
            vm((4, 32, 2048), BF16),
            vm((32, 8192), BF16),
            vm((32, 8192), BF16),
            vm((3, 64, 256), F32),
            vm((64, 128), F32),
            vm((8, 256), F32),
            vm((16, 1, 384), F32),
            vm((16, 1, 384), F32),
            vm((1, 384), F32),
            vm((4, 1, 384), F32),
            dma((2,)),
            dma((2,)),
            dma,
            dma,
            dma,
            dma,
            dma((4,)),
            dma,
            dma,
            dma,
            dma,
            dma,
            dma((5, PIECES)),
            dma,
            dma,
            dma,
            dma((9,)),
            dma,
            dma,
            dma,
            dma,
            dma,
            dma,
        ],
        compiler_params=pltpu.CompilerParams(collective_id=0, has_side_effects=True, vmem_limit_bytes=48 << 20),
    )(layer_early.T, layer_late)
    return sim[0, 0], share[0, :32], early_rows, late_rows


def solution(mesh):
    return jax.shard_map(
        body,
        mesh=mesh,
        in_specs=(P(None, ("gx", "gy")), P(("gx", "gy"), None)),
        out_specs=(P(), P(("gx", "gy")), P(("gx", "gy"), None), P(("gx", "gy"), None)),
        check_vma=False,
    )
```

```python
import jax
import jax.numpy as jnp
from jax import lax
from jax.experimental import pallas as pl
from jax.experimental.pallas import tpu as pltpu
from jax.sharding import PartitionSpec as P

MESH = pl.DeviceIdType.MESH
F32 = jnp.float32
BF16 = jnp.bfloat16

SLOTS = ((0, 0), (1, 0), (0, 1), (1, 1), (1, 3), (3, 1))
TILES = (
    (0, 0, False),
    (1, 0, True),
    (2, 0, True),
    (1, 2, True),
    (4, 2, True),
    (5, 1, True),
    (4, 5, False),
    (3, 0, True),
    (3, 5, False),
    (4, 3, False),
)
K_CORE = 1
L_CORE = 0
PIECES = 8
ORDER = ((0, 0), (0, 1), (1, 0), (1, 1), (3, 0), (3, 1), (2, 0), (2, 1))


def send(src, dst, send_sem, recv_sem, gx, gy):
    pltpu.make_async_remote_copy(
        src_ref=src,
        dst_ref=dst,
        send_sem=send_sem,
        recv_sem=recv_sem,
        device_id=(gx, gy),
        device_id_type=MESH,
    ).start()


def kernel(
    xt_hbm,
    late_hbm,
    share_ref,
    sim_ref,
    eout_hbm,
    lout_hbm,
    xt,
    late,
    cen,
    rt,
    blocks,
    gram,
    stage,
    parts,
    parts0,
    own_sum,
    plane_sums,
    mean_out,
    means,
    early_pieces,
    early_out,
    late_out,
    acc,
    row_cols,
    col_acc,
    msg,
    msg_in,
    total,
    total_in,
    load_sem,
    out_sem,
    late_send,
    late_recv,
    early_send,
    early_recv,
    pair_send,
    sums_send,
    sums_recv,
    mean_send,
    mean_recv,
    gather_send,
    gather_recv,
    rows_send,
    rows_recv,
    part_send,
    part_recv,
    part0_send,
    part0_recv,
    msg_send,
    msg_recv,
    total_send,
    total_recv,
):
    gx = lax.axis_index("gx")
    z = lax.axis_index("gy")
    core = lax.rem(gx, 2)
    chip = gx // 2
    x = chip // 4
    y = lax.rem(chip, 4)
    partner = gx + 1 - 2 * core
    k_dev = 2 * chip + K_CORE
    l_dev = 2 * chip + L_CORE
    is_k = core == K_CORE
    is_l = core == L_CORE

    def arrived(ref, sem, name="wait"):
        with jax.named_scope(name):
            pltpu.make_async_remote_copy(
                src_ref=ref, dst_ref=ref, send_sem=sem, recv_sem=sem, device_id=(partner, z), device_id_type=MESH
            ).wait_recv()

    def left(ref, sem):
        pltpu.make_async_remote_copy(
            src_ref=ref, dst_ref=ref, send_sem=sem, recv_sem=sem, device_id=(partner, z), device_id_type=MESH
        ).wait_send()

    def chip_at(dx, dy):
        return lax.rem(x + dx, 4) * 4 + lax.rem(y + dy, 4)

    def level(dz):
        return lax.rem(z + dz, 4)

    load_x = pltpu.make_async_copy(xt_hbm, xt, load_sem.at[0])
    load_y = pltpu.make_async_copy(late_hbm, late, load_sem.at[1])
    load_x.start()
    load_y.start()
    barrier = pltpu.get_barrier_semaphore()

    @pl.loop(1, 16)
    def _(r):
        other = lax.rem(chip + r, 16)
        pl.semaphore_signal(barrier, inc=1, device_id=(2 * other, z), device_id_type=MESH)
        pl.semaphore_signal(barrier, inc=1, device_id=(2 * other + 1, z), device_id_type=MESH)

    for dz in (1, 2, 3):
        pl.semaphore_signal(barrier, inc=1, device_id=(2 * chip, level(dz)), device_id_type=MESH)
        pl.semaphore_signal(barrier, inc=1, device_id=(2 * chip + 1, level(dz)), device_id_type=MESH)
    pl.semaphore_signal(barrier, inc=1, device_id=(partner, z), device_id_type=MESH)

    with jax.named_scope("load"):
        load_x.wait()

    sums = jnp.zeros((64, 256), F32)
    for u in range(16):
        sums = sums + xt[:, 256 * u : 256 * (u + 1)].astype(F32)
    col_mean = jnp.sum(sums, axis=1, keepdims=True) / 4096.0
    for u in range(16):
        cen[u] = (xt[:, 256 * u : 256 * (u + 1)].astype(F32) - col_mean).astype(BF16)
    load_y.wait()

    with jax.named_scope("barrier"):
        pl.semaphore_wait(barrier, 37)

    def piece(j):
        dz, q = ORDER[j]
        return pl.ds(pl.multiple_of(32 * (4 * q + level(dz)), 32), 32)

    my_rows = pl.ds(pl.multiple_of(32 * (4 * core + z), 32), 32)
    for dz in (1, 3, 2):
        to = level(dz)
        send(
            late.at[:, pl.ds(pl.multiple_of(2048 * to, 2048), 2048)],
            blocks.at[0, my_rows, :],
            late_send,
            late_recv.at[2 * (4 - dz) + core],
            l_dev,
            to,
        )
    own_cols = pl.ds(pl.multiple_of(2048 * z, 2048), 2048)

    @pl.loop(1, 16)
    def _(r):
        other = lax.rem(chip + r, 16)
        send(cen.at[other], rt.at[gx], early_send, early_recv.at[x], 2 * other + K_CORE, z)

    def forward(src, dst, j, ex, ey):
        to = 2 * chip_at(4 - ex, 4 - ey) + core
        rows = piece(j)
        send(blocks.at[src, rows, :], blocks.at[dst, rows, :], gather_send, gather_recv.at[dst - 1, j], to, z)

    def start(j):
        forward(0, 1, j, 1, 0)
        forward(0, 2, j, 0, 1)

    @pl.when(is_k)
    def _():
        send(late.at[:, own_cols], blocks.at[0, my_rows, :], pair_send.at[0], late_recv.at[1], l_dev, z)
        rt[gx] = cen[chip]
        for dx in (0, 1, 3, 2):
            xs = lax.rem(x + dx, 4)
            arrived(rt.at[0 : 8 if dx else 7], early_recv.at[xs], f"w_early{dx}")

            @pl.loop(0, 4)
            def _(k):
                u = 4 * xs + k
                cols = jnp.concatenate([rt[2 * u].astype(F32), rt[2 * u + 1].astype(F32)], axis=0)
                at = pl.ds(pl.multiple_of(128 * u, 128), 128)
                blocks[0, :, at] = cols.T.astype(BF16)

        for j in range(PIECES):
            start(j)
        for dz in (1, 2, 3):
            for q in (0, 1):
                rows = pl.ds(pl.multiple_of(32 * (4 * q + level(dz)), 32), 32)
                send(blocks.at[0, rows, :], early_pieces.at[z], rows_send, rows_recv, 2 * chip + q, level(dz))
        rows = pl.ds(pl.multiple_of(32 * (4 * L_CORE + z), 32), 32)
        send(blocks.at[0, rows, :], early_pieces.at[z], pair_send.at[1], rows_recv, l_dev, z)
        early_pieces[z] = blocks[0, my_rows, :]

    @pl.when(is_l)
    def _():
        send(cen.at[chip], rt.at[gx], pair_send.at[0], early_recv.at[x], k_dev, z)
        blocks[0, my_rows, :] = late[:, own_cols]
        for j in range(PIECES):
            if j:
                arrived(blocks.at[0, piece(j), :], late_recv.at[2 * ORDER[j][0] + ORDER[j][1]], f"w_late{j}")
            if j < 6:
                start(j)
        for c in range(4):
            at = slice(512 * c, 512 * (c + 1))
            part = jnp.zeros((32, 512), F32)
            for r in range(8):
                part = part + blocks[0, 32 * r : 32 * (r + 1), at].astype(F32)
            own_sum[:, at] = jnp.sum(part, axis=0, keepdims=True)
        plane_sums[chip] = own_sum[...]

        @pl.loop(1, 16)
        def _(r):
            other = lax.rem(chip + r, 16)
            send(own_sum, plane_sums.at[chip], sums_send, sums_recv, 2 * other + L_CORE, z)

        start(6)
        start(7)

    def center(slot):
        for c in range(4):
            at = slice(512 * c, 512 * (c + 1))
            m = mean_out[:, at]
            for r in range(8):
                rows = slice(32 * r, 32 * (r + 1))
                blocks[6 + slot, rows, at] = (blocks[slot, rows, at].astype(F32) - m).astype(BF16)

    def late_mean():
        arrived(plane_sums.at[0:15], sums_recv, "w_sums")
        mean = plane_sums[0]
        for u in range(1, 16):
            mean = mean + plane_sums[u]
        mean_out[...] = mean / 4096.0
        means[z] = mean_out[...]
        send(mean_out, means.at[z], pair_send.at[1], mean_recv, k_dev, z)
        for dz in (1, 2, 3):
            send(mean_out, means.at[z], mean_send, mean_recv, k_dev, level(dz))
            send(mean_out, means.at[z], mean_send, mean_recv, l_dev, level(dz))
        center(0)

    dims = (((1,), (1,)), ((), ()))

    ready = 6 * (1 - core)

    def product(t):
        a, b, _ = TILES[t]
        with jax.named_scope(f"dot{t}"):
            gram[t] = lax.dot_general(blocks[a + ready], blocks[b + ready], dims, preferred_element_type=F32)
        if t > 0:
            stage[t - 1] = gram[t].astype(BF16)
        for dz in (1, 2, 3):
            to = level(dz)
            rows = pl.ds(pl.multiple_of(64 * to, 64), 64)
            slot = dz - 1 + 4 * (1 - core)
            if t == 0:
                send(gram.at[0, rows, :], parts0.at[slot], part0_send, part0_recv, k_dev, to)
            else:
                send(stage.at[t - 1, rows, :], parts.at[t - 1, slot], part_send, part_recv.at[t - 1], k_dev, to)

        @pl.when(is_l)
        def _():
            rows = pl.ds(pl.multiple_of(64 * z, 64), 64)
            if t == 0:
                send(gram.at[0, rows, :], parts0.at[3], pair_send.at[2], part0_recv, k_dev, z)
            else:
                send(stage.at[t - 1, rows, :], parts.at[t - 1, 3], pair_send.at[3], part_recv.at[t - 1], k_dev, z)

    lane = lax.broadcasted_iota(jnp.int32, (64, 128), 1)

    def settle(t):
        _, b, both = TILES[t]
        rows = pl.ds(pl.multiple_of(64 * z, 64), 64)
        if t == 0:
            arrived(parts0, part0_recv, "wp0")
            get = lambda s: parts0[s]
        else:
            arrived(parts.at[t - 1], part_recv.at[t - 1], f"wp{t}")
            get = lambda s: parts[t - 1, s].astype(F32)
        k = gram[t, rows, :] + ((get(0) + get(1)) + get(2))
        l = (get(3) + get(4)) + (get(5) + get(6))
        h = k * l
        row_cols[...] += jnp.where(lane == t, jnp.sum(h, axis=1, keepdims=True), 0.0)
        weight = 1.0
        if both:
            weight = 2.0
            col_acc[b : b + 1, :] += jnp.sum(h, axis=0, keepdims=True)
        acc[0] += weight * (k * k)
        acc[1] += weight * (l * l)
        acc[2] += weight * h

    @pl.when(is_k)
    def _():
        acc[...] = jnp.zeros_like(acc)
        row_cols[...] = jnp.zeros_like(row_cols)
        col_acc[...] = jnp.zeros_like(col_acc)

    for j in range(PIECES):
        rows = piece(j)
        arrived(blocks.at[1, rows, :], gather_recv.at[0, j], f"w1_{j}")
        forward(1, 4, j, 0, 3)
        arrived(blocks.at[2, rows, :], gather_recv.at[1, j], f"w2_{j}")
        forward(2, 5, j, 3, 0)
        to = 2 * chip_at(4 - (1 - core), 4 - core) + core
        send(blocks.at[2 - core, rows, :], blocks.at[3, rows, :], gather_send, gather_recv.at[2, j], to, z)
        if j == 4:
            pl.when(is_l)(late_mean)
            product(0)

    @pl.when(is_l)
    def _():
        center(1)
        center(2)

    for t in (1, 2, 3):
        product(t)

    @pl.when(is_k)
    def _():
        arrived(means, mean_recv, "w_mean")
        arrived(early_pieces.at[0:3], rows_recv, "w_rows")

    @pl.when(is_l)
    def _():
        arrived(means.at[0:3], mean_recv, "w_mean")
        arrived(early_pieces, rows_recv, "w_rows")

    for c in range(4):
        at = slice(2048 * c, 2048 * (c + 1))
        late_out[:, at] = (late[:, at].astype(F32) - means[c]).astype(BF16)
    low = lax.broadcasted_iota(jnp.int32, (32, 128), 1) < 64
    for u in range(16):
        p = [early_pieces[c, :, 128 * u : 128 * (u + 1)].astype(F32) for c in range(4)]
        turned = [pltpu.roll(v, 64, 1) for v in p]
        for j in range(2):
            first = jnp.where(low, p[2 * j], turned[2 * j + 1])
            second = jnp.where(low, turned[2 * j], p[2 * j + 1])
            early_out[:, 128 * (4 * u + j) : 128 * (4 * u + j + 1)] = first.astype(BF16)
            early_out[:, 128 * (4 * u + 2 + j) : 128 * (4 * u + 3 + j)] = second.astype(BF16)
    put_e = pltpu.make_async_copy(early_out, eout_hbm, out_sem.at[0])
    put_l = pltpu.make_async_copy(late_out, lout_hbm, out_sem.at[1])
    put_e.start()
    put_l.start()

    def take(slot):
        for j in range(PIECES):
            arrived(blocks.at[slot, piece(j), :], gather_recv.at[slot - 1, j], f"w{slot}_{j}")
        pl.when(is_l)(lambda: center(slot))

    take(4)
    product(4)
    take(5)
    product(5)
    product(6)

    @pl.when(is_k)
    def _():
        for t in (0, 1, 2, 3):
            settle(t)

    take(3)
    for t in (7, 8, 9):
        product(t)

    @pl.when(is_k)
    def _():
        for t in (4, 5, 6, 7, 8, 9):
            settle(t)
        sides = row_cols[...]
        turned = jnp.concatenate([sides] * 4, axis=0).T
        mine = lax.broadcasted_iota(jnp.int32, (1, 256), 1) // 64 == z
        scal_lane = lax.broadcasted_iota(jnp.int32, (1, 128), 1)
        scal = jnp.zeros((1, 128), F32)
        for j in range(3):
            s = jnp.sum(jnp.sum(acc[j], axis=0, keepdims=True), axis=1, keepdims=True)
            scal = jnp.where(scal_lane == j, s, scal)
        for dx in range(4):
            for dy in range(4):
                r = 4 * dx + dy
                if (dx, dy) in SLOTS:
                    slot = SLOTS.index((dx, dy))
                    row = jnp.zeros((1, 256), F32)
                    for t, (a, _, _) in enumerate(TILES):
                        if a == slot:
                            row = row + turned[t : t + 1, :]
                    msg[r, :, 0:256] = col_acc[slot : slot + 1, :] + jnp.where(mine, row, 0.0)
                else:
                    msg[r, :, 0:256] = jnp.zeros((1, 256), F32)
                msg[r, :, 256:384] = scal
        for dx in range(4):
            for dy in range(4):
                r = 4 * dx + dy
                if r:
                    send(msg.at[r], msg_in.at[r], msg_send, msg_recv, 2 * chip_at(dx, dy) + K_CORE, z)
        msg_in[0] = msg[0]
        arrived(msg_in.at[0:15], msg_recv, "w_msg")
        s = msg_in[0]
        for r in range(1, 16):
            s = s + msg_in[r]
        total[...] = s
        for dz in (1, 2, 3):
            send(total, total_in.at[dz - 1], total_send, total_recv, k_dev, level(dz))
            send(total, total_in.at[dz - 1], total_send, total_recv, l_dev, level(dz))
        send(total, total_in.at[3], pair_send.at[2], total_recv, l_dev, z)
        total_in[3] = total[...]
        arrived(total_in.at[0:3], total_recv, "w_tot")

    @pl.when(is_l)
    def _():
        arrived(total_in, total_recv, "w_tot")

    final = (total_in[0] + total_in[1]) + (total_in[2] + total_in[3])
    scal_lane = lax.broadcasted_iota(jnp.int32, (1, 128), 1)
    scal = final[:, 256:384]
    kk, ll, kl = (jnp.sum(jnp.where(scal_lane == j, scal, 0.0), axis=1, keepdims=True) for j in range(3))
    norm = jnp.sqrt(kk * ll)
    sim_ref[...] = jnp.broadcast_to(kl / norm, (1, 128))
    half = jnp.where(core == 0, final[:, 0:128], final[:, 128:256])
    tokens = half
    for j in (1, 2, 3):
        tokens = jnp.where(z == j, pltpu.roll(half, 128 - 32 * j, 1), tokens)
    share_ref[...] = 4096.0 * tokens / norm

    with jax.named_scope("end"):
        put_e.wait()
    put_l.wait()
    left(late.at[:, 0:6144], late_send)
    left(cen.at[0:15], early_send)
    left(blocks.at[1:6], gather_send)
    left(parts.at[:, 0:3], part_send)
    left(parts0.at[0:3], part0_send)

    @pl.when(is_k)
    def _():
        left(late.at[:, 0:2048], pair_send.at[0])
        left(early_pieces.at[0], pair_send.at[1])
        left(total, pair_send.at[2])
        left(blocks.at[0, 0:192, :], rows_send)
        left(msg.at[0:15], msg_send)
        left(msg.at[0:6], total_send)

    @pl.when(is_l)
    def _():
        left(cen.at[0], pair_send.at[0])
        left(mean_out, pair_send.at[1])
        left(parts0.at[0], pair_send.at[2])
        left(parts.at[:, 0], pair_send.at[3])
        left(plane_sums.at[0:15], sums_send)
        left(plane_sums.at[0:6], mean_send)


CHUNKS = 4


def publish(share_in, sim_in, early_in, late_in, share, sim, early, late, bufs, in_sem, out_sem):
    width = 8192 // CHUNKS
    moves = []
    for k, (src, dst) in enumerate(((early_in, early), (late_in, late))):
        for c in range(CHUNKS):
            at = pl.ds(width * c, width)
            n = CHUNKS * k + c
            moves.append(
                (
                    pltpu.make_async_copy(src.at[:, at], bufs.at[n], in_sem.at[n]),
                    pltpu.make_async_copy(bufs.at[n], dst.at[:, at], out_sem.at[n]),
                )
            )
    for get, _ in moves:
        get.start()
    share[...] = share_in[:, 0:32]
    sim[...] = sim_in[:, 0:1]
    for get, put in moves:
        get.wait()
        put.start()
    for _, put in moves:
        put.wait()


def body(layer_early, layer_late):
    vm = pltpu.VMEM
    dma = pltpu.SemaphoreType.DMA
    hbm = pl.BlockSpec(memory_space=pltpu.HBM)
    whole = pl.BlockSpec(memory_space=pltpu.VMEM)
    share, sim, early_rows, late_rows = pl.pallas_call(
        kernel,
        out_shape=(
            jax.ShapeDtypeStruct((1, 128), F32),
            jax.ShapeDtypeStruct((1, 128), F32),
            jax.ShapeDtypeStruct((32, 8192), BF16),
            jax.ShapeDtypeStruct((32, 8192), BF16),
        ),
        in_specs=[hbm, hbm],
        out_specs=(whole, whole, hbm, hbm),
        scratch_shapes=[
            vm((64, 4096), BF16),
            vm((32, 8192), BF16),
            vm((16, 64, 256), BF16),
            vm((32, 64, 256), BF16),
            vm((12, 256, 2048), BF16),
            vm((10, 256, 256), F32),
            vm((9, 256, 256), BF16),
            vm((9, 7, 64, 256), BF16),
            vm((7, 64, 256), F32),
            vm((1, 2048), F32),
            vm((16, 1, 2048), F32),
            vm((1, 2048), F32),
            vm((4, 1, 2048), F32),
            vm((4, 32, 2048), BF16),
            vm((32, 8192), BF16),
            vm((32, 8192), BF16),
            vm((3, 64, 256), F32),
            vm((64, 128), F32),
            vm((8, 256), F32),
            vm((16, 1, 384), F32),
            vm((16, 1, 384), F32),
            vm((1, 384), F32),
            vm((4, 1, 384), F32),
            dma((2,)),
            dma((2,)),
            dma,
            dma((8,)),
            dma,
            dma((4,)),
            dma((4,)),
            dma,
            dma,
            dma,
            dma,
            dma,
            dma((5, PIECES)),
            dma,
            dma,
            dma,
            dma((9,)),
            dma,
            dma,
            dma,
            dma,
            dma,
            dma,
        ],
        compiler_params=pltpu.CompilerParams(collective_id=0, has_side_effects=True, vmem_limit_bytes=67043328),
    )(layer_early.T, layer_late)
    share, sim, early_rows, late_rows = pl.pallas_call(
        publish,
        out_shape=(
            jax.ShapeDtypeStruct((1, 32), F32),
            jax.ShapeDtypeStruct((1, 1), F32),
            jax.ShapeDtypeStruct((32, 8192), BF16),
            jax.ShapeDtypeStruct((32, 8192), BF16),
        ),
        in_specs=[whole, whole, hbm, hbm],
        out_specs=(whole, whole, hbm, hbm),
        scratch_shapes=[vm((2 * CHUNKS, 32, 8192 // CHUNKS), BF16), dma((2 * CHUNKS,)), dma((2 * CHUNKS,))],
    )(share, sim, early_rows, late_rows)
    return sim.reshape(()), share.reshape(32), early_rows, late_rows


def solution(mesh):
    return jax.shard_map(
        body,
        mesh=mesh,
        in_specs=(P(None, ("gx", "gy")), P(("gx", "gy"), None)),
        out_specs=(P(), P(("gx", "gy")), P(("gx", "gy"), None), P(("gx", "gy"), None)),
        check_vma=False,
    )
```

```python
import jax
import jax.numpy as jnp
from jax import lax
from jax.experimental import pallas as pl
from jax.experimental.pallas import tpu as pltpu
from jax.sharding import PartitionSpec as P

MESH = pl.DeviceIdType.MESH
F32 = jnp.float32
BF16 = jnp.bfloat16

SLOTS = ((0, 0), (1, 0), (0, 1), (1, 1), (1, 3), (3, 1))
TILES = (
    (0, 0, False),
    (1, 0, True),
    (2, 0, True),
    (1, 2, True),
    (4, 2, True),
    (5, 1, True),
    (4, 5, False),
    (3, 0, True),
    (3, 5, False),
    (4, 3, False),
)
K_CORE = 1
L_CORE = 0
PIECES = 8
ORDER = ((0, 0), (0, 1), (1, 0), (1, 1), (3, 0), (3, 1), (2, 0), (2, 1))


def send(src, dst, send_sem, recv_sem, gx, gy):
    pltpu.make_async_remote_copy(
        src_ref=src,
        dst_ref=dst,
        send_sem=send_sem,
        recv_sem=recv_sem,
        device_id=(gx, gy),
        device_id_type=MESH,
    ).start()


def kernel(
    xt_hbm,
    late_hbm,
    share_ref,
    sim_ref,
    eout_hbm,
    lout_hbm,
    xt,
    late,
    cen,
    rt,
    blocks,
    gram,
    stage,
    parts,
    parts0,
    own_sum,
    plane_sums,
    mean_out,
    means,
    early_pieces,
    early_out,
    late_out,
    acc,
    row_cols,
    col_acc,
    msg,
    msg_in,
    total,
    total_in,
    load_sem,
    out_sem,
    late_send,
    late_recv,
    early_send,
    early_recv,
    pair_send,
    sums_send,
    sums_recv,
    mean_send,
    mean_recv,
    gather_send,
    gather_recv,
    rows_send,
    rows_recv,
    part_send,
    part_recv,
    part0_send,
    part0_recv,
    msg_send,
    msg_recv,
    total_send,
    total_recv,
):
    gx = lax.axis_index("gx")
    z = lax.axis_index("gy")
    core = lax.rem(gx, 2)
    chip = gx // 2
    x = chip // 4
    y = lax.rem(chip, 4)
    partner = gx + 1 - 2 * core
    k_dev = 2 * chip + K_CORE
    l_dev = 2 * chip + L_CORE
    is_k = core == K_CORE
    is_l = core == L_CORE

    def arrived(ref, sem, name="wait"):
        with jax.named_scope(name):
            pltpu.make_async_remote_copy(
                src_ref=ref, dst_ref=ref, send_sem=sem, recv_sem=sem, device_id=(partner, z), device_id_type=MESH
            ).wait_recv()

    def left(ref, sem):
        pltpu.make_async_remote_copy(
            src_ref=ref, dst_ref=ref, send_sem=sem, recv_sem=sem, device_id=(partner, z), device_id_type=MESH
        ).wait_send()

    def chip_at(dx, dy):
        return lax.rem(x + dx, 4) * 4 + lax.rem(y + dy, 4)

    def level(dz):
        return lax.rem(z + dz, 4)

    load_x = pltpu.make_async_copy(xt_hbm, xt, load_sem.at[0])
    load_y = pltpu.make_async_copy(late_hbm, late, load_sem.at[1])
    load_x.start()
    load_y.start()
    barrier = pltpu.get_barrier_semaphore()

    @pl.loop(1, 16)
    def _(r):
        other = lax.rem(chip + r, 16)
        pl.semaphore_signal(barrier, inc=1, device_id=(2 * other, z), device_id_type=MESH)
        pl.semaphore_signal(barrier, inc=1, device_id=(2 * other + 1, z), device_id_type=MESH)

    for dz in (1, 2, 3):
        pl.semaphore_signal(barrier, inc=1, device_id=(2 * chip, level(dz)), device_id_type=MESH)
        pl.semaphore_signal(barrier, inc=1, device_id=(2 * chip + 1, level(dz)), device_id_type=MESH)
    pl.semaphore_signal(barrier, inc=1, device_id=(partner, z), device_id_type=MESH)

    with jax.named_scope("load"):
        load_x.wait()

    sums = jnp.zeros((64, 256), F32)
    for u in range(16):
        sums = sums + xt[:, 256 * u : 256 * (u + 1)].astype(F32)
    col_mean = jnp.sum(sums, axis=1, keepdims=True) / 4096.0
    for u in range(16):
        cen[u] = (xt[:, 256 * u : 256 * (u + 1)].astype(F32) - col_mean).astype(BF16)
    load_y.wait()

    with jax.named_scope("barrier"):
        pl.semaphore_wait(barrier, 37)

    def piece(j):
        dz, q = ORDER[j]
        return pl.ds(pl.multiple_of(32 * (4 * q + level(dz)), 32), 32)

    my_rows = pl.ds(pl.multiple_of(32 * (4 * core + z), 32), 32)
    for dz in (1, 3, 2):
        to = level(dz)
        send(
            late.at[:, pl.ds(pl.multiple_of(2048 * to, 2048), 2048)],
            blocks.at[0, my_rows, :],
            late_send,
            late_recv.at[2 * (4 - dz) + core],
            l_dev,
            to,
        )
    own_cols = pl.ds(pl.multiple_of(2048 * z, 2048), 2048)

    @pl.loop(1, 16)
    def _(r):
        other = lax.rem(chip + r, 16)
        send(cen.at[other], rt.at[gx], early_send, early_recv.at[x], 2 * other + K_CORE, z)

    def forward(src, dst, j, ex, ey):
        to = 2 * chip_at(4 - ex, 4 - ey) + core
        rows = piece(j)
        send(blocks.at[src, rows, :], blocks.at[dst, rows, :], gather_send, gather_recv.at[dst - 1, j], to, z)

    def start(j):
        forward(0, 1, j, 1, 0)
        forward(0, 2, j, 0, 1)

    @pl.when(is_k)
    def _():
        send(late.at[:, own_cols], blocks.at[0, my_rows, :], pair_send.at[0], late_recv.at[1], l_dev, z)
        rt[gx] = cen[chip]
        for dx in (0, 1, 3, 2):
            xs = lax.rem(x + dx, 4)
            arrived(rt.at[0 : 8 if dx else 7], early_recv.at[xs], f"w_early{dx}")

            @pl.loop(0, 4)
            def _(k):
                u = 4 * xs + k
                cols = jnp.concatenate([rt[2 * u].astype(F32), rt[2 * u + 1].astype(F32)], axis=0)
                at = pl.ds(pl.multiple_of(128 * u, 128), 128)
                blocks[0, :, at] = cols.T.astype(BF16)

        for j in range(PIECES):
            start(j)
        for dz in (1, 2, 3):
            for q in (0, 1):
                rows = pl.ds(pl.multiple_of(32 * (4 * q + level(dz)), 32), 32)
                send(blocks.at[0, rows, :], early_pieces.at[z], rows_send, rows_recv, 2 * chip + q, level(dz))
        rows = pl.ds(pl.multiple_of(32 * (4 * L_CORE + z), 32), 32)
        send(blocks.at[0, rows, :], early_pieces.at[z], pair_send.at[1], rows_recv, l_dev, z)
        early_pieces[z] = blocks[0, my_rows, :]

    @pl.when(is_l)
    def _():
        send(cen.at[chip], rt.at[gx], pair_send.at[0], early_recv.at[x], k_dev, z)
        blocks[0, my_rows, :] = late[:, own_cols]
        for j in range(PIECES):
            if j:
                arrived(blocks.at[0, piece(j), :], late_recv.at[2 * ORDER[j][0] + ORDER[j][1]], f"w_late{j}")
            if j < 6:
                start(j)
        for c in range(4):
            at = slice(512 * c, 512 * (c + 1))
            part = jnp.zeros((32, 512), F32)
            for r in range(8):
                part = part + blocks[0, 32 * r : 32 * (r + 1), at].astype(F32)
            own_sum[:, at] = jnp.sum(part, axis=0, keepdims=True)
        plane_sums[chip] = own_sum[...]

        @pl.loop(1, 16)
        def _(r):
            other = lax.rem(chip + r, 16)
            send(own_sum, plane_sums.at[chip], sums_send, sums_recv, 2 * other + L_CORE, z)

        start(6)
        start(7)

    def center(slot):
        for c in range(4):
            at = slice(512 * c, 512 * (c + 1))
            m = mean_out[:, at]
            for r in range(8):
                rows = slice(32 * r, 32 * (r + 1))
                blocks[6 + slot, rows, at] = (blocks[slot, rows, at].astype(F32) - m).astype(BF16)

    def late_mean():
        arrived(plane_sums.at[0:15], sums_recv, "w_sums")
        mean = plane_sums[0]
        for u in range(1, 16):
            mean = mean + plane_sums[u]
        mean_out[...] = mean / 4096.0
        means[z] = mean_out[...]
        send(mean_out, means.at[z], pair_send.at[1], mean_recv, k_dev, z)
        for dz in (1, 2, 3):
            send(mean_out, means.at[z], mean_send, mean_recv, k_dev, level(dz))
            send(mean_out, means.at[z], mean_send, mean_recv, l_dev, level(dz))
        center(0)
        product(0)

    dims = (((1,), (1,)), ((), ()))

    ready = 6 * (1 - core)

    def product(t):
        a, b, _ = TILES[t]
        with jax.named_scope(f"dot{t}"):
            gram[t] = lax.dot_general(blocks[a + ready], blocks[b + ready], dims, preferred_element_type=F32)
        if t > 0:
            stage[t - 1] = gram[t].astype(BF16)
        for dz in (1, 2, 3):
            to = level(dz)
            rows = pl.ds(pl.multiple_of(64 * to, 64), 64)
            slot = dz - 1 + 4 * (1 - core)
            if t == 0:
                send(gram.at[0, rows, :], parts0.at[slot], part0_send, part0_recv, k_dev, to)
            else:
                send(stage.at[t - 1, rows, :], parts.at[t - 1, slot], part_send, part_recv.at[t - 1], k_dev, to)

        @pl.when(is_l)
        def _():
            rows = pl.ds(pl.multiple_of(64 * z, 64), 64)
            if t == 0:
                send(gram.at[0, rows, :], parts0.at[3], pair_send.at[2], part0_recv, k_dev, z)
            else:
                send(stage.at[t - 1, rows, :], parts.at[t - 1, 3], pair_send.at[3], part_recv.at[t - 1], k_dev, z)

    lane = lax.broadcasted_iota(jnp.int32, (64, 128), 1)

    def settle(t):
        _, b, both = TILES[t]
        rows = pl.ds(pl.multiple_of(64 * z, 64), 64)
        if t == 0:
            arrived(parts0, part0_recv, "wp0")
            get = lambda s: parts0[s]
        else:
            arrived(parts.at[t - 1], part_recv.at[t - 1], f"wp{t}")
            get = lambda s: parts[t - 1, s].astype(F32)
        k = gram[t, rows, :] + ((get(0) + get(1)) + get(2))
        l = (get(3) + get(4)) + (get(5) + get(6))
        h = k * l
        row_cols[...] += jnp.where(lane == t, jnp.sum(h, axis=1, keepdims=True), 0.0)
        weight = 1.0
        if both:
            weight = 2.0
            col_acc[b : b + 1, :] += jnp.sum(h, axis=0, keepdims=True)
        acc[0] += weight * (k * k)
        acc[1] += weight * (l * l)
        acc[2] += weight * h

    @pl.when(is_k)
    def _():
        acc[...] = jnp.zeros_like(acc)
        row_cols[...] = jnp.zeros_like(row_cols)
        col_acc[...] = jnp.zeros_like(col_acc)

        product(0)

    for j in range(PIECES):
        rows = piece(j)
        arrived(blocks.at[1, rows, :], gather_recv.at[0, j], f"w1_{j}")
        forward(1, 4, j, 0, 3)
        arrived(blocks.at[2, rows, :], gather_recv.at[1, j], f"w2_{j}")
        forward(2, 5, j, 3, 0)
        if j == 6:
            pl.when(is_l)(late_mean)

    for j in range(PIECES):
        forward(2 - core, 3, j, 1 - core, core)

    @pl.when(is_l)
    def _():
        center(1)
        center(2)

    for t in (1, 2, 3):
        product(t)

    @pl.when(is_k)
    def _():
        arrived(means, mean_recv, "w_mean")
        arrived(early_pieces.at[0:3], rows_recv, "w_rows")

    @pl.when(is_l)
    def _():
        arrived(means.at[0:3], mean_recv, "w_mean")
        arrived(early_pieces, rows_recv, "w_rows")

    for c in range(4):
        at = slice(2048 * c, 2048 * (c + 1))
        late_out[:, at] = (late[:, at].astype(F32) - means[c]).astype(BF16)
    low = lax.broadcasted_iota(jnp.int32, (32, 128), 1) < 64
    for u in range(16):
        p = [early_pieces[c, :, 128 * u : 128 * (u + 1)].astype(F32) for c in range(4)]
        turned = [pltpu.roll(v, 64, 1) for v in p]
        for j in range(2):
            first = jnp.where(low, p[2 * j], turned[2 * j + 1])
            second = jnp.where(low, turned[2 * j], p[2 * j + 1])
            early_out[:, 128 * (4 * u + j) : 128 * (4 * u + j + 1)] = first.astype(BF16)
            early_out[:, 128 * (4 * u + 2 + j) : 128 * (4 * u + 3 + j)] = second.astype(BF16)
    put_e = pltpu.make_async_copy(early_out, eout_hbm, out_sem.at[0])
    put_l = pltpu.make_async_copy(late_out, lout_hbm, out_sem.at[1])
    put_e.start()
    put_l.start()

    def take(slot):
        for j in range(PIECES):
            arrived(blocks.at[slot, piece(j), :], gather_recv.at[slot - 1, j], f"w{slot}_{j}")
        pl.when(is_l)(lambda: center(slot))

    take(4)
    product(4)
    take(5)
    product(5)
    product(6)

    @pl.when(is_k)
    def _():
        for t in (0, 1, 2, 3):
            settle(t)

    take(3)
    for t in (7, 8, 9):
        product(t)

    @pl.when(is_k)
    def _():
        for t in (4, 5, 6, 7, 8, 9):
            settle(t)
        sides = row_cols[...]
        turned = jnp.concatenate([sides] * 4, axis=0).T
        mine = lax.broadcasted_iota(jnp.int32, (1, 256), 1) // 64 == z
        scal_lane = lax.broadcasted_iota(jnp.int32, (1, 128), 1)
        scal = jnp.zeros((1, 128), F32)
        for j in range(3):
            s = jnp.sum(jnp.sum(acc[j], axis=0, keepdims=True), axis=1, keepdims=True)
            scal = jnp.where(scal_lane == j, s, scal)
        for dx in range(4):
            for dy in range(4):
                r = 4 * dx + dy
                if (dx, dy) in SLOTS:
                    slot = SLOTS.index((dx, dy))
                    row = jnp.zeros((1, 256), F32)
                    for t, (a, _, _) in enumerate(TILES):
                        if a == slot:
                            row = row + turned[t : t + 1, :]
                    msg[r, :, 0:256] = col_acc[slot : slot + 1, :] + jnp.where(mine, row, 0.0)
                else:
                    msg[r, :, 0:256] = jnp.zeros((1, 256), F32)
                msg[r, :, 256:384] = scal
        for dx in range(4):
            for dy in range(4):
                r = 4 * dx + dy
                if r:
                    send(msg.at[r], msg_in.at[r], msg_send, msg_recv, 2 * chip_at(dx, dy) + K_CORE, z)
        msg_in[0] = msg[0]
        arrived(msg_in.at[0:15], msg_recv, "w_msg")
        s = msg_in[0]
        for r in range(1, 16):
            s = s + msg_in[r]
        total[...] = s
        for dz in (1, 2, 3):
            send(total, total_in.at[dz - 1], total_send, total_recv, k_dev, level(dz))
            send(total, total_in.at[dz - 1], total_send, total_recv, l_dev, level(dz))
        send(total, total_in.at[3], pair_send.at[2], total_recv, l_dev, z)
        total_in[3] = total[...]
        arrived(total_in.at[0:3], total_recv, "w_tot")

    @pl.when(is_l)
    def _():
        arrived(total_in, total_recv, "w_tot")

    final = (total_in[0] + total_in[1]) + (total_in[2] + total_in[3])
    scal_lane = lax.broadcasted_iota(jnp.int32, (1, 128), 1)
    scal = final[:, 256:384]
    kk, ll, kl = (jnp.sum(jnp.where(scal_lane == j, scal, 0.0), axis=1, keepdims=True) for j in range(3))
    norm = jnp.sqrt(kk * ll)
    sim_ref[...] = jnp.broadcast_to(kl / norm, (1, 128))
    half = jnp.where(core == 0, final[:, 0:128], final[:, 128:256])
    tokens = half
    for j in (1, 2, 3):
        tokens = jnp.where(z == j, pltpu.roll(half, 128 - 32 * j, 1), tokens)
    share_ref[...] = 4096.0 * tokens / norm

    with jax.named_scope("end"):
        put_e.wait()
    put_l.wait()
    left(late.at[:, 0:6144], late_send)
    left(cen.at[0:15], early_send)
    left(blocks.at[1:6], gather_send)
    left(parts.at[:, 0:3], part_send)
    left(parts0.at[0:3], part0_send)

    @pl.when(is_k)
    def _():
        left(late.at[:, 0:2048], pair_send.at[0])
        left(early_pieces.at[0], pair_send.at[1])
        left(total, pair_send.at[2])
        left(blocks.at[0, 0:192, :], rows_send)
        left(msg.at[0:15], msg_send)
        left(msg.at[0:6], total_send)

    @pl.when(is_l)
    def _():
        left(cen.at[0], pair_send.at[0])
        left(mean_out, pair_send.at[1])
        left(parts0.at[0], pair_send.at[2])
        left(parts.at[:, 0], pair_send.at[3])
        left(plane_sums.at[0:15], sums_send)
        left(plane_sums.at[0:6], mean_send)


CHUNKS = 4


def publish(share_in, sim_in, early_in, late_in, share, sim, early, late, bufs, in_sem, out_sem):
    width = 8192 // CHUNKS
    moves = []
    for k, (src, dst) in enumerate(((early_in, early), (late_in, late))):
        for c in range(CHUNKS):
            at = pl.ds(width * c, width)
            n = CHUNKS * k + c
            moves.append(
                (
                    pltpu.make_async_copy(src.at[:, at], bufs.at[n], in_sem.at[n]),
                    pltpu.make_async_copy(bufs.at[n], dst.at[:, at], out_sem.at[n]),
                )
            )
    for get, _ in moves:
        get.start()
    share[...] = share_in[:, 0:32]
    sim[...] = sim_in[:, 0:1]
    for get, put in moves:
        get.wait()
        put.start()
    for _, put in moves:
        put.wait()


def body(layer_early, layer_late):
    vm = pltpu.VMEM
    dma = pltpu.SemaphoreType.DMA
    hbm = pl.BlockSpec(memory_space=pltpu.HBM)
    whole = pl.BlockSpec(memory_space=pltpu.VMEM)
    share, sim, early_rows, late_rows = pl.pallas_call(
        kernel,
        out_shape=(
            jax.ShapeDtypeStruct((1, 128), F32),
            jax.ShapeDtypeStruct((1, 128), F32),
            jax.ShapeDtypeStruct((32, 8192), BF16),
            jax.ShapeDtypeStruct((32, 8192), BF16),
        ),
        in_specs=[hbm, hbm],
        out_specs=(whole, whole, hbm, hbm),
        scratch_shapes=[
            vm((64, 4096), BF16),
            vm((32, 8192), BF16),
            vm((16, 64, 256), BF16),
            vm((32, 64, 256), BF16),
            vm((12, 256, 2048), BF16),
            vm((10, 256, 256), F32),
            vm((9, 256, 256), BF16),
            vm((9, 7, 64, 256), BF16),
            vm((7, 64, 256), F32),
            vm((1, 2048), F32),
            vm((16, 1, 2048), F32),
            vm((1, 2048), F32),
            vm((4, 1, 2048), F32),
            vm((4, 32, 2048), BF16),
            vm((32, 8192), BF16),
            vm((32, 8192), BF16),
            vm((3, 64, 256), F32),
            vm((64, 128), F32),
            vm((8, 256), F32),
            vm((16, 1, 384), F32),
            vm((16, 1, 384), F32),
            vm((1, 384), F32),
            vm((4, 1, 384), F32),
            dma((2,)),
            dma((2,)),
            dma,
            dma((8,)),
            dma,
            dma((4,)),
            dma((4,)),
            dma,
            dma,
            dma,
            dma,
            dma,
            dma((5, PIECES)),
            dma,
            dma,
            dma,
            dma((9,)),
            dma,
            dma,
            dma,
            dma,
            dma,
            dma,
        ],
        compiler_params=pltpu.CompilerParams(collective_id=0, has_side_effects=True, vmem_limit_bytes=67043328),
    )(layer_early.T, layer_late)
    share, sim, early_rows, late_rows = pl.pallas_call(
        publish,
        out_shape=(
            jax.ShapeDtypeStruct((1, 32), F32),
            jax.ShapeDtypeStruct((1, 1), F32),
            jax.ShapeDtypeStruct((32, 8192), BF16),
            jax.ShapeDtypeStruct((32, 8192), BF16),
        ),
        in_specs=[whole, whole, hbm, hbm],
        out_specs=(whole, whole, hbm, hbm),
        scratch_shapes=[vm((2 * CHUNKS, 32, 8192 // CHUNKS), BF16), dma((2 * CHUNKS,)), dma((2 * CHUNKS,))],
    )(share, sim, early_rows, late_rows)
    return sim.reshape(()), share.reshape(32), early_rows, late_rows


def solution(mesh):
    return jax.shard_map(
        body,
        mesh=mesh,
        in_specs=(P(None, ("gx", "gy")), P(("gx", "gy"), None)),
        out_specs=(P(), P(("gx", "gy")), P(("gx", "gy"), None), P(("gx", "gy"), None)),
        check_vma=False,
    )
```

```python
import jax
import jax.numpy as jnp
from jax import lax
from jax.experimental import pallas as pl
from jax.experimental.pallas import tpu as pltpu
from jax.sharding import PartitionSpec as P

MESH = pl.DeviceIdType.MESH
F32 = jnp.float32
BF16 = jnp.bfloat16

SLOTS = ((0, 0), (1, 0), (0, 1), (1, 1), (1, 3), (3, 1))
TILES = ((0, 0), (1, 0), (2, 0), (1, 2), (4, 2), (5, 1), (3, 0), (4, 5), (3, 5), (3, 4))
SHARED = 7
K_CORE = 1
L_CORE = 0
PIECES = 8
ORDER = ((0, 0), (0, 1), (1, 0), (1, 1), (3, 0), (3, 1), (2, 0), (2, 1))


def send(src, dst, send_sem, recv_sem, gx, gy):
    pltpu.make_async_remote_copy(
        src_ref=src,
        dst_ref=dst,
        send_sem=send_sem,
        recv_sem=recv_sem,
        device_id=(gx, gy),
        device_id_type=MESH,
    ).start()


def kernel(
    xt_hbm,
    late_hbm,
    share_ref,
    sim_ref,
    eout_hbm,
    lout_hbm,
    xt,
    late,
    cen,
    rt,
    blocks,
    gram,
    stage,
    parts,
    halves,
    half_parts,
    parts0,
    own_sum,
    plane_sums,
    mean_out,
    means,
    early_pieces,
    early_out,
    late_out,
    acc,
    row_cols,
    half_cols,
    col_acc,
    msg,
    msg_in,
    total,
    total_in,
    load_sem,
    out_sem,
    late_send,
    late_recv,
    early_send,
    early_recv,
    pair_send,
    sums_send,
    sums_recv,
    mean_send,
    mean_recv,
    gather_send,
    gather_recv,
    rows_send,
    rows_recv,
    part_send,
    part_recv,
    half_send,
    part0_send,
    part0_recv,
    msg_send,
    msg_recv,
    total_send,
    total_recv,
):
    gx = lax.axis_index("gx")
    z = lax.axis_index("gy")
    core = lax.rem(gx, 2)
    chip = gx // 2
    x = chip // 4
    y = lax.rem(chip, 4)
    partner = gx + 1 - 2 * core
    k_dev = 2 * chip + K_CORE
    l_dev = 2 * chip + L_CORE
    is_k = core == K_CORE
    is_l = core == L_CORE

    def arrived(ref, sem, name="wait"):
        with jax.named_scope(name):
            pltpu.make_async_remote_copy(
                src_ref=ref, dst_ref=ref, send_sem=sem, recv_sem=sem, device_id=(partner, z), device_id_type=MESH
            ).wait_recv()

    def left(ref, sem):
        pltpu.make_async_remote_copy(
            src_ref=ref, dst_ref=ref, send_sem=sem, recv_sem=sem, device_id=(partner, z), device_id_type=MESH
        ).wait_send()

    def chip_at(dx, dy):
        return lax.rem(x + dx, 4) * 4 + lax.rem(y + dy, 4)

    def level(dz):
        return lax.rem(z + dz, 4)

    load_x = pltpu.make_async_copy(xt_hbm, xt, load_sem.at[0])
    load_y = pltpu.make_async_copy(late_hbm, late, load_sem.at[1])
    load_x.start()
    load_y.start()
    barrier = pltpu.get_barrier_semaphore()

    for r in range(1, 16):
        other = lax.rem(chip + r, 16)
        pl.semaphore_signal(barrier, inc=1, device_id=(2 * other, z), device_id_type=MESH)
        pl.semaphore_signal(barrier, inc=1, device_id=(2 * other + 1, z), device_id_type=MESH)

    for dz in (1, 2, 3):
        pl.semaphore_signal(barrier, inc=1, device_id=(2 * chip, level(dz)), device_id_type=MESH)
        pl.semaphore_signal(barrier, inc=1, device_id=(2 * chip + 1, level(dz)), device_id_type=MESH)
    pl.semaphore_signal(barrier, inc=1, device_id=(partner, z), device_id_type=MESH)

    with jax.named_scope("load"):
        load_x.wait()

    sums = jnp.zeros((64, 256), F32)
    for u in range(16):
        sums = sums + xt[:, 256 * u : 256 * (u + 1)].astype(F32)
    col_mean = jnp.sum(sums, axis=1, keepdims=True) / 4096.0
    for u in range(16):
        cen[u] = (xt[:, 256 * u : 256 * (u + 1)].astype(F32) - col_mean).astype(BF16)
    load_y.wait()

    with jax.named_scope("barrier"):
        pl.semaphore_wait(barrier, 37)

    def piece(j):
        dz, q = ORDER[j]
        return pl.ds(pl.multiple_of(32 * (4 * q + level(dz)), 32), 32)

    my_rows = pl.ds(pl.multiple_of(32 * (4 * core + z), 32), 32)
    for dz in (1, 3, 2):
        to = level(dz)
        send(
            late.at[:, pl.ds(pl.multiple_of(2048 * to, 2048), 2048)],
            blocks.at[0, my_rows, :],
            late_send,
            late_recv.at[2 * (4 - dz) + core],
            l_dev,
            to,
        )
    own_cols = pl.ds(pl.multiple_of(2048 * z, 2048), 2048)

    @pl.loop(1, 16)
    def _(r):
        other = lax.rem(chip + r, 16)
        send(cen.at[other], rt.at[gx], early_send, early_recv.at[x], 2 * other + K_CORE, z)

    def forward(src, dst, j, ex, ey):
        to = 2 * chip_at(4 - ex, 4 - ey) + core
        rows = piece(j)
        send(blocks.at[src, rows, :], blocks.at[dst, rows, :], gather_send, gather_recv.at[dst - 1, j], to, z)

    def start(j):
        forward(0, 1, j, 1, 0)
        forward(0, 2, j, 0, 1)

    @pl.when(is_k)
    def _():
        send(late.at[:, own_cols], blocks.at[0, my_rows, :], pair_send.at[0], late_recv.at[1], l_dev, z)
        rt[gx] = cen[chip]
        for dx in (0, 1, 3, 2):
            xs = lax.rem(x + dx, 4)
            arrived(rt.at[0 : 8 if dx else 7], early_recv.at[xs], f"w_early{dx}")

            @pl.loop(0, 4)
            def _(k):
                u = 4 * xs + k
                cols = jnp.concatenate([rt[2 * u].astype(F32), rt[2 * u + 1].astype(F32)], axis=0)
                at = pl.ds(pl.multiple_of(128 * u, 128), 128)
                blocks[0, :, at] = cols.T.astype(BF16)

        for j in range(PIECES):
            start(j)
        for dz in (1, 2, 3):
            for q in (0, 1):
                rows = pl.ds(pl.multiple_of(32 * (4 * q + level(dz)), 32), 32)
                send(blocks.at[0, rows, :], early_pieces.at[z], rows_send, rows_recv, 2 * chip + q, level(dz))
        rows = pl.ds(pl.multiple_of(32 * (4 * L_CORE + z), 32), 32)
        send(blocks.at[0, rows, :], early_pieces.at[z], pair_send.at[1], rows_recv, l_dev, z)
        early_pieces[z] = blocks[0, my_rows, :]

    @pl.when(is_l)
    def _():
        send(cen.at[chip], rt.at[gx], pair_send.at[0], early_recv.at[x], k_dev, z)
        blocks[0, my_rows, :] = late[:, own_cols]
        for j in range(PIECES):
            if j:
                arrived(blocks.at[0, piece(j), :], late_recv.at[2 * ORDER[j][0] + ORDER[j][1]], f"w_late{j}")
            if j < 6:
                start(j)
        for c in range(4):
            at = slice(512 * c, 512 * (c + 1))
            part = jnp.zeros((32, 512), F32)
            for r in range(8):
                part = part + blocks[0, 32 * r : 32 * (r + 1), at].astype(F32)
            own_sum[:, at] = jnp.sum(part, axis=0, keepdims=True)
        plane_sums[chip] = own_sum[...]

        @pl.loop(1, 16)
        def _(r):
            other = lax.rem(chip + r, 16)
            send(own_sum, plane_sums.at[chip], sums_send, sums_recv, 2 * other + L_CORE, z)

        start(6)
        start(7)

    def center(slot):
        for c in range(4):
            at = slice(512 * c, 512 * (c + 1))
            m = mean_out[:, at]
            for r in range(8):
                rows = slice(32 * r, 32 * (r + 1))
                blocks[6 + slot, rows, at] = (blocks[slot, rows, at].astype(F32) - m).astype(BF16)

    def late_mean():
        arrived(plane_sums.at[0:15], sums_recv, "w_sums")
        mean = plane_sums[0]
        for u in range(1, 16):
            mean = mean + plane_sums[u]
        mean_out[...] = mean / 4096.0
        means[z] = mean_out[...]
        send(mean_out, means.at[z], pair_send.at[1], mean_recv, k_dev, z)
        for dz in (1, 2, 3):
            send(mean_out, means.at[z], mean_send, mean_recv, k_dev, level(dz))
            send(mean_out, means.at[z], mean_send, mean_recv, l_dev, level(dz))
        center(0)
        product(0)

    dims = (((1,), (1,)), ((), ()))

    ready = 6 * (1 - core)

    def sides(t):
        a, b = TILES[t]
        if t < SHARED:
            return a, b, 0
        half = (y if t == 9 else x) // 2
        return a + half * (b - a), b + half * (a - b), half

    def product(t):
        a, b, half = sides(t)
        with jax.named_scope(f"dot{t}"):
            if t < SHARED:
                gram[t] = lax.dot_general(blocks[a + ready], blocks[b + ready], dims, preferred_element_type=F32)
            else:
                top = pl.ds(pl.multiple_of(128 * half, 128), 128)
                gram[t, 0:128, :] = lax.dot_general(
                    blocks[a + ready, top, :], blocks[b + ready], dims, preferred_element_type=F32
                )
        if t == 0:
            src, dst, size, out, into, pair = gram.at[0], parts0, 64, part0_send, part0_recv, 2
        elif t < SHARED:
            src, dst, size, out, into, pair = stage.at[t - 1], parts.at[t - 1], 64, part_send, part_recv.at[t - 1], 3
            stage[t - 1] = gram[t].astype(BF16)
        else:
            n = t - SHARED
            src, dst, size, out, into, pair = halves.at[n], half_parts.at[n], 32, half_send, part_recv.at[t - 1], 4
            halves[n] = gram[t, 0:128, :].astype(BF16)
        for dz in (1, 2, 3):
            to = level(dz)
            rows = pl.ds(pl.multiple_of(size * to, size), size)
            send(src.at[rows, :], dst.at[dz - 1 + 4 * (1 - core)], out, into, k_dev, to)

        @pl.when(is_l)
        def _():
            rows = pl.ds(pl.multiple_of(size * z, size), size)
            send(src.at[rows, :], dst.at[3], pair_send.at[pair], into, k_dev, z)

    def settle(t):
        _, b, _ = sides(t)
        if t == 0:
            size, buf, sem = 64, parts0, part0_recv
        elif t < SHARED:
            size, buf, sem = 64, parts.at[t - 1], part_recv.at[t - 1]
        else:
            size, buf, sem = 32, half_parts.at[t - SHARED], part_recv.at[t - 1]
        arrived(buf, sem, f"wp{t}")
        part = [buf[n].astype(F32) for n in range(7)]
        rows = pl.ds(pl.multiple_of(size * z, size), size)
        k = gram[t, rows, :] + ((part[0] + part[1]) + part[2])
        l = (part[3] + part[4]) + (part[5] + part[6])
        h = k * l
        lane = lax.broadcasted_iota(jnp.int32, (size, 128), 1)
        own = jnp.where(lane == t, jnp.sum(h, axis=1, keepdims=True), 0.0)
        weight = 1.0
        if t:
            weight = 2.0
            across = jnp.sum(h, axis=0, keepdims=True)
            col_acc[...] += jnp.where(slot_row == b, across, 0.0)
        if t < SHARED:
            row_cols[...] += own
        else:
            half_cols[...] += own
        acc[0, 0:size] += weight * (k * k)
        acc[1, 0:size] += weight * (l * l)
        acc[2, 0:size] += weight * h

    slot_row = lax.broadcasted_iota(jnp.int32, (8, 256), 0)

    @pl.when(is_k)
    def _():
        acc[...] = jnp.zeros_like(acc)
        row_cols[...] = jnp.zeros_like(row_cols)
        half_cols[...] = jnp.zeros_like(half_cols)
        col_acc[...] = jnp.zeros_like(col_acc)

        product(0)

    for j in range(PIECES):
        rows = piece(j)
        arrived(blocks.at[1, rows, :], gather_recv.at[0, j], f"w1_{j}")
        forward(1, 4, j, 0, 3)
        arrived(blocks.at[2, rows, :], gather_recv.at[1, j], f"w2_{j}")
        forward(2, 5, j, 3, 0)
        pl.when(is_k)(lambda: forward(1, 3, j, 0, 1))
        if j == 6:
            pl.when(is_l)(late_mean)

    @pl.when(is_l)
    def _():
        for j in range(PIECES):
            forward(2, 3, j, 1, 0)

    @pl.when(is_l)
    def _():
        center(1)
        center(2)

    for t in (1, 2, 3):
        product(t)

    @pl.when(is_k)
    def _():
        arrived(means, mean_recv, "w_mean")
        arrived(early_pieces.at[0:3], rows_recv, "w_rows")

    @pl.when(is_l)
    def _():
        arrived(means.at[0:3], mean_recv, "w_mean")
        arrived(early_pieces, rows_recv, "w_rows")

    for c in range(4):
        at = slice(2048 * c, 2048 * (c + 1))
        late_out[:, at] = (late[:, at].astype(F32) - means[c]).astype(BF16)
    low = lax.broadcasted_iota(jnp.int32, (32, 128), 1) < 64
    for u in range(16):
        p = [early_pieces[c, :, 128 * u : 128 * (u + 1)].astype(F32) for c in range(4)]
        turned = [pltpu.roll(v, 64, 1) for v in p]
        for j in range(2):
            first = jnp.where(low, p[2 * j], turned[2 * j + 1])
            second = jnp.where(low, turned[2 * j], p[2 * j + 1])
            early_out[:, 128 * (4 * u + j) : 128 * (4 * u + j + 1)] = first.astype(BF16)
            early_out[:, 128 * (4 * u + 2 + j) : 128 * (4 * u + 3 + j)] = second.astype(BF16)
    put_e = pltpu.make_async_copy(early_out, eout_hbm, out_sem.at[0])
    put_l = pltpu.make_async_copy(late_out, lout_hbm, out_sem.at[1])
    put_e.start()
    put_l.start()

    def take(slot):
        for j in range(PIECES):
            arrived(blocks.at[slot, piece(j), :], gather_recv.at[slot - 1, j], f"w{slot}_{j}")
        pl.when(is_l)(lambda: center(slot))

    take(4)
    product(4)
    take(5)
    product(5)
    product(7)

    @pl.when(is_k)
    def _():
        for t in (0, 1, 2, 3):
            settle(t)

    take(3)
    for t in (6, 8, 9):
        product(t)

    @pl.when(is_k)
    def _():
        for t in (4, 5, 7, 6, 8, 9):
            settle(t)
        turned = jnp.concatenate([row_cols[...]] * 4, axis=0).T
        half_turned = jnp.concatenate([half_cols[...]] * 8, axis=0).T
        col = lax.broadcasted_iota(jnp.int32, (1, 256), 1)
        both = col_acc[...]
        for t in range(len(TILES)):
            a, _, half = sides(t)
            if t < SHARED:
                row = jnp.where(col // 64 == z, turned[t : t + 1, :], 0.0)
            else:
                row = jnp.where(col // 32 == 4 * half + z, half_turned[t : t + 1, :], 0.0)
            both = both + jnp.where(slot_row == a, row, 0.0)
        scal_lane = lax.broadcasted_iota(jnp.int32, (1, 128), 1)
        scal = jnp.zeros((1, 128), F32)
        for j in range(3):
            s = jnp.sum(jnp.sum(acc[j], axis=0, keepdims=True), axis=1, keepdims=True)
            scal = jnp.where(scal_lane == j, s, scal)
        for dx in range(4):
            for dy in range(4):
                r = 4 * dx + dy
                if (dx, dy) in SLOTS:
                    slot = SLOTS.index((dx, dy))
                    msg[r, :, 0:256] = both[slot : slot + 1, :]
                else:
                    msg[r, :, 0:256] = jnp.zeros((1, 256), F32)
                msg[r, :, 256:384] = scal
        for dx in range(4):
            for dy in range(4):
                r = 4 * dx + dy
                if r:
                    send(msg.at[r], msg_in.at[r], msg_send, msg_recv, 2 * chip_at(dx, dy) + K_CORE, z)
        msg_in[0] = msg[0]
        arrived(msg_in.at[0:15], msg_recv, "w_msg")
        s = msg_in[0]
        for r in range(1, 16):
            s = s + msg_in[r]
        total[...] = s
        for dz in (1, 2, 3):
            send(total, total_in.at[dz - 1], total_send, total_recv, k_dev, level(dz))
            send(total, total_in.at[dz - 1], total_send, total_recv, l_dev, level(dz))
        send(total, total_in.at[3], pair_send.at[2], total_recv, l_dev, z)
        total_in[3] = total[...]
        arrived(total_in.at[0:3], total_recv, "w_tot")

    @pl.when(is_l)
    def _():
        arrived(total_in, total_recv, "w_tot")

    final = (total_in[0] + total_in[1]) + (total_in[2] + total_in[3])
    scal_lane = lax.broadcasted_iota(jnp.int32, (1, 128), 1)
    scal = final[:, 256:384]
    kk, ll, kl = (jnp.sum(jnp.where(scal_lane == j, scal, 0.0), axis=1, keepdims=True) for j in range(3))
    norm = jnp.sqrt(kk * ll)
    sim_ref[...] = kl / norm
    half = jnp.where(core == 0, final[:, 0:128], final[:, 128:256])
    tokens = half
    for j in (1, 2, 3):
        tokens = jnp.where(z == j, pltpu.roll(half, 128 - 32 * j, 1), tokens)
    share_ref[...] = (4096.0 * tokens / norm)[:, 0:32]

    with jax.named_scope("end"):
        put_e.wait()
    put_l.wait()
    left(late.at[:, 0:6144], late_send)
    left(cen.at[0:15], early_send)
    left(blocks.at[1:6], gather_send)
    left(parts.at[:, 0:3], part_send)
    left(half_parts.at[:, 0:3], half_send)
    left(parts0.at[0:3], part0_send)

    @pl.when(is_k)
    def _():
        left(late.at[:, 0:2048], pair_send.at[0])
        left(early_pieces.at[0], pair_send.at[1])
        left(total, pair_send.at[2])
        left(blocks.at[0, 0:192, :], rows_send)
        left(msg.at[0:15], msg_send)
        left(msg.at[0:6], total_send)

    @pl.when(is_l)
    def _():
        left(cen.at[0], pair_send.at[0])
        left(mean_out, pair_send.at[1])
        left(parts0.at[0], pair_send.at[2])
        left(parts.at[:, 0], pair_send.at[3])
        left(half_parts.at[:, 0], pair_send.at[4])
        left(plane_sums.at[0:15], sums_send)
        left(plane_sums.at[0:6], mean_send)


CHUNKS = 4


def publish(share_in, sim_in, early_in, late_in, share, sim, early, late, bufs, share_buf, sim_buf, in_sem, out_sem):
    width = 8192 // CHUNKS
    ways = [(share_in, share_buf, share), (sim_in, sim_buf, sim)]
    for k, (src, dst) in enumerate(((early_in, early), (late_in, late))):
        for c in range(CHUNKS):
            at = pl.ds(width * c, width)
            ways.append((src.at[:, at], bufs.at[CHUNKS * k + c], dst.at[:, at]))
    gets = [pltpu.make_async_copy(a, b, in_sem.at[n]) for n, (a, b, _) in enumerate(ways)]
    puts = [pltpu.make_async_copy(b, c, out_sem.at[n]) for n, (_, b, c) in enumerate(ways)]
    for get in gets:
        get.start()
    for get, put in zip(gets, puts):
        get.wait()
        put.start()
    for put in puts:
        put.wait()


def body(layer_early, layer_late):
    vm = pltpu.VMEM
    dma = pltpu.SemaphoreType.DMA
    hbm = pl.BlockSpec(memory_space=pltpu.HBM)
    whole = pl.BlockSpec(memory_space=pltpu.VMEM)
    share, sim, early_rows, late_rows = pl.pallas_call(
        kernel,
        out_shape=(
            jax.ShapeDtypeStruct((1, 32), F32),
            jax.ShapeDtypeStruct((1, 1), F32),
            jax.ShapeDtypeStruct((32, 8192), BF16),
            jax.ShapeDtypeStruct((32, 8192), BF16),
        ),
        in_specs=[hbm, hbm],
        out_specs=(whole, whole, hbm, hbm),
        scratch_shapes=[
            vm((64, 4096), BF16),
            vm((32, 8192), BF16),
            vm((16, 64, 256), BF16),
            vm((32, 64, 256), BF16),
            vm((12, 256, 2048), BF16),
            vm((10, 256, 256), F32),
            vm((6, 256, 256), BF16),
            vm((6, 7, 64, 256), BF16),
            vm((3, 128, 256), BF16),
            vm((3, 7, 32, 256), BF16),
            vm((7, 64, 256), F32),
            vm((1, 2048), F32),
            vm((16, 1, 2048), F32),
            vm((1, 2048), F32),
            vm((4, 1, 2048), F32),
            vm((4, 32, 2048), BF16),
            vm((32, 8192), BF16),
            vm((32, 8192), BF16),
            vm((3, 64, 256), F32),
            vm((64, 128), F32),
            vm((32, 128), F32),
            vm((8, 256), F32),
            vm((16, 1, 384), F32),
            vm((16, 1, 384), F32),
            vm((1, 384), F32),
            vm((4, 1, 384), F32),
            dma((2,)),
            dma((2,)),
            dma,
            dma((8,)),
            dma,
            dma((4,)),
            dma((5,)),
            dma,
            dma,
            dma,
            dma,
            dma,
            dma((5, PIECES)),
            dma,
            dma,
            dma,
            dma((9,)),
            dma,
            dma,
            dma,
            dma,
            dma,
            dma,
            dma,
        ],
        compiler_params=pltpu.CompilerParams(collective_id=0, has_side_effects=True, vmem_limit_bytes=67043328),
    )(layer_early.T, layer_late)
    share, sim, early_rows, late_rows = pl.pallas_call(
        publish,
        out_shape=(
            jax.ShapeDtypeStruct((1, 32), F32),
            jax.ShapeDtypeStruct((1, 1), F32),
            jax.ShapeDtypeStruct((32, 8192), BF16),
            jax.ShapeDtypeStruct((32, 8192), BF16),
        ),
        in_specs=[hbm] * 4,
        out_specs=(hbm,) * 4,
        scratch_shapes=[
            vm((2 * CHUNKS, 32, 8192 // CHUNKS), BF16),
            vm((1, 32), F32),
            vm((1, 1), F32),
            dma((2 * CHUNKS + 2,)),
            dma((2 * CHUNKS + 2,)),
        ],
    )(share, sim, early_rows, late_rows)
    return sim.reshape(()), share.reshape(32), early_rows, late_rows


def solution(mesh):
    return jax.shard_map(
        body,
        mesh=mesh,
        in_specs=(P(None, ("gx", "gy")), P(("gx", "gy"), None)),
        out_specs=(P(), P(("gx", "gy")), P(("gx", "gy"), None), P(("gx", "gy"), None)),
        check_vma=False,
    )
```

```python
import jax
import jax.numpy as jnp
from jax import lax
from jax.experimental import pallas as pl
from jax.experimental.pallas import tpu as pltpu
from jax.sharding import PartitionSpec as P

MESH = pl.DeviceIdType.MESH
F32 = jnp.float32
BF16 = jnp.bfloat16

SLOTS = ((0, 0), (1, 0), (0, 1), (1, 1), (1, 3), (3, 1))
TILES = ((0, 0), (1, 0), (2, 0), (1, 2), (4, 2), (5, 1), (3, 0), (4, 5), (3, 5), (3, 4))
SHARED = 7
K_CORE = 1
L_CORE = 0
PIECES = 8
ORDER = ((0, 0), (0, 1), (2, 0), (2, 1), (1, 0), (1, 1), (3, 0), (3, 1))
OTHERS = tuple((dx, dy) for dx in (2, 1, 3, 0) for dy in (2, 1, 3, 0) if dx or dy)


def send(src, dst, send_sem, recv_sem, gx, gy):
    pltpu.make_async_remote_copy(
        src_ref=src,
        dst_ref=dst,
        send_sem=send_sem,
        recv_sem=recv_sem,
        device_id=(gx, gy),
        device_id_type=MESH,
    ).start()


def kernel(
    xt_hbm,
    late_hbm,
    share_ref,
    sim_ref,
    eout_hbm,
    lout_hbm,
    xt,
    late,
    cen,
    rt,
    blocks,
    gram,
    stage,
    parts,
    halves,
    half_parts,
    parts0,
    own_sum,
    plane_sums,
    mean_out,
    means,
    early_pieces,
    early_out,
    late_out,
    acc,
    row_cols,
    half_cols,
    col_acc,
    msg,
    msg_in,
    total,
    total_in,
    load_sem,
    out_sem,
    late_send,
    late_recv,
    early_send,
    early_recv,
    pair_send,
    sums_send,
    sums_recv,
    mean_send,
    mean_recv,
    gather_send,
    gather_recv,
    rows_send,
    rows_recv,
    part_send,
    part_recv,
    half_send,
    part0_send,
    part0_recv,
    msg_send,
    msg_recv,
    total_send,
    total_recv,
):
    gx = lax.axis_index("gx")
    z = lax.axis_index("gy")
    core = lax.rem(gx, 2)
    chip = gx // 2
    x = chip // 4
    y = lax.rem(chip, 4)
    partner = gx + 1 - 2 * core
    k_dev = 2 * chip + K_CORE
    l_dev = 2 * chip + L_CORE
    is_k = core == K_CORE
    is_l = core == L_CORE

    def arrived(ref, sem, name="wait"):
        with jax.named_scope(name):
            pltpu.make_async_remote_copy(
                src_ref=ref, dst_ref=ref, send_sem=sem, recv_sem=sem, device_id=(partner, z), device_id_type=MESH
            ).wait_recv()

    def left(ref, sem):
        pltpu.make_async_remote_copy(
            src_ref=ref, dst_ref=ref, send_sem=sem, recv_sem=sem, device_id=(partner, z), device_id_type=MESH
        ).wait_send()

    def chip_at(dx, dy):
        return lax.rem(x + dx, 4) * 4 + lax.rem(y + dy, 4)

    def level(dz):
        return lax.rem(z + dz, 4)

    load_x = pltpu.make_async_copy(xt_hbm, xt, load_sem.at[0])
    load_y = pltpu.make_async_copy(late_hbm, late, load_sem.at[1])
    load_x.start()
    load_y.start()
    barrier = pltpu.get_barrier_semaphore()

    for dx, dy in OTHERS:
        other = chip_at(dx, dy)
        pl.semaphore_signal(barrier, inc=1, device_id=(2 * other + core, z), device_id_type=MESH)

    @pl.when(is_k)
    def _():
        for dx, dy in OTHERS:
            other = chip_at(dx, dy)
            pl.semaphore_signal(barrier, inc=1, device_id=(2 * other + L_CORE, z), device_id_type=MESH)

    for dz in (1, 2, 3):
        pl.semaphore_signal(barrier, inc=1, device_id=(2 * chip, level(dz)), device_id_type=MESH)
        pl.semaphore_signal(barrier, inc=1, device_id=(2 * chip + 1, level(dz)), device_id_type=MESH)
    pl.semaphore_signal(barrier, inc=1, device_id=(partner, z), device_id_type=MESH)

    with jax.named_scope("load"):
        load_x.wait()

    sums = jnp.zeros((64, 256), F32)
    for u in range(16):
        sums = sums + xt[:, 256 * u : 256 * (u + 1)].astype(F32)
    col_mean = jnp.sum(sums, axis=1, keepdims=True) / 4096.0
    for u in range(16):
        cen[u] = (xt[:, 256 * u : 256 * (u + 1)].astype(F32) - col_mean).astype(BF16)
    load_y.wait()

    with jax.named_scope("barrier"):
        pl.semaphore_wait(barrier, 22 + 15 * (1 - core))

    def piece(j):
        dz, q = ORDER[j]
        return pl.ds(pl.multiple_of(32 * (4 * q + level(dz)), 32), 32)

    my_rows = pl.ds(pl.multiple_of(32 * (4 * core + z), 32), 32)
    for dz in (2, 1, 3):
        to = level(dz)
        send(
            late.at[:, pl.ds(pl.multiple_of(2048 * to, 2048), 2048)],
            blocks.at[0, my_rows, :],
            late_send,
            late_recv.at[2 * (4 - dz) + core],
            l_dev,
            to,
        )
    own_cols = pl.ds(pl.multiple_of(2048 * z, 2048), 2048)

    for dx, dy in OTHERS:
        other = chip_at(dx, dy)
        send(cen.at[other], rt.at[gx], early_send, early_recv.at[x], 2 * other + K_CORE, z)

    def forward(src, dst, j, ex, ey):
        to = 2 * chip_at(4 - ex, 4 - ey) + core
        rows = piece(j)
        send(blocks.at[src, rows, :], blocks.at[dst, rows, :], gather_send, gather_recv.at[dst - 1, j], to, z)

    def start(j):
        forward(0, 1, j, 1, 0)
        forward(0, 2, j, 0, 1)

    @pl.when(is_k)
    def _():
        send(late.at[:, own_cols], blocks.at[0, my_rows, :], pair_send.at[0], late_recv.at[1], l_dev, z)
        rt[gx] = cen[chip]
        for dx in (2, 1, 3, 0):
            xs = lax.rem(x + dx, 4)
            arrived(rt.at[0 : 8 if dx else 7], early_recv.at[xs], f"w_early{dx}")

            @pl.loop(0, 4)
            def _(k):
                u = 4 * xs + k
                cols = jnp.concatenate([rt[2 * u].astype(F32), rt[2 * u + 1].astype(F32)], axis=0)
                at = pl.ds(pl.multiple_of(128 * u, 128), 128)
                blocks[0, :, at] = cols.T.astype(BF16)

        for j in range(PIECES):
            start(j)
        for dz in (1, 2, 3):
            for q in (0, 1):
                rows = pl.ds(pl.multiple_of(32 * (4 * q + level(dz)), 32), 32)
                send(blocks.at[0, rows, :], early_pieces.at[z], rows_send, rows_recv, 2 * chip + q, level(dz))
        rows = pl.ds(pl.multiple_of(32 * (4 * L_CORE + z), 32), 32)
        send(blocks.at[0, rows, :], early_pieces.at[z], pair_send.at[1], rows_recv, l_dev, z)
        early_pieces[z] = blocks[0, my_rows, :]

    @pl.when(is_l)
    def _():
        send(cen.at[chip], rt.at[gx], pair_send.at[0], early_recv.at[x], k_dev, z)
        blocks[0, my_rows, :] = late[:, own_cols]
        for j in range(PIECES):
            if j:
                arrived(blocks.at[0, piece(j), :], late_recv.at[2 * ORDER[j][0] + ORDER[j][1]], f"w_late{j}")
            if j < 6:
                start(j)
        for c in range(4):
            at = slice(512 * c, 512 * (c + 1))
            part = jnp.zeros((32, 512), F32)
            for r in range(8):
                part = part + blocks[0, 32 * r : 32 * (r + 1), at].astype(F32)
            own_sum[:, at] = jnp.sum(part, axis=0, keepdims=True)
        plane_sums[chip] = own_sum[...]

        @pl.loop(1, 16)
        def _(r):
            other = lax.rem(chip + r, 16)
            send(own_sum, plane_sums.at[chip], sums_send, sums_recv, 2 * other + L_CORE, z)

        start(6)
        start(7)

    def center(slot):
        for c in range(4):
            at = slice(512 * c, 512 * (c + 1))
            m = mean_out[:, at]
            for r in range(8):
                rows = slice(32 * r, 32 * (r + 1))
                blocks[6 + slot, rows, at] = (blocks[slot, rows, at].astype(F32) - m).astype(BF16)

    def late_mean():
        arrived(plane_sums.at[0:15], sums_recv, "w_sums")
        mean = plane_sums[0]
        for u in range(1, 16):
            mean = mean + plane_sums[u]
        mean_out[...] = mean / 4096.0
        means[z] = mean_out[...]
        send(mean_out, means.at[z], pair_send.at[1], mean_recv, k_dev, z)
        for dz in (1, 2, 3):
            send(mean_out, means.at[z], mean_send, mean_recv, k_dev, level(dz))
            send(mean_out, means.at[z], mean_send, mean_recv, l_dev, level(dz))
        center(0)
        product(0)

    dims = (((1,), (1,)), ((), ()))

    ready = 6 * (1 - core)

    def sides(t):
        a, b = TILES[t]
        if t < SHARED:
            return a, b, 0
        half = (y if t == 9 else x) // 2
        return a + half * (b - a), b + half * (a - b), half

    def product(t):
        a, b, half = sides(t)
        with jax.named_scope(f"dot{t}"):
            if t < SHARED:
                gram[t] = lax.dot_general(blocks[a + ready], blocks[b + ready], dims, preferred_element_type=F32)
            else:
                top = pl.ds(pl.multiple_of(128 * half, 128), 128)
                gram[t, 0:128, :] = lax.dot_general(
                    blocks[a + ready, top, :], blocks[b + ready], dims, preferred_element_type=F32
                )
        if t == 0:
            src, dst, size, out, into, pair = gram.at[0], parts0, 64, part0_send, part0_recv, 2
        elif t < SHARED:
            src, dst, size, out, into, pair = stage.at[t - 1], parts.at[t - 1], 64, part_send, part_recv.at[t - 1], 3
            stage[t - 1] = gram[t].astype(BF16)
        else:
            n = t - SHARED
            src, dst, size, out, into, pair = halves.at[n], half_parts.at[n], 32, half_send, part_recv.at[t - 1], 4
            halves[n] = gram[t, 0:128, :].astype(BF16)
        for dz in (1, 2, 3):
            to = level(dz)
            rows = pl.ds(pl.multiple_of(size * to, size), size)
            send(src.at[rows, :], dst.at[dz - 1 + 4 * (1 - core)], out, into, k_dev, to)

        @pl.when(is_l)
        def _():
            rows = pl.ds(pl.multiple_of(size * z, size), size)
            send(src.at[rows, :], dst.at[3], pair_send.at[pair], into, k_dev, z)

    def settle(t):
        _, b, _ = sides(t)
        if t == 0:
            size, buf, sem = 64, parts0, part0_recv
        elif t < SHARED:
            size, buf, sem = 64, parts.at[t - 1], part_recv.at[t - 1]
        else:
            size, buf, sem = 32, half_parts.at[t - SHARED], part_recv.at[t - 1]
        arrived(buf, sem, f"wp{t}")
        part = [buf[n].astype(F32) for n in range(7)]
        rows = pl.ds(pl.multiple_of(size * z, size), size)
        k = gram[t, rows, :] + ((part[0] + part[1]) + part[2])
        l = (part[3] + part[4]) + (part[5] + part[6])
        h = k * l
        lane = lax.broadcasted_iota(jnp.int32, (size, 128), 1)
        own = jnp.where(lane == t, jnp.sum(h, axis=1, keepdims=True), 0.0)
        weight = 1.0
        if t:
            weight = 2.0
            across = jnp.sum(h, axis=0, keepdims=True)
            col_acc[...] += jnp.where(slot_row == b, across, 0.0)
        if t < SHARED:
            row_cols[...] += own
        else:
            half_cols[...] += own
        acc[0, 0:size] += weight * (k * k)
        acc[1, 0:size] += weight * (l * l)
        acc[2, 0:size] += weight * h

    slot_row = lax.broadcasted_iota(jnp.int32, (8, 256), 0)

    @pl.when(is_k)
    def _():
        acc[...] = jnp.zeros_like(acc)
        row_cols[...] = jnp.zeros_like(row_cols)
        half_cols[...] = jnp.zeros_like(half_cols)
        col_acc[...] = jnp.zeros_like(col_acc)

        product(0)

    for j in range(PIECES):
        rows = piece(j)
        arrived(blocks.at[1, rows, :], gather_recv.at[0, j], f"w1_{j}")
        forward(1, 4, j, 0, 3)
        arrived(blocks.at[2, rows, :], gather_recv.at[1, j], f"w2_{j}")
        forward(2, 5, j, 3, 0)
        pl.when(is_k)(lambda: forward(1, 3, j, 0, 1))
        if j == 6:
            pl.when(is_l)(late_mean)

    @pl.when(is_l)
    def _():
        for j in range(PIECES):
            forward(2, 3, j, 1, 0)

    @pl.when(is_l)
    def _():
        center(1)
        center(2)

    for t in (1, 2, 3):
        product(t)

    @pl.when(is_k)
    def _():
        arrived(means, mean_recv, "w_mean")
        arrived(early_pieces.at[0:3], rows_recv, "w_rows")

    @pl.when(is_l)
    def _():
        arrived(means.at[0:3], mean_recv, "w_mean")
        arrived(early_pieces, rows_recv, "w_rows")

    for c in range(4):
        at = slice(2048 * c, 2048 * (c + 1))
        late_out[:, at] = (late[:, at].astype(F32) - means[c]).astype(BF16)
    low = lax.broadcasted_iota(jnp.int32, (32, 128), 1) < 64
    for u in range(16):
        p = [early_pieces[c, :, 128 * u : 128 * (u + 1)].astype(F32) for c in range(4)]
        turned = [pltpu.roll(v, 64, 1) for v in p]
        for j in range(2):
            first = jnp.where(low, p[2 * j], turned[2 * j + 1])
            second = jnp.where(low, turned[2 * j], p[2 * j + 1])
            early_out[:, 128 * (4 * u + j) : 128 * (4 * u + j + 1)] = first.astype(BF16)
            early_out[:, 128 * (4 * u + 2 + j) : 128 * (4 * u + 3 + j)] = second.astype(BF16)
    put_e = pltpu.make_async_copy(early_out, eout_hbm, out_sem.at[0])
    put_l = pltpu.make_async_copy(late_out, lout_hbm, out_sem.at[1])
    put_e.start()
    put_l.start()

    def take(slot):
        for j in range(PIECES):
            arrived(blocks.at[slot, piece(j), :], gather_recv.at[slot - 1, j], f"w{slot}_{j}")
        pl.when(is_l)(lambda: center(slot))

    take(4)
    product(4)
    take(5)
    product(5)
    product(7)

    @pl.when(is_k)
    def _():
        for t in (0, 1, 2, 3):
            settle(t)

    take(3)
    for t in (6, 8, 9):
        product(t)

    @pl.when(is_k)
    def _():
        for t in (4, 5, 7, 6, 8, 9):
            settle(t)
        turned = jnp.concatenate([row_cols[...]] * 4, axis=0).T
        half_turned = jnp.concatenate([half_cols[...]] * 8, axis=0).T
        col = lax.broadcasted_iota(jnp.int32, (1, 256), 1)
        both = col_acc[...]
        for t in range(len(TILES)):
            a, _, half = sides(t)
            if t < SHARED:
                row = jnp.where(col // 64 == z, turned[t : t + 1, :], 0.0)
            else:
                row = jnp.where(col // 32 == 4 * half + z, half_turned[t : t + 1, :], 0.0)
            both = both + jnp.where(slot_row == a, row, 0.0)
        scal_lane = lax.broadcasted_iota(jnp.int32, (1, 128), 1)
        scal = jnp.zeros((1, 128), F32)
        for j in range(3):
            s = jnp.sum(jnp.sum(acc[j], axis=0, keepdims=True), axis=1, keepdims=True)
            scal = jnp.where(scal_lane == j, s, scal)
        for dx in range(4):
            for dy in range(4):
                r = 4 * dx + dy
                if (dx, dy) in SLOTS:
                    slot = SLOTS.index((dx, dy))
                    msg[r, :, 0:256] = both[slot : slot + 1, :]
                else:
                    msg[r, :, 0:256] = jnp.zeros((1, 256), F32)
                msg[r, :, 256:384] = scal
        for dx in range(4):
            for dy in range(4):
                r = 4 * dx + dy
                if r:
                    send(msg.at[r], msg_in.at[r], msg_send, msg_recv, 2 * chip_at(dx, dy) + K_CORE, z)
        msg_in[0] = msg[0]
        arrived(msg_in.at[0:15], msg_recv, "w_msg")
        s = msg_in[0]
        for r in range(1, 16):
            s = s + msg_in[r]
        total[...] = s
        for dz in (1, 2, 3):
            send(total, total_in.at[dz - 1], total_send, total_recv, k_dev, level(dz))
            send(total, total_in.at[dz - 1], total_send, total_recv, l_dev, level(dz))
        send(total, total_in.at[3], pair_send.at[2], total_recv, l_dev, z)
        total_in[3] = total[...]
        arrived(total_in.at[0:3], total_recv, "w_tot")

    @pl.when(is_l)
    def _():
        arrived(total_in, total_recv, "w_tot")

    final = (total_in[0] + total_in[1]) + (total_in[2] + total_in[3])
    scal_lane = lax.broadcasted_iota(jnp.int32, (1, 128), 1)
    scal = final[:, 256:384]
    kk, ll, kl = (jnp.sum(jnp.where(scal_lane == j, scal, 0.0), axis=1, keepdims=True) for j in range(3))
    norm = jnp.sqrt(kk * ll)
    sim_ref[...] = kl / norm
    half = jnp.where(core == 0, final[:, 0:128], final[:, 128:256])
    tokens = half
    for j in (1, 2, 3):
        tokens = jnp.where(z == j, pltpu.roll(half, 128 - 32 * j, 1), tokens)
    share_ref[...] = (4096.0 * tokens / norm)[:, 0:32]

    with jax.named_scope("end"):
        put_e.wait()
    put_l.wait()
    left(late.at[:, 0:6144], late_send)
    left(cen.at[0:15], early_send)
    left(blocks.at[1:6], gather_send)
    left(parts.at[:, 0:3], part_send)
    left(half_parts.at[:, 0:3], half_send)
    left(parts0.at[0:3], part0_send)

    @pl.when(is_k)
    def _():
        left(late.at[:, 0:2048], pair_send.at[0])
        left(early_pieces.at[0], pair_send.at[1])
        left(total, pair_send.at[2])
        left(blocks.at[0, 0:192, :], rows_send)
        left(msg.at[0:15], msg_send)
        left(msg.at[0:6], total_send)

    @pl.when(is_l)
    def _():
        left(cen.at[0], pair_send.at[0])
        left(mean_out, pair_send.at[1])
        left(parts0.at[0], pair_send.at[2])
        left(parts.at[:, 0], pair_send.at[3])
        left(half_parts.at[:, 0], pair_send.at[4])
        left(plane_sums.at[0:15], sums_send)
        left(plane_sums.at[0:6], mean_send)


def publish(share_in, sim_in, early_in, late_in, share, sim, early, late, bufs, share_buf, sim_buf, in_sem, out_sem):
    ways = (
        (early_in, bufs.at[0], early),
        (late_in, bufs.at[1], late),
        (share_in, share_buf, share),
        (sim_in, sim_buf, sim),
    )
    gets = [pltpu.make_async_copy(a, b, in_sem.at[n]) for n, (a, b, _) in enumerate(ways)]
    puts = [pltpu.make_async_copy(b, c, out_sem.at[n]) for n, (_, b, c) in enumerate(ways)]
    for get in gets:
        get.start()
    for get, put in zip(gets, puts):
        get.wait()
        put.start()
    for put in puts:
        put.wait()


def body(layer_early, layer_late):
    vm = pltpu.VMEM
    dma = pltpu.SemaphoreType.DMA
    hbm = pl.BlockSpec(memory_space=pltpu.HBM)
    whole = pl.BlockSpec(memory_space=pltpu.VMEM)
    share, sim, early_rows, late_rows = pl.pallas_call(
        kernel,
        out_shape=(
            jax.ShapeDtypeStruct((1, 32), F32),
            jax.ShapeDtypeStruct((1, 1), F32),
            jax.ShapeDtypeStruct((32, 8192), BF16),
            jax.ShapeDtypeStruct((32, 8192), BF16),
        ),
        in_specs=[hbm, hbm],
        out_specs=(whole, whole, hbm, hbm),
        scratch_shapes=[
            vm((64, 4096), BF16),
            vm((32, 8192), BF16),
            vm((16, 64, 256), BF16),
            vm((32, 64, 256), BF16),
            vm((12, 256, 2048), BF16),
            vm((10, 256, 256), F32),
            vm((6, 256, 256), BF16),
            vm((6, 7, 64, 256), BF16),
            vm((3, 128, 256), BF16),
            vm((3, 7, 32, 256), BF16),
            vm((7, 64, 256), F32),
            vm((1, 2048), F32),
            vm((16, 1, 2048), F32),
            vm((1, 2048), F32),
            vm((4, 1, 2048), F32),
            vm((4, 32, 2048), BF16),
            vm((32, 8192), BF16),
            vm((32, 8192), BF16),
            vm((3, 64, 256), F32),
            vm((64, 128), F32),
            vm((32, 128), F32),
            vm((8, 256), F32),
            vm((16, 1, 384), F32),
            vm((16, 1, 384), F32),
            vm((1, 384), F32),
            vm((4, 1, 384), F32),
            dma((2,)),
            dma((2,)),
            dma,
            dma((8,)),
            dma,
            dma((4,)),
            dma((5,)),
            dma,
            dma,
            dma,
            dma,
            dma,
            dma((5, PIECES)),
            dma,
            dma,
            dma,
            dma((9,)),
            dma,
            dma,
            dma,
            dma,
            dma,
            dma,
            dma,
        ],
        compiler_params=pltpu.CompilerParams(collective_id=0, has_side_effects=True, vmem_limit_bytes=67043328),
    )(layer_early.T, layer_late)
    share, sim, early_rows, late_rows = pl.pallas_call(
        publish,
        out_shape=(
            jax.ShapeDtypeStruct((1, 32), F32),
            jax.ShapeDtypeStruct((1, 1), F32),
            jax.ShapeDtypeStruct((32, 8192), BF16),
            jax.ShapeDtypeStruct((32, 8192), BF16),
        ),
        in_specs=[hbm] * 4,
        out_specs=(hbm,) * 4,
        scratch_shapes=[
            vm((2, 32, 8192), BF16),
            vm((1, 32), F32),
            vm((1, 1), F32),
            dma((4,)),
            dma((4,)),
        ],
    )(share, sim, early_rows, late_rows)
    return sim.reshape(()), share.reshape(32), early_rows, late_rows


def solution(mesh):
    return jax.shard_map(
        body,
        mesh=mesh,
        in_specs=(P(None, ("gx", "gy")), P(("gx", "gy"), None)),
        out_specs=(P(), P(("gx", "gy")), P(("gx", "gy"), None), P(("gx", "gy"), None)),
        check_vma=False,
    )
```

```python
import jax
import jax.numpy as jnp
from jax import lax
from jax.experimental import pallas as pl
from jax.experimental.pallas import tpu as pltpu
from jax.sharding import PartitionSpec as P

MESH = pl.DeviceIdType.MESH
F32 = jnp.float32
BF16 = jnp.bfloat16

SLOTS = ((0, 0), (1, 0), (0, 1), (1, 1), (1, 3), (3, 1))
TILES = ((0, 0), (1, 0), (2, 0), (1, 2), (4, 2), (5, 1), (3, 0), (4, 5), (3, 5), (3, 4))
SHARED = 7
K_CORE = 1
L_CORE = 0
PIECES = 8
ORDER = ((0, 0), (0, 1), (2, 0), (2, 1), (1, 0), (1, 1), (3, 0), (3, 1))
EVERYONE = sorted(
    [(dx, dy, dz) for dx in range(4) for dy in range(4) for dz in range(4)],
    key=lambda d: -sum(min(v, 4 - v) for v in d),
)
OTHERS = tuple((dx, dy) for dx in (2, 1, 3, 0) for dy in (2, 1, 3, 0) if dx or dy)


def send(src, dst, send_sem, recv_sem, gx, gy):
    pltpu.make_async_remote_copy(
        src_ref=src,
        dst_ref=dst,
        send_sem=send_sem,
        recv_sem=recv_sem,
        device_id=(gx, gy),
        device_id_type=MESH,
    ).start()


def kernel(
    xt_hbm,
    late_hbm,
    share_ref,
    sim_ref,
    eout_hbm,
    lout_hbm,
    xt,
    late,
    cen,
    rt,
    blocks,
    gram,
    stage,
    parts,
    halves,
    half_parts,
    parts0,
    own_sum,
    plane_sums,
    mean_out,
    means,
    early_pieces,
    early_out,
    late_out,
    acc,
    row_cols,
    half_cols,
    col_acc,
    msg,
    msg_in,
    load_sem,
    out_sem,
    late_send,
    late_recv,
    early_send,
    early_recv,
    pair_send,
    sums_send,
    sums_recv,
    mean_send,
    mean_recv,
    gather_send,
    gather_recv,
    rows_send,
    rows_recv,
    part_send,
    part_recv,
    half_send,
    part0_send,
    part0_recv,
    msg_send,
    msg_recv,
):
    gx = lax.axis_index("gx")
    z = lax.axis_index("gy")
    core = lax.rem(gx, 2)
    chip = gx // 2
    x = chip // 4
    y = lax.rem(chip, 4)
    partner = gx + 1 - 2 * core
    k_dev = 2 * chip + K_CORE
    l_dev = 2 * chip + L_CORE
    is_k = core == K_CORE
    is_l = core == L_CORE

    def arrived(ref, sem, name="wait"):
        with jax.named_scope(name):
            pltpu.make_async_remote_copy(
                src_ref=ref, dst_ref=ref, send_sem=sem, recv_sem=sem, device_id=(partner, z), device_id_type=MESH
            ).wait_recv()

    def left(ref, sem):
        pltpu.make_async_remote_copy(
            src_ref=ref, dst_ref=ref, send_sem=sem, recv_sem=sem, device_id=(partner, z), device_id_type=MESH
        ).wait_send()

    def chip_at(dx, dy):
        return lax.rem(x + dx, 4) * 4 + lax.rem(y + dy, 4)

    def level(dz):
        return lax.rem(z + dz, 4)

    load_x = pltpu.make_async_copy(xt_hbm, xt, load_sem.at[0])
    load_y = pltpu.make_async_copy(late_hbm, late, load_sem.at[1])
    load_x.start()
    load_y.start()
    barrier = pltpu.get_barrier_semaphore()

    for dx, dy in OTHERS:
        other = chip_at(dx, dy)
        pl.semaphore_signal(barrier, inc=1, device_id=(2 * other + core, z), device_id_type=MESH)

    @pl.when(is_k)
    def _():
        for dx, dy in OTHERS:
            other = chip_at(dx, dy)
            pl.semaphore_signal(barrier, inc=1, device_id=(2 * other + L_CORE, z), device_id_type=MESH)

    for dz in (1, 2, 3):
        pl.semaphore_signal(barrier, inc=1, device_id=(2 * chip, level(dz)), device_id_type=MESH)
        pl.semaphore_signal(barrier, inc=1, device_id=(2 * chip + 1, level(dz)), device_id_type=MESH)
    pl.semaphore_signal(barrier, inc=1, device_id=(partner, z), device_id_type=MESH)

    with jax.named_scope("load"):
        load_x.wait()

    sums = jnp.zeros((64, 256), F32)
    for u in range(16):
        sums = sums + xt[:, 256 * u : 256 * (u + 1)].astype(F32)
    col_mean = jnp.sum(sums, axis=1, keepdims=True) / 4096.0
    for u in range(16):
        cen[u] = (xt[:, 256 * u : 256 * (u + 1)].astype(F32) - col_mean).astype(BF16)
    load_y.wait()

    with jax.named_scope("barrier"):
        pl.semaphore_wait(barrier, 22 + 15 * (1 - core))

    def piece(j):
        dz, q = ORDER[j]
        return pl.ds(pl.multiple_of(32 * (4 * q + level(dz)), 32), 32)

    my_rows = pl.ds(pl.multiple_of(32 * (4 * core + z), 32), 32)
    for dz in (2, 1, 3):
        to = level(dz)
        send(
            late.at[:, pl.ds(pl.multiple_of(2048 * to, 2048), 2048)],
            blocks.at[0, my_rows, :],
            late_send,
            late_recv.at[2 * (4 - dz) + core],
            l_dev,
            to,
        )
    own_cols = pl.ds(pl.multiple_of(2048 * z, 2048), 2048)

    for dx, dy in OTHERS:
        other = chip_at(dx, dy)
        send(cen.at[other], rt.at[gx], early_send, early_recv.at[x], 2 * other + K_CORE, z)

    def forward(src, dst, j, ex, ey):
        to = 2 * chip_at(4 - ex, 4 - ey) + core
        rows = piece(j)
        send(blocks.at[src, rows, :], blocks.at[dst, rows, :], gather_send, gather_recv.at[dst - 1, j], to, z)

    def start(j):
        forward(0, 1, j, 1, 0)
        forward(0, 2, j, 0, 1)

    @pl.when(is_k)
    def _():
        send(late.at[:, own_cols], blocks.at[0, my_rows, :], pair_send.at[0], late_recv.at[1], l_dev, z)
        rt[gx] = cen[chip]
        for dx in (2, 1, 3, 0):
            xs = lax.rem(x + dx, 4)
            arrived(rt.at[0 : 8 if dx else 7], early_recv.at[xs], f"w_early{dx}")

            @pl.loop(0, 4)
            def _(k):
                u = 4 * xs + k
                cols = jnp.concatenate([rt[2 * u].astype(F32), rt[2 * u + 1].astype(F32)], axis=0)
                at = pl.ds(pl.multiple_of(128 * u, 128), 128)
                blocks[0, :, at] = cols.T.astype(BF16)

        for j in range(PIECES):
            start(j)
        for dz in (1, 2, 3):
            for q in (0, 1):
                rows = pl.ds(pl.multiple_of(32 * (4 * q + level(dz)), 32), 32)
                send(blocks.at[0, rows, :], early_pieces.at[z], rows_send, rows_recv, 2 * chip + q, level(dz))
        rows = pl.ds(pl.multiple_of(32 * (4 * L_CORE + z), 32), 32)
        send(blocks.at[0, rows, :], early_pieces.at[z], pair_send.at[1], rows_recv, l_dev, z)
        early_pieces[z] = blocks[0, my_rows, :]

    @pl.when(is_l)
    def _():
        send(cen.at[chip], rt.at[gx], pair_send.at[0], early_recv.at[x], k_dev, z)
        blocks[0, my_rows, :] = late[:, own_cols]
        for j in range(PIECES):
            if j:
                arrived(blocks.at[0, piece(j), :], late_recv.at[2 * ORDER[j][0] + ORDER[j][1]], f"w_late{j}")
            if j < 6:
                start(j)
        for c in range(4):
            at = slice(512 * c, 512 * (c + 1))
            part = jnp.zeros((32, 512), F32)
            for r in range(8):
                part = part + blocks[0, 32 * r : 32 * (r + 1), at].astype(F32)
            own_sum[:, at] = jnp.sum(part, axis=0, keepdims=True)
        plane_sums[chip] = own_sum[...]

        @pl.loop(1, 16)
        def _(r):
            other = lax.rem(chip + r, 16)
            send(own_sum, plane_sums.at[chip], sums_send, sums_recv, 2 * other + L_CORE, z)

        start(6)
        start(7)

    def center(slot):
        for c in range(4):
            at = slice(512 * c, 512 * (c + 1))
            m = mean_out[:, at]
            for r in range(8):
                rows = slice(32 * r, 32 * (r + 1))
                blocks[6 + slot, rows, at] = (blocks[slot, rows, at].astype(F32) - m).astype(BF16)

    def late_mean():
        arrived(plane_sums.at[0:15], sums_recv, "w_sums")
        mean = plane_sums[0]
        for u in range(1, 16):
            mean = mean + plane_sums[u]
        mean_out[...] = mean / 4096.0
        means[z] = mean_out[...]
        send(mean_out, means.at[z], pair_send.at[1], mean_recv, k_dev, z)
        for dz in (1, 2, 3):
            send(mean_out, means.at[z], mean_send, mean_recv, k_dev, level(dz))
            send(mean_out, means.at[z], mean_send, mean_recv, l_dev, level(dz))
        center(0)
        product(0)

    dims = (((1,), (1,)), ((), ()))

    ready = 6 * (1 - core)

    def sides(t):
        a, b = TILES[t]
        if t < SHARED:
            return a, b, 0
        half = (y if t == 9 else x) // 2
        return a + half * (b - a), b + half * (a - b), half

    def product(t):
        a, b, half = sides(t)
        with jax.named_scope(f"dot{t}"):
            if t < SHARED:
                gram[t] = lax.dot_general(blocks[a + ready], blocks[b + ready], dims, preferred_element_type=F32)
            else:
                top = pl.ds(pl.multiple_of(128 * half, 128), 128)
                gram[t, 0:128, :] = lax.dot_general(
                    blocks[a + ready, top, :], blocks[b + ready], dims, preferred_element_type=F32
                )
        if t == 0:
            src, dst, size, out, into, pair = gram.at[0], parts0, 64, part0_send, part0_recv, 2
        elif t < SHARED:
            src, dst, size, out, into, pair = stage.at[t - 1], parts.at[t - 1], 64, part_send, part_recv.at[t - 1], 3
            stage[t - 1] = gram[t].astype(BF16)
        else:
            n = t - SHARED
            src, dst, size, out, into, pair = halves.at[n], half_parts.at[n], 32, half_send, part_recv.at[t - 1], 4
            halves[n] = gram[t, 0:128, :].astype(BF16)
        for dz in (1, 2, 3):
            to = level(dz)
            rows = pl.ds(pl.multiple_of(size * to, size), size)
            send(src.at[rows, :], dst.at[dz - 1 + 4 * (1 - core)], out, into, k_dev, to)

        @pl.when(is_l)
        def _():
            rows = pl.ds(pl.multiple_of(size * z, size), size)
            send(src.at[rows, :], dst.at[3], pair_send.at[pair], into, k_dev, z)

    def settle(t):
        _, b, _ = sides(t)
        if t == 0:
            size, buf, sem = 64, parts0, part0_recv
        elif t < SHARED:
            size, buf, sem = 64, parts.at[t - 1], part_recv.at[t - 1]
        else:
            size, buf, sem = 32, half_parts.at[t - SHARED], part_recv.at[t - 1]
        arrived(buf, sem, f"wp{t}")
        part = [buf[n].astype(F32) for n in range(7)]
        rows = pl.ds(pl.multiple_of(size * z, size), size)
        k = gram[t, rows, :] + ((part[0] + part[1]) + part[2])
        l = (part[3] + part[4]) + (part[5] + part[6])
        h = k * l
        lane = lax.broadcasted_iota(jnp.int32, (size, 128), 1)
        own = jnp.where(lane == t, jnp.sum(h, axis=1, keepdims=True), 0.0)
        weight = 1.0
        if t:
            weight = 2.0
            across = jnp.sum(h, axis=0, keepdims=True)
            col_acc[...] += jnp.where(slot_row == b, across, 0.0)
        if t < SHARED:
            row_cols[...] += own
        else:
            half_cols[...] += own
        acc[0, 0:size] += weight * (k * k)
        acc[1, 0:size] += weight * (l * l)
        acc[2, 0:size] += weight * h

    slot_row = lax.broadcasted_iota(jnp.int32, (8, 256), 0)

    @pl.when(is_k)
    def _():
        acc[...] = jnp.zeros_like(acc)
        row_cols[...] = jnp.zeros_like(row_cols)
        half_cols[...] = jnp.zeros_like(half_cols)
        col_acc[...] = jnp.zeros_like(col_acc)

        product(0)

    for j in range(PIECES):
        rows = piece(j)
        arrived(blocks.at[1, rows, :], gather_recv.at[0, j], f"w1_{j}")
        forward(1, 4, j, 0, 3)
        arrived(blocks.at[2, rows, :], gather_recv.at[1, j], f"w2_{j}")
        forward(2, 5, j, 3, 0)
        pl.when(is_k)(lambda: forward(1, 3, j, 0, 1))
        if j == 6:
            pl.when(is_l)(late_mean)

    @pl.when(is_l)
    def _():
        for j in range(PIECES):
            forward(2, 3, j, 1, 0)

    @pl.when(is_l)
    def _():
        center(1)
        center(2)

    for t in (1, 2, 3):
        product(t)

    @pl.when(is_k)
    def _():
        arrived(means, mean_recv, "w_mean")
        arrived(early_pieces.at[0:3], rows_recv, "w_rows")

    @pl.when(is_l)
    def _():
        arrived(means.at[0:3], mean_recv, "w_mean")
        arrived(early_pieces, rows_recv, "w_rows")

    for c in range(4):
        at = slice(2048 * c, 2048 * (c + 1))
        late_out[:, at] = (late[:, at].astype(F32) - means[c]).astype(BF16)
    low = lax.broadcasted_iota(jnp.int32, (32, 128), 1) < 64
    for u in range(16):
        p = [early_pieces[c, :, 128 * u : 128 * (u + 1)].astype(F32) for c in range(4)]
        turned = [pltpu.roll(v, 64, 1) for v in p]
        for j in range(2):
            first = jnp.where(low, p[2 * j], turned[2 * j + 1])
            second = jnp.where(low, turned[2 * j], p[2 * j + 1])
            early_out[:, 128 * (4 * u + j) : 128 * (4 * u + j + 1)] = first.astype(BF16)
            early_out[:, 128 * (4 * u + 2 + j) : 128 * (4 * u + 3 + j)] = second.astype(BF16)
    put_e = pltpu.make_async_copy(early_out, eout_hbm, out_sem.at[0])
    put_l = pltpu.make_async_copy(late_out, lout_hbm, out_sem.at[1])
    put_e.start()
    put_l.start()

    def take(slot):
        for j in range(PIECES):
            arrived(blocks.at[slot, piece(j), :], gather_recv.at[slot - 1, j], f"w{slot}_{j}")
        pl.when(is_l)(lambda: center(slot))

    take(4)
    product(4)
    take(5)
    product(5)
    product(7)

    @pl.when(is_k)
    def _():
        for t in (0, 1, 2, 3):
            settle(t)

    take(3)
    for t in (6, 8, 9):
        product(t)

    @pl.when(is_k)
    def _():
        for t in (4, 5, 7, 6, 8, 9):
            settle(t)
        turned = jnp.concatenate([row_cols[...]] * 4, axis=0).T
        half_turned = jnp.concatenate([half_cols[...]] * 8, axis=0).T
        col = lax.broadcasted_iota(jnp.int32, (1, 256), 1)
        both = col_acc[...]
        for t in range(len(TILES)):
            a, _, half = sides(t)
            if t < SHARED:
                row = jnp.where(col // 64 == z, turned[t : t + 1, :], 0.0)
            else:
                row = jnp.where(col // 32 == 4 * half + z, half_turned[t : t + 1, :], 0.0)
            both = both + jnp.where(slot_row == a, row, 0.0)
        scal_lane = lax.broadcasted_iota(jnp.int32, (1, 128), 1)
        scal = jnp.zeros((1, 128), F32)
        for j in range(3):
            s = jnp.sum(jnp.sum(acc[j], axis=0, keepdims=True), axis=1, keepdims=True)
            scal = jnp.where(scal_lane == j, s, scal)
        for dx in range(4):
            for dy in range(4):
                r = 4 * dx + dy
                if (dx, dy) in SLOTS:
                    slot = SLOTS.index((dx, dy))
                    msg[r, :, 0:256] = both[slot : slot + 1, :]
                else:
                    msg[r, :, 0:256] = jnp.zeros((1, 256), F32)
                msg[r, :, 256:384] = scal
        for dx, dy, dz in EVERYONE:
            r = 4 * dx + dy
            there = msg_in.at[16 * dz + r]
            chip_there = 2 * chip_at(dx, dy)
            if dx or dy or dz:
                send(msg.at[r], there, msg_send.at[K_CORE], msg_recv, chip_there + K_CORE, level(dz))
            send(msg.at[r], there, msg_send.at[L_CORE], msg_recv, chip_there + L_CORE, level(dz))
        msg_in[0] = msg[0]
        arrived(msg_in.at[0:63], msg_recv, "w_msg")

    @pl.when(is_l)
    def _():
        arrived(msg_in, msg_recv, "w_msg")

    rows = [msg_in[r] for r in range(64)]
    while len(rows) > 1:
        rows = [a + b for a, b in zip(rows[0::2], rows[1::2])]
    final = rows[0]
    scal_lane = lax.broadcasted_iota(jnp.int32, (1, 128), 1)
    scal = final[:, 256:384]
    kk, ll, kl = (jnp.sum(jnp.where(scal_lane == j, scal, 0.0), axis=1, keepdims=True) for j in range(3))
    norm = jnp.sqrt(kk * ll)
    sim_ref[...] = kl / norm
    half = jnp.where(core == 0, final[:, 0:128], final[:, 128:256])
    tokens = half
    for j in (1, 2, 3):
        tokens = jnp.where(z == j, pltpu.roll(half, 128 - 32 * j, 1), tokens)
    share_ref[...] = (4096.0 * tokens / norm)[:, 0:32]

    with jax.named_scope("end"):
        put_e.wait()
    put_l.wait()
    left(late.at[:, 0:6144], late_send)
    left(cen.at[0:15], early_send)
    left(blocks.at[1:6], gather_send)
    left(parts.at[:, 0:3], part_send)
    left(half_parts.at[:, 0:3], half_send)
    left(parts0.at[0:3], part0_send)

    @pl.when(is_k)
    def _():
        left(late.at[:, 0:2048], pair_send.at[0])
        left(early_pieces.at[0], pair_send.at[1])
        left(blocks.at[0, 0:192, :], rows_send)
        left(msg_in.at[0:63], msg_send.at[K_CORE])
        left(msg_in, msg_send.at[L_CORE])

    @pl.when(is_l)
    def _():
        left(cen.at[0], pair_send.at[0])
        left(mean_out, pair_send.at[1])
        left(parts0.at[0], pair_send.at[2])
        left(parts.at[:, 0], pair_send.at[3])
        left(half_parts.at[:, 0], pair_send.at[4])
        left(plane_sums.at[0:15], sums_send)
        left(plane_sums.at[0:6], mean_send)


def publish(share_in, sim_in, early_in, late_in, share, sim, early, late, bufs, share_buf, sim_buf, in_sem, out_sem):
    ways = (
        (early_in, bufs.at[0], early),
        (late_in, bufs.at[1], late),
        (share_in, share_buf, share),
        (sim_in, sim_buf, sim),
    )
    gets = [pltpu.make_async_copy(a, b, in_sem.at[n]) for n, (a, b, _) in enumerate(ways)]
    puts = [pltpu.make_async_copy(b, c, out_sem.at[n]) for n, (_, b, c) in enumerate(ways)]
    for get in gets:
        get.start()
    for get, put in zip(gets, puts):
        get.wait()
        put.start()
    for put in puts:
        put.wait()


def body(layer_early, layer_late):
    vm = pltpu.VMEM
    dma = pltpu.SemaphoreType.DMA
    hbm = pl.BlockSpec(memory_space=pltpu.HBM)
    whole = pl.BlockSpec(memory_space=pltpu.VMEM)
    share, sim, early_rows, late_rows = pl.pallas_call(
        kernel,
        out_shape=(
            jax.ShapeDtypeStruct((1, 32), F32),
            jax.ShapeDtypeStruct((1, 1), F32),
            jax.ShapeDtypeStruct((32, 8192), BF16),
            jax.ShapeDtypeStruct((32, 8192), BF16),
        ),
        in_specs=[hbm, hbm],
        out_specs=(whole, whole, hbm, hbm),
        scratch_shapes=[
            vm((64, 4096), BF16),
            vm((32, 8192), BF16),
            vm((16, 64, 256), BF16),
            vm((32, 64, 256), BF16),
            vm((12, 256, 2048), BF16),
            vm((10, 256, 256), F32),
            vm((6, 256, 256), BF16),
            vm((6, 7, 64, 256), BF16),
            vm((3, 128, 256), BF16),
            vm((3, 7, 32, 256), BF16),
            vm((7, 64, 256), F32),
            vm((1, 2048), F32),
            vm((16, 1, 2048), F32),
            vm((1, 2048), F32),
            vm((4, 1, 2048), F32),
            vm((4, 32, 2048), BF16),
            vm((32, 8192), BF16),
            vm((32, 8192), BF16),
            vm((3, 64, 256), F32),
            vm((64, 128), F32),
            vm((32, 128), F32),
            vm((8, 256), F32),
            vm((16, 1, 384), F32),
            vm((64, 1, 384), F32),
            dma((2,)),
            dma((2,)),
            dma,
            dma((8,)),
            dma,
            dma((4,)),
            dma((5,)),
            dma,
            dma,
            dma,
            dma,
            dma,
            dma((5, PIECES)),
            dma,
            dma,
            dma,
            dma((9,)),
            dma,
            dma,
            dma,
            dma((2,)),
            dma,
        ],
        compiler_params=pltpu.CompilerParams(collective_id=0, has_side_effects=True, vmem_limit_bytes=67043328),
    )(layer_early.T, layer_late)
    share, sim, early_rows, late_rows = pl.pallas_call(
        publish,
        out_shape=(
            jax.ShapeDtypeStruct((1, 32), F32),
            jax.ShapeDtypeStruct((1, 1), F32),
            jax.ShapeDtypeStruct((32, 8192), BF16),
            jax.ShapeDtypeStruct((32, 8192), BF16),
        ),
        in_specs=[hbm] * 4,
        out_specs=(hbm,) * 4,
        scratch_shapes=[
            vm((2, 32, 8192), BF16),
            vm((1, 32), F32),
            vm((1, 1), F32),
            dma((4,)),
            dma((4,)),
        ],
    )(share, sim, early_rows, late_rows)
    return sim.reshape(()), share.reshape(32), early_rows, late_rows


def solution(mesh):
    return jax.shard_map(
        body,
        mesh=mesh,
        in_specs=(P(None, ("gx", "gy")), P(("gx", "gy"), None)),
        out_specs=(P(), P(("gx", "gy")), P(("gx", "gy"), None), P(("gx", "gy"), None)),
        check_vma=False,
    )
```

```python
import jax
import jax.numpy as jnp
from jax import lax
from jax.experimental import pallas as pl
from jax.experimental.pallas import tpu as pltpu
from jax.sharding import PartitionSpec as P

MESH = pl.DeviceIdType.MESH
F32 = jnp.float32
BF16 = jnp.bfloat16

SLOTS = ((0, 0), (1, 0), (0, 1), (1, 1), (1, 3), (3, 1))
TILES = ((0, 0), (1, 0), (2, 0), (1, 2), (4, 2), (5, 1), (3, 0), (4, 5), (3, 5), (3, 4))
SHARED = 7
K_CORE = 1
L_CORE = 0
PIECES = 8
DETOUR = (2, 3)
ORDER = ((0, 0), (0, 1), (2, 0), (2, 1), (1, 0), (1, 1), (3, 0), (3, 1))
EVERYONE = sorted(
    [(dx, dy, dz) for dx in range(4) for dy in range(4) for dz in range(4)],
    key=lambda d: -sum(min(v, 4 - v) for v in d),
)
OTHERS = tuple((dx, dy) for dx in (2, 1, 3, 0) for dy in (2, 1, 3, 0) if dx or dy)


def send(src, dst, send_sem, recv_sem, gx, gy):
    pltpu.make_async_remote_copy(
        src_ref=src,
        dst_ref=dst,
        send_sem=send_sem,
        recv_sem=recv_sem,
        device_id=(gx, gy),
        device_id_type=MESH,
    ).start()


def kernel(
    xt_hbm,
    late_hbm,
    share_ref,
    sim_ref,
    eout_hbm,
    lout_hbm,
    xt,
    late,
    cen,
    rt,
    blocks,
    gram,
    stage,
    parts,
    halves,
    half_parts,
    parts0,
    own_sum,
    plane_sums,
    mean_out,
    means,
    early_pieces,
    early_out,
    late_out,
    acc,
    row_cols,
    half_cols,
    col_acc,
    msg,
    msg_in,
    load_sem,
    out_sem,
    late_send,
    late_recv,
    early_send,
    early_recv,
    pair_send,
    sums_send,
    sums_recv,
    mean_send,
    mean_recv,
    gather_send,
    gather_recv,
    rows_send,
    rows_recv,
    part_send,
    part_recv,
    half_send,
    part0_send,
    part0_recv,
    msg_send,
    msg_recv,
):
    gx = lax.axis_index("gx")
    z = lax.axis_index("gy")
    core = lax.rem(gx, 2)
    chip = gx // 2
    x = chip // 4
    y = lax.rem(chip, 4)
    partner = gx + 1 - 2 * core
    k_dev = 2 * chip + K_CORE
    l_dev = 2 * chip + L_CORE
    is_k = core == K_CORE
    is_l = core == L_CORE

    def arrived(ref, sem, name="wait"):
        with jax.named_scope(name):
            pltpu.make_async_remote_copy(
                src_ref=ref, dst_ref=ref, send_sem=sem, recv_sem=sem, device_id=(partner, z), device_id_type=MESH
            ).wait_recv()

    def left(ref, sem):
        pltpu.make_async_remote_copy(
            src_ref=ref, dst_ref=ref, send_sem=sem, recv_sem=sem, device_id=(partner, z), device_id_type=MESH
        ).wait_send()

    def chip_at(dx, dy):
        return lax.rem(x + dx, 4) * 4 + lax.rem(y + dy, 4)

    def level(dz):
        return lax.rem(z + dz, 4)

    load_x = pltpu.make_async_copy(xt_hbm, xt, load_sem.at[0])
    load_y = pltpu.make_async_copy(late_hbm, late, load_sem.at[1])
    load_x.start()
    load_y.start()
    barrier = pltpu.get_barrier_semaphore()

    for dx, dy in OTHERS:
        other = chip_at(dx, dy)
        pl.semaphore_signal(barrier, inc=1, device_id=(2 * other + core, z), device_id_type=MESH)

    @pl.when(is_k)
    def _():
        for dx, dy in OTHERS:
            other = chip_at(dx, dy)
            pl.semaphore_signal(barrier, inc=1, device_id=(2 * other + L_CORE, z), device_id_type=MESH)

    for dz in (1, 2, 3):
        pl.semaphore_signal(barrier, inc=1, device_id=(2 * chip, level(dz)), device_id_type=MESH)
        pl.semaphore_signal(barrier, inc=1, device_id=(2 * chip + 1, level(dz)), device_id_type=MESH)
    pl.semaphore_signal(barrier, inc=1, device_id=(partner, z), device_id_type=MESH)

    with jax.named_scope("load"):
        load_x.wait()

    sums = jnp.zeros((64, 256), F32)
    for u in range(16):
        sums = sums + xt[:, 256 * u : 256 * (u + 1)].astype(F32)
    col_mean = jnp.sum(sums, axis=1, keepdims=True) / 4096.0
    for u in range(16):
        cen[u] = (xt[:, 256 * u : 256 * (u + 1)].astype(F32) - col_mean).astype(BF16)
    load_y.wait()

    with jax.named_scope("barrier"):
        pl.semaphore_wait(barrier, 22 + 15 * (1 - core))

    def piece(j):
        dz, q = ORDER[j]
        return pl.ds(pl.multiple_of(32 * (4 * q + level(dz)), 32), 32)

    my_rows = pl.ds(pl.multiple_of(32 * (4 * core + z), 32), 32)
    for dz in (2, 1, 3):
        to = level(dz)
        send(
            late.at[:, pl.ds(pl.multiple_of(2048 * to, 2048), 2048)],
            blocks.at[0, my_rows, :],
            late_send,
            late_recv.at[2 * (4 - dz) + core],
            l_dev,
            to,
        )
    own_cols = pl.ds(pl.multiple_of(2048 * z, 2048), 2048)

    for dx, dy in OTHERS:
        other = chip_at(dx, dy)
        send(cen.at[other], rt.at[gx], early_send, early_recv.at[x], 2 * other + K_CORE, z)

    def forward(src, dst, j, ex, ey):
        to = 2 * chip_at(4 - ex, 4 - ey) + core
        rows = piece(j)
        send(blocks.at[src, rows, :], blocks.at[dst, rows, :], gather_send, gather_recv.at[dst - 1, j], to, z)

    def take(slot, j):
        arrived(blocks.at[slot, piece(j), :], gather_recv.at[slot - 1, j], f"g{slot}_{j}")

    @pl.when(is_k)
    def _():
        send(late.at[:, own_cols], blocks.at[0, my_rows, :], pair_send.at[0], late_recv.at[1], l_dev, z)
        rt[gx] = cen[chip]
        for dx in (2, 1, 3, 0):
            xs = lax.rem(x + dx, 4)
            arrived(rt.at[0 : 8 if dx else 7], early_recv.at[xs], f"w_early{dx}")

            @pl.loop(0, 4)
            def _(k):
                u = 4 * xs + k
                cols = jnp.concatenate([rt[2 * u].astype(F32), rt[2 * u + 1].astype(F32)], axis=0)
                at = pl.ds(pl.multiple_of(128 * u, 128), 128)
                blocks[0, :, at] = cols.T.astype(BF16)

        for j in range(PIECES):
            forward(0, 1, j, 1, 0)
            forward(0, 2, j, 0, 1)
        for dz in (1, 2, 3):
            for q in (0, 1):
                rows = pl.ds(pl.multiple_of(32 * (4 * q + level(dz)), 32), 32)
                send(blocks.at[0, rows, :], early_pieces.at[z], rows_send, rows_recv, 2 * chip + q, level(dz))
        rows = pl.ds(pl.multiple_of(32 * (4 * L_CORE + z), 32), 32)
        send(blocks.at[0, rows, :], early_pieces.at[z], pair_send.at[1], rows_recv, l_dev, z)
        early_pieces[z] = blocks[0, my_rows, :]

    def start(j):
        forward(0, 2, j, 0, 1)
        if j not in DETOUR:
            forward(0, 1, j, 1, 0)

    @pl.when(is_l)
    def _():
        send(cen.at[chip], rt.at[gx], pair_send.at[0], early_recv.at[x], k_dev, z)
        blocks[0, my_rows, :] = late[:, own_cols]
        for j in range(PIECES):
            if j:
                arrived(blocks.at[0, piece(j), :], late_recv.at[2 * ORDER[j][0] + ORDER[j][1]], f"w_late{j}")
            if j < 6:
                start(j)
        for c in range(4):
            at = slice(512 * c, 512 * (c + 1))
            part = jnp.zeros((32, 512), F32)
            for r in range(8):
                part = part + blocks[0, 32 * r : 32 * (r + 1), at].astype(F32)
            own_sum[:, at] = jnp.sum(part, axis=0, keepdims=True)
        plane_sums[chip] = own_sum[...]

        @pl.loop(1, 16)
        def _(r):
            other = lax.rem(chip + r, 16)
            send(own_sum, plane_sums.at[chip], sums_send, sums_recv, 2 * other + L_CORE, z)

        start(6)
        start(7)

    def center(slot):
        for c in range(4):
            at = slice(512 * c, 512 * (c + 1))
            m = mean_out[:, at]
            for r in range(8):
                rows = slice(32 * r, 32 * (r + 1))
                blocks[6 + slot, rows, at] = (blocks[slot, rows, at].astype(F32) - m).astype(BF16)

    def late_mean():
        arrived(plane_sums.at[0:15], sums_recv, "w_sums")
        mean = plane_sums[0]
        for u in range(1, 16):
            mean = mean + plane_sums[u]
        mean_out[...] = mean / 4096.0
        means[z] = mean_out[...]
        send(mean_out, means.at[z], pair_send.at[1], mean_recv, k_dev, z)
        for dz in (1, 2, 3):
            send(mean_out, means.at[z], mean_send, mean_recv, k_dev, level(dz))
            send(mean_out, means.at[z], mean_send, mean_recv, l_dev, level(dz))
        center(0)
        product(0)

    dims = (((1,), (1,)), ((), ()))

    ready = 6 * (1 - core)

    def sides(t):
        a, b = TILES[t]
        if t < SHARED:
            return a, b, 0
        half = (y if t == 9 else x) // 2
        return a + half * (b - a), b + half * (a - b), half

    def product(t):
        a, b, half = sides(t)
        with jax.named_scope(f"dot{t}"):
            if t < SHARED:
                gram[t] = lax.dot_general(blocks[a + ready], blocks[b + ready], dims, preferred_element_type=F32)
            else:
                top = pl.ds(pl.multiple_of(128 * half, 128), 128)
                gram[t, 0:128, :] = lax.dot_general(
                    blocks[a + ready, top, :], blocks[b + ready], dims, preferred_element_type=F32
                )
        if t == 0:
            src, dst, size, out, into, pair = gram.at[0], parts0, 64, part0_send, part0_recv, 2
        elif t < SHARED:
            src, dst, size, out, into, pair = stage.at[t - 1], parts.at[t - 1], 64, part_send, part_recv.at[t - 1], 3
            stage[t - 1] = gram[t].astype(BF16)
        else:
            n = t - SHARED
            src, dst, size, out, into, pair = halves.at[n], half_parts.at[n], 32, half_send, part_recv.at[t - 1], 4
            halves[n] = gram[t, 0:128, :].astype(BF16)
        for dz in (1, 2, 3):
            to = level(dz)
            rows = pl.ds(pl.multiple_of(size * to, size), size)
            send(src.at[rows, :], dst.at[dz - 1 + 4 * (1 - core)], out, into, k_dev, to)

        @pl.when(is_l)
        def _():
            rows = pl.ds(pl.multiple_of(size * z, size), size)
            send(src.at[rows, :], dst.at[3], pair_send.at[pair], into, k_dev, z)

    def settle(t):
        _, b, _ = sides(t)
        if t == 0:
            size, buf, sem = 64, parts0, part0_recv
        elif t < SHARED:
            size, buf, sem = 64, parts.at[t - 1], part_recv.at[t - 1]
        else:
            size, buf, sem = 32, half_parts.at[t - SHARED], part_recv.at[t - 1]
        arrived(buf, sem, f"wp{t}")
        part = [buf[n].astype(F32) for n in range(7)]
        rows = pl.ds(pl.multiple_of(size * z, size), size)
        k = gram[t, rows, :] + ((part[0] + part[1]) + part[2])
        l = (part[3] + part[4]) + (part[5] + part[6])
        h = k * l
        lane = lax.broadcasted_iota(jnp.int32, (size, 128), 1)
        own = jnp.where(lane == t, jnp.sum(h, axis=1, keepdims=True), 0.0)
        weight = 1.0
        if t:
            weight = 2.0
            across = jnp.sum(h, axis=0, keepdims=True)
            col_acc[...] += jnp.where(slot_row == b, across, 0.0)
        if t < SHARED:
            row_cols[...] += own
        else:
            half_cols[...] += own
        acc[0, 0:size] += weight * (k * k)
        acc[1, 0:size] += weight * (l * l)
        acc[2, 0:size] += weight * h

    slot_row = lax.broadcasted_iota(jnp.int32, (8, 256), 0)

    @pl.when(is_k)
    def _():
        acc[...] = jnp.zeros_like(acc)
        row_cols[...] = jnp.zeros_like(row_cols)
        half_cols[...] = jnp.zeros_like(half_cols)
        col_acc[...] = jnp.zeros_like(col_acc)
        product(0)
        for j in range(PIECES):
            take(1, j)
            forward(1, 4, j, 0, 3)
            if j % 2 == 0:
                forward(1, 3, j, 0, 1)
            take(2, j)
            forward(2, 5, j, 3, 0)
            if j % 2:
                forward(2, 3, j, 1, 0)

    @pl.when(is_l)
    def _():
        def from_1(j):
            take(1, j)
            forward(1, 4, j, 0, 3)

        def from_2(j):
            take(2, j)
            forward(2, 5, j, 3, 0)
            if j in DETOUR:
                forward(2, 3, j, 1, 0)

        def from_3(j):
            take(3, j)
            forward(3, 1, j, 0, 3)

        for near, far in ((0, 0), (1, 1), (4, 2), (5, 3), (6, 4), (7, 5)):
            from_1(near)
            from_2(far)
        from_3(DETOUR[0])
        from_2(6)
        late_mean()
        from_3(DETOUR[1])
        from_2(7)
        for j in range(PIECES):
            if j in DETOUR:
                continue
            if j in (4, 5, 6):
                forward(2, 3, j, 1, 0)
            else:
                forward(1, 3, j, 0, 1)
        for j in DETOUR:
            from_1(j)

    @pl.when(is_l)
    def _():
        center(1)
        center(2)

    for t in (1, 2, 3):
        product(t)

    @pl.when(is_k)
    def _():
        arrived(means, mean_recv, "w_mean")
        arrived(early_pieces.at[0:3], rows_recv, "w_rows")

    @pl.when(is_l)
    def _():
        arrived(means.at[0:3], mean_recv, "w_mean")
        arrived(early_pieces, rows_recv, "w_rows")

    for c in range(4):
        at = slice(2048 * c, 2048 * (c + 1))
        late_out[:, at] = (late[:, at].astype(F32) - means[c]).astype(BF16)
    low = lax.broadcasted_iota(jnp.int32, (32, 128), 1) < 64
    for u in range(16):
        p = [early_pieces[c, :, 128 * u : 128 * (u + 1)].astype(F32) for c in range(4)]
        turned = [pltpu.roll(v, 64, 1) for v in p]
        for j in range(2):
            first = jnp.where(low, p[2 * j], turned[2 * j + 1])
            second = jnp.where(low, turned[2 * j], p[2 * j + 1])
            early_out[:, 128 * (4 * u + j) : 128 * (4 * u + j + 1)] = first.astype(BF16)
            early_out[:, 128 * (4 * u + 2 + j) : 128 * (4 * u + 3 + j)] = second.astype(BF16)
    put_e = pltpu.make_async_copy(early_out, eout_hbm, out_sem.at[0])
    put_l = pltpu.make_async_copy(late_out, lout_hbm, out_sem.at[1])
    put_e.start()
    put_l.start()

    for slot in (4, 5):
        for j in range(PIECES):
            take(slot, j)
        pl.when(is_l)(lambda: center(slot))
        product(slot)
    product(7)

    @pl.when(is_k)
    def _():
        for t in (0, 1, 2, 3):
            settle(t)

    for j in range(PIECES):
        if j in DETOUR:
            pl.when(is_k)(lambda: take(3, j))
        else:
            take(3, j)
    pl.when(is_l)(lambda: center(3))
    for t in (6, 8, 9):
        product(t)

    @pl.when(is_k)
    def _():
        for t in (4, 5, 7, 6, 8, 9):
            settle(t)
        turned = jnp.concatenate([row_cols[...]] * 4, axis=0).T
        half_turned = jnp.concatenate([half_cols[...]] * 8, axis=0).T
        col = lax.broadcasted_iota(jnp.int32, (1, 256), 1)
        both = col_acc[...]
        for t in range(len(TILES)):
            a, _, half = sides(t)
            if t < SHARED:
                row = jnp.where(col // 64 == z, turned[t : t + 1, :], 0.0)
            else:
                row = jnp.where(col // 32 == 4 * half + z, half_turned[t : t + 1, :], 0.0)
            both = both + jnp.where(slot_row == a, row, 0.0)
        scal_lane = lax.broadcasted_iota(jnp.int32, (1, 128), 1)
        scal = jnp.zeros((1, 128), F32)
        for j in range(3):
            s = jnp.sum(jnp.sum(acc[j], axis=0, keepdims=True), axis=1, keepdims=True)
            scal = jnp.where(scal_lane == j, s, scal)
        for dx in range(4):
            for dy in range(4):
                r = 4 * dx + dy
                if (dx, dy) in SLOTS:
                    slot = SLOTS.index((dx, dy))
                    msg[r, :, 0:256] = both[slot : slot + 1, :]
                else:
                    msg[r, :, 0:256] = jnp.zeros((1, 256), F32)
                msg[r, :, 256:384] = scal
        for dx, dy, dz in EVERYONE:
            r = 4 * dx + dy
            there = msg_in.at[16 * dz + r]
            chip_there = 2 * chip_at(dx, dy)
            if dx or dy or dz:
                send(msg.at[r], there, msg_send.at[K_CORE], msg_recv, chip_there + K_CORE, level(dz))
            send(msg.at[r], there, msg_send.at[L_CORE], msg_recv, chip_there + L_CORE, level(dz))
        msg_in[0] = msg[0]
        arrived(msg_in.at[0:63], msg_recv, "w_msg")

    @pl.when(is_l)
    def _():
        arrived(msg_in, msg_recv, "w_msg")

    rows = [msg_in[r] for r in range(64)]
    while len(rows) > 1:
        rows = [a + b for a, b in zip(rows[0::2], rows[1::2])]
    final = rows[0]
    scal_lane = lax.broadcasted_iota(jnp.int32, (1, 128), 1)
    scal = final[:, 256:384]
    kk, ll, kl = (jnp.sum(jnp.where(scal_lane == j, scal, 0.0), axis=1, keepdims=True) for j in range(3))
    norm = jnp.sqrt(kk * ll)
    sim_ref[...] = kl / norm
    half = jnp.where(core == 0, final[:, 0:128], final[:, 128:256])
    tokens = half
    for j in (1, 2, 3):
        tokens = jnp.where(z == j, pltpu.roll(half, 128 - 32 * j, 1), tokens)
    share_ref[...] = (4096.0 * tokens / norm)[:, 0:32]

    with jax.named_scope("end"):
        put_e.wait()
    put_l.wait()
    left(late.at[:, 0:6144], late_send)
    left(cen.at[0:15], early_send)
    left(blocks.at[1:6], gather_send)
    left(parts.at[:, 0:3], part_send)
    left(half_parts.at[:, 0:3], half_send)
    left(parts0.at[0:3], part0_send)

    @pl.when(is_k)
    def _():
        left(late.at[:, 0:2048], pair_send.at[0])
        left(early_pieces.at[0], pair_send.at[1])
        left(blocks.at[0, 0:192, :], rows_send)
        left(msg_in.at[0:63], msg_send.at[K_CORE])
        left(msg_in, msg_send.at[L_CORE])

    @pl.when(is_l)
    def _():
        left(cen.at[0], pair_send.at[0])
        left(mean_out, pair_send.at[1])
        left(parts0.at[0], pair_send.at[2])
        left(parts.at[:, 0], pair_send.at[3])
        left(half_parts.at[:, 0], pair_send.at[4])
        left(plane_sums.at[0:15], sums_send)
        left(plane_sums.at[0:6], mean_send)


def publish(share_in, sim_in, early_in, late_in, share, sim, early, late, bufs, share_buf, sim_buf, in_sem, out_sem):
    ways = (
        (early_in, bufs.at[0], early),
        (late_in, bufs.at[1], late),
        (share_in, share_buf, share),
        (sim_in, sim_buf, sim),
    )
    gets = [pltpu.make_async_copy(a, b, in_sem.at[n]) for n, (a, b, _) in enumerate(ways)]
    puts = [pltpu.make_async_copy(b, c, out_sem.at[n]) for n, (_, b, c) in enumerate(ways)]
    for get in gets:
        get.start()
    for get, put in zip(gets, puts):
        get.wait()
        put.start()
    for put in puts:
        put.wait()


def body(layer_early, layer_late):
    vm = pltpu.VMEM
    dma = pltpu.SemaphoreType.DMA
    hbm = pl.BlockSpec(memory_space=pltpu.HBM)
    whole = pl.BlockSpec(memory_space=pltpu.VMEM)
    share, sim, early_rows, late_rows = pl.pallas_call(
        kernel,
        out_shape=(
            jax.ShapeDtypeStruct((1, 32), F32),
            jax.ShapeDtypeStruct((1, 1), F32),
            jax.ShapeDtypeStruct((32, 8192), BF16),
            jax.ShapeDtypeStruct((32, 8192), BF16),
        ),
        in_specs=[hbm, hbm],
        out_specs=(whole, whole, hbm, hbm),
        scratch_shapes=[
            vm((64, 4096), BF16),
            vm((32, 8192), BF16),
            vm((16, 64, 256), BF16),
            vm((32, 64, 256), BF16),
            vm((12, 256, 2048), BF16),
            vm((10, 256, 256), F32),
            vm((6, 256, 256), BF16),
            vm((6, 7, 64, 256), BF16),
            vm((3, 128, 256), BF16),
            vm((3, 7, 32, 256), BF16),
            vm((7, 64, 256), F32),
            vm((1, 2048), F32),
            vm((16, 1, 2048), F32),
            vm((1, 2048), F32),
            vm((4, 1, 2048), F32),
            vm((4, 32, 2048), BF16),
            vm((32, 8192), BF16),
            vm((32, 8192), BF16),
            vm((3, 64, 256), F32),
            vm((64, 128), F32),
            vm((32, 128), F32),
            vm((8, 256), F32),
            vm((16, 1, 384), F32),
            vm((64, 1, 384), F32),
            dma((2,)),
            dma((2,)),
            dma,
            dma((8,)),
            dma,
            dma((4,)),
            dma((5,)),
            dma,
            dma,
            dma,
            dma,
            dma,
            dma((5, PIECES)),
            dma,
            dma,
            dma,
            dma((9,)),
            dma,
            dma,
            dma,
            dma((2,)),
            dma,
        ],
        compiler_params=pltpu.CompilerParams(collective_id=0, has_side_effects=True, vmem_limit_bytes=67043328),
    )(layer_early.T, layer_late)
    share, sim, early_rows, late_rows = pl.pallas_call(
        publish,
        out_shape=(
            jax.ShapeDtypeStruct((1, 32), F32),
            jax.ShapeDtypeStruct((1, 1), F32),
            jax.ShapeDtypeStruct((32, 8192), BF16),
            jax.ShapeDtypeStruct((32, 8192), BF16),
        ),
        in_specs=[hbm] * 4,
        out_specs=(hbm,) * 4,
        scratch_shapes=[
            vm((2, 32, 8192), BF16),
            vm((1, 32), F32),
            vm((1, 1), F32),
            dma((4,)),
            dma((4,)),
        ],
    )(share, sim, early_rows, late_rows)
    return sim.reshape(()), share.reshape(32), early_rows, late_rows


def solution(mesh):
    return jax.shard_map(
        body,
        mesh=mesh,
        in_specs=(P(None, ("gx", "gy")), P(("gx", "gy"), None)),
        out_specs=(P(), P(("gx", "gy")), P(("gx", "gy"), None), P(("gx", "gy"), None)),
        check_vma=False,
    )
```

```python
import jax
import jax.numpy as jnp
from jax import lax
from jax.experimental import pallas as pl
from jax.experimental.pallas import tpu as pltpu
from jax.sharding import PartitionSpec as P

MESH = pl.DeviceIdType.MESH
F32 = jnp.float32
BF16 = jnp.bfloat16

SLOTS = ((0, 0), (1, 0), (0, 1), (1, 1), (1, 3), (3, 1))
TILES = ((0, 0), (1, 0), (2, 0), (1, 2), (4, 2), (5, 1), (3, 0), (4, 5), (3, 5), (3, 4))
SHARED = 7
K_CORE = 1
L_CORE = 0
PIECES = 8
DETOUR = (2, 3)
ORDER = ((0, 0), (0, 1), (2, 0), (2, 1), (1, 0), (1, 1), (3, 0), (3, 1))
EVERYONE = sorted(
    [(dx, dy, dz) for dx in range(4) for dy in range(4) for dz in range(4)],
    key=lambda d: -sum(min(v, 4 - v) for v in d),
)
OTHERS = tuple((dx, dy) for dx in (2, 1, 3, 0) for dy in (2, 1, 3, 0) if dx or dy)


def send(src, dst, send_sem, recv_sem, gx, gy):
    pltpu.make_async_remote_copy(
        src_ref=src,
        dst_ref=dst,
        send_sem=send_sem,
        recv_sem=recv_sem,
        device_id=(gx, gy),
        device_id_type=MESH,
    ).start()


def kernel(
    xt_hbm,
    late_hbm,
    share_ref,
    sim_ref,
    eout_hbm,
    lout_hbm,
    xt,
    late,
    cen,
    rt,
    blocks,
    gram,
    stage,
    parts,
    halves,
    half_parts,
    parts0,
    own_sum,
    plane_sums,
    mean_out,
    means,
    early_pieces,
    early_out,
    late_out,
    acc,
    row_cols,
    half_cols,
    col_acc,
    msg,
    msg_in,
    load_sem,
    out_sem,
    late_send,
    late_recv,
    early_send,
    early_recv,
    pair_send,
    sums_send,
    sums_recv,
    mean_send,
    mean_recv,
    gather_send,
    gather_recv,
    rows_send,
    rows_recv,
    part_send,
    part_recv,
    half_send,
    part0_send,
    part0_recv,
    msg_send,
    msg_recv,
):
    gx = lax.axis_index("gx")
    z = lax.axis_index("gy")
    core = lax.rem(gx, 2)
    chip = gx // 2
    x = chip // 4
    y = lax.rem(chip, 4)
    partner = gx + 1 - 2 * core
    k_dev = 2 * chip + K_CORE
    l_dev = 2 * chip + L_CORE
    is_k = core == K_CORE
    is_l = core == L_CORE

    def arrived(ref, sem, name="wait"):
        with jax.named_scope(name):
            pltpu.make_async_remote_copy(
                src_ref=ref, dst_ref=ref, send_sem=sem, recv_sem=sem, device_id=(partner, z), device_id_type=MESH
            ).wait_recv()

    def left(ref, sem):
        pltpu.make_async_remote_copy(
            src_ref=ref, dst_ref=ref, send_sem=sem, recv_sem=sem, device_id=(partner, z), device_id_type=MESH
        ).wait_send()

    def chip_at(dx, dy):
        return lax.rem(x + dx, 4) * 4 + lax.rem(y + dy, 4)

    def level(dz):
        return lax.rem(z + dz, 4)

    load_x = pltpu.make_async_copy(xt_hbm, xt, load_sem.at[0])
    load_y = pltpu.make_async_copy(late_hbm, late, load_sem.at[1])
    load_x.start()
    load_y.start()
    barrier = pltpu.get_barrier_semaphore()

    for dx, dy in OTHERS:
        other = chip_at(dx, dy)
        pl.semaphore_signal(barrier, inc=1, device_id=(2 * other + core, z), device_id_type=MESH)

    @pl.when(is_k)
    def _():
        for dx, dy in OTHERS:
            other = chip_at(dx, dy)
            pl.semaphore_signal(barrier, inc=1, device_id=(2 * other + L_CORE, z), device_id_type=MESH)

    for dz in (1, 2, 3):
        pl.semaphore_signal(barrier, inc=1, device_id=(2 * chip, level(dz)), device_id_type=MESH)
        pl.semaphore_signal(barrier, inc=1, device_id=(2 * chip + 1, level(dz)), device_id_type=MESH)
    pl.semaphore_signal(barrier, inc=1, device_id=(partner, z), device_id_type=MESH)

    with jax.named_scope("load"):
        load_x.wait()

    sums = jnp.zeros((64, 256), F32)
    for u in range(16):
        sums = sums + xt[:, 256 * u : 256 * (u + 1)].astype(F32)
    col_mean = jnp.sum(sums, axis=1, keepdims=True) / 4096.0
    for u in range(16):
        cen[u] = (xt[:, 256 * u : 256 * (u + 1)].astype(F32) - col_mean).astype(BF16)
    load_y.wait()

    with jax.named_scope("barrier"):
        pl.semaphore_wait(barrier, 22 + 15 * (1 - core))

    def piece(j):
        dz, q = ORDER[j]
        return pl.ds(pl.multiple_of(32 * (4 * q + level(dz)), 32), 32)

    my_rows = pl.ds(pl.multiple_of(32 * (4 * core + z), 32), 32)
    for dz in (2, 1, 3):
        to = level(dz)
        send(
            late.at[:, pl.ds(pl.multiple_of(2048 * to, 2048), 2048)],
            blocks.at[0, my_rows, :],
            late_send,
            late_recv.at[2 * (4 - dz) + core],
            l_dev,
            to,
        )
    own_cols = pl.ds(pl.multiple_of(2048 * z, 2048), 2048)

    for dx, dy in OTHERS:
        other = chip_at(dx, dy)
        send(cen.at[other], rt.at[gx], early_send, early_recv.at[x], 2 * other + K_CORE, z)

    def forward(src, dst, j, ex, ey):
        to = 2 * chip_at(4 - ex, 4 - ey) + core
        rows = piece(j)
        send(blocks.at[src, rows, :], blocks.at[dst, rows, :], gather_send, gather_recv.at[dst - 1, j], to, z)

    def take(slot, j):
        arrived(blocks.at[slot, piece(j), :], gather_recv.at[slot - 1, j], f"g{slot}_{j}")

    @pl.when(is_k)
    def _():
        send(late.at[:, own_cols], blocks.at[0, my_rows, :], pair_send.at[0], late_recv.at[1], l_dev, z)
        rt[gx] = cen[chip]
        for dx in (2, 1, 3, 0):
            xs = lax.rem(x + dx, 4)
            arrived(rt.at[0 : 8 if dx else 7], early_recv.at[xs], f"w_early{dx}")

            @pl.loop(0, 4)
            def _(k):
                u = 4 * xs + k
                cols = jnp.concatenate([rt[2 * u].astype(F32), rt[2 * u + 1].astype(F32)], axis=0)
                at = pl.ds(pl.multiple_of(128 * u, 128), 128)
                blocks[0, :, at] = cols.T.astype(BF16)

        for j in range(PIECES):
            forward(0, 1, j, 1, 0)
            forward(0, 2, j, 0, 1)
        for dz in (1, 2, 3):
            for q in (0, 1):
                rows = pl.ds(pl.multiple_of(32 * (4 * q + level(dz)), 32), 32)
                send(blocks.at[0, rows, :], early_pieces.at[z], rows_send, rows_recv, 2 * chip + q, level(dz))
        rows = pl.ds(pl.multiple_of(32 * (4 * L_CORE + z), 32), 32)
        send(blocks.at[0, rows, :], early_pieces.at[z], pair_send.at[1], rows_recv, l_dev, z)
        early_pieces[z] = blocks[0, my_rows, :]

    def start(j):
        if j != DETOUR[1]:
            forward(0, 2, j, 0, 1)
        if j != DETOUR[0]:
            forward(0, 1, j, 1, 0)

    @pl.when(is_l)
    def _():
        send(cen.at[chip], rt.at[gx], pair_send.at[0], early_recv.at[x], k_dev, z)
        blocks[0, my_rows, :] = late[:, own_cols]
        for j in range(PIECES):
            if j:
                arrived(blocks.at[0, piece(j), :], late_recv.at[2 * ORDER[j][0] + ORDER[j][1]], f"w_late{j}")
            if j < 6:
                start(j)
        for c in range(4):
            at = slice(512 * c, 512 * (c + 1))
            part = jnp.zeros((32, 512), F32)
            for r in range(8):
                part = part + blocks[0, 32 * r : 32 * (r + 1), at].astype(F32)
            own_sum[:, at] = jnp.sum(part, axis=0, keepdims=True)
        plane_sums[chip] = own_sum[...]

        @pl.loop(1, 16)
        def _(r):
            other = lax.rem(chip + r, 16)
            send(own_sum, plane_sums.at[chip], sums_send, sums_recv, 2 * other + L_CORE, z)

        start(6)
        start(7)

    def center(slot):
        for c in range(4):
            at = slice(512 * c, 512 * (c + 1))
            m = mean_out[:, at]
            for r in range(8):
                rows = slice(32 * r, 32 * (r + 1))
                blocks[6 + slot, rows, at] = (blocks[slot, rows, at].astype(F32) - m).astype(BF16)

    def late_mean():
        arrived(plane_sums.at[0:15], sums_recv, "w_sums")
        mean = plane_sums[0]
        for u in range(1, 16):
            mean = mean + plane_sums[u]
        mean_out[...] = mean / 4096.0
        means[z] = mean_out[...]
        send(mean_out, means.at[z], pair_send.at[1], mean_recv, k_dev, z)
        for dz in (1, 2, 3):
            send(mean_out, means.at[z], mean_send, mean_recv, k_dev, level(dz))
            send(mean_out, means.at[z], mean_send, mean_recv, l_dev, level(dz))
        center(0)
        product(0)

    dims = (((1,), (1,)), ((), ()))

    ready = 6 * (1 - core)

    def sides(t):
        a, b = TILES[t]
        if t < SHARED:
            return a, b, 0
        half = (y if t == 9 else x) // 2
        return a + half * (b - a), b + half * (a - b), half

    def product(t):
        a, b, half = sides(t)
        with jax.named_scope(f"dot{t}"):
            if t < SHARED:
                gram[t] = lax.dot_general(blocks[a + ready], blocks[b + ready], dims, preferred_element_type=F32)
            else:
                top = pl.ds(pl.multiple_of(128 * half, 128), 128)
                gram[t, 0:128, :] = lax.dot_general(
                    blocks[a + ready, top, :], blocks[b + ready], dims, preferred_element_type=F32
                )
        if t == 0:
            src, dst, size, out, into, pair = gram.at[0], parts0, 64, part0_send, part0_recv, 2
        elif t < SHARED:
            src, dst, size, out, into, pair = stage.at[t - 1], parts.at[t - 1], 64, part_send, part_recv.at[t - 1], 3
            stage[t - 1] = gram[t].astype(BF16)
        else:
            n = t - SHARED
            src, dst, size, out, into, pair = halves.at[n], half_parts.at[n], 32, half_send, part_recv.at[t - 1], 4
            halves[n] = gram[t, 0:128, :].astype(BF16)
        for dz in (1, 2, 3):
            to = level(dz)
            rows = pl.ds(pl.multiple_of(size * to, size), size)
            send(src.at[rows, :], dst.at[dz - 1 + 4 * (1 - core)], out, into, k_dev, to)

        @pl.when(is_l)
        def _():
            rows = pl.ds(pl.multiple_of(size * z, size), size)
            send(src.at[rows, :], dst.at[3], pair_send.at[pair], into, k_dev, z)

    def settle(t):
        _, b, _ = sides(t)
        if t == 0:
            size, buf, sem = 64, parts0, part0_recv
        elif t < SHARED:
            size, buf, sem = 64, parts.at[t - 1], part_recv.at[t - 1]
        else:
            size, buf, sem = 32, half_parts.at[t - SHARED], part_recv.at[t - 1]
        arrived(buf, sem, f"wp{t}")
        part = [buf[n].astype(F32) for n in range(7)]
        rows = pl.ds(pl.multiple_of(size * z, size), size)
        k = gram[t, rows, :] + ((part[0] + part[1]) + part[2])
        l = (part[3] + part[4]) + (part[5] + part[6])
        h = k * l
        lane = lax.broadcasted_iota(jnp.int32, (size, 128), 1)
        own = jnp.where(lane == t, jnp.sum(h, axis=1, keepdims=True), 0.0)
        weight = 1.0
        if t:
            weight = 2.0
            across = jnp.sum(h, axis=0, keepdims=True)
            col_acc[...] += jnp.where(slot_row == b, across, 0.0)
        if t < SHARED:
            row_cols[...] += own
        else:
            half_cols[...] += own
        acc[0, 0:size] += weight * (k * k)
        acc[1, 0:size] += weight * (l * l)
        acc[2, 0:size] += weight * h

    slot_row = lax.broadcasted_iota(jnp.int32, (8, 256), 0)

    @pl.when(is_k)
    def _():
        acc[...] = jnp.zeros_like(acc)
        row_cols[...] = jnp.zeros_like(row_cols)
        half_cols[...] = jnp.zeros_like(half_cols)
        col_acc[...] = jnp.zeros_like(col_acc)
        product(0)
        for j in range(PIECES):
            take(1, j)
            forward(1, 4, j, 0, 3)
            if j % 2 == 0:
                forward(1, 3, j, 0, 1)
            take(2, j)
            forward(2, 5, j, 3, 0)
            if j % 2:
                forward(2, 3, j, 1, 0)

    @pl.when(is_l)
    def _():
        def from_1(j):
            take(1, j)
            forward(1, 4, j, 0, 3)
            if j == DETOUR[1]:
                forward(1, 3, j, 0, 1)

        def from_2(j):
            take(2, j)
            forward(2, 5, j, 3, 0)
            if j == DETOUR[0]:
                forward(2, 3, j, 1, 0)

        for near, far in ((0, 0), (1, 1), (3, 2), (4, 4), (5, 5), (6, 6), (7, 7)):
            from_1(near)
            from_2(far)
        for j in (0, 1, 4):
            forward(1, 3, j, 0, 1)
        for j in (5, 6, 7):
            forward(2, 3, j, 1, 0)
        take(3, DETOUR[0])
        forward(3, 1, DETOUR[0], 0, 3)
        take(3, DETOUR[1])
        forward(3, 2, DETOUR[1], 3, 0)
        late_mean()
        from_2(DETOUR[1])
        from_1(DETOUR[0])

    @pl.when(is_l)
    def _():
        center(1)
        center(2)

    for t in (1, 2, 3):
        product(t)

    @pl.when(is_k)
    def _():
        arrived(means, mean_recv, "w_mean")
        arrived(early_pieces.at[0:3], rows_recv, "w_rows")

    @pl.when(is_l)
    def _():
        arrived(means.at[0:3], mean_recv, "w_mean")
        arrived(early_pieces, rows_recv, "w_rows")

    for c in range(4):
        at = slice(2048 * c, 2048 * (c + 1))
        late_out[:, at] = (late[:, at].astype(F32) - means[c]).astype(BF16)
    low = lax.broadcasted_iota(jnp.int32, (32, 128), 1) < 64
    for u in range(16):
        p = [early_pieces[c, :, 128 * u : 128 * (u + 1)].astype(F32) for c in range(4)]
        turned = [pltpu.roll(v, 64, 1) for v in p]
        for j in range(2):
            first = jnp.where(low, p[2 * j], turned[2 * j + 1])
            second = jnp.where(low, turned[2 * j], p[2 * j + 1])
            early_out[:, 128 * (4 * u + j) : 128 * (4 * u + j + 1)] = first.astype(BF16)
            early_out[:, 128 * (4 * u + 2 + j) : 128 * (4 * u + 3 + j)] = second.astype(BF16)
    put_e = pltpu.make_async_copy(early_out, eout_hbm, out_sem.at[0])
    put_l = pltpu.make_async_copy(late_out, lout_hbm, out_sem.at[1])
    put_e.start()
    put_l.start()

    for slot in (4, 5):
        for j in range(PIECES):
            take(slot, j)
        pl.when(is_l)(lambda: center(slot))
        product(slot)
    product(7)

    @pl.when(is_k)
    def _():
        for t in (0, 1, 2, 3):
            settle(t)

    for j in range(PIECES):
        if j in DETOUR:
            pl.when(is_k)(lambda: take(3, j))
        else:
            take(3, j)
    pl.when(is_l)(lambda: center(3))
    for t in (6, 8, 9):
        product(t)

    @pl.when(is_k)
    def _():
        for t in (4, 5, 7, 6, 8, 9):
            settle(t)
        turned = jnp.concatenate([row_cols[...]] * 4, axis=0).T
        half_turned = jnp.concatenate([half_cols[...]] * 8, axis=0).T
        col = lax.broadcasted_iota(jnp.int32, (1, 256), 1)
        both = col_acc[...]
        for t in range(len(TILES)):
            a, _, half = sides(t)
            if t < SHARED:
                row = jnp.where(col // 64 == z, turned[t : t + 1, :], 0.0)
            else:
                row = jnp.where(col // 32 == 4 * half + z, half_turned[t : t + 1, :], 0.0)
            both = both + jnp.where(slot_row == a, row, 0.0)
        scal_lane = lax.broadcasted_iota(jnp.int32, (1, 128), 1)
        scal = jnp.zeros((1, 128), F32)
        for j in range(3):
            s = jnp.sum(jnp.sum(acc[j], axis=0, keepdims=True), axis=1, keepdims=True)
            scal = jnp.where(scal_lane == j, s, scal)
        for dx in range(4):
            for dy in range(4):
                r = 4 * dx + dy
                if (dx, dy) in SLOTS:
                    slot = SLOTS.index((dx, dy))
                    msg[r, :, 0:256] = both[slot : slot + 1, :]
                else:
                    msg[r, :, 0:256] = jnp.zeros((1, 256), F32)
                msg[r, :, 256:384] = scal
        for dx, dy, dz in EVERYONE:
            r = 4 * dx + dy
            there = msg_in.at[16 * dz + r]
            chip_there = 2 * chip_at(dx, dy)
            if dx or dy or dz:
                send(msg.at[r], there, msg_send.at[K_CORE], msg_recv, chip_there + K_CORE, level(dz))
            send(msg.at[r], there, msg_send.at[L_CORE], msg_recv, chip_there + L_CORE, level(dz))
        msg_in[0] = msg[0]
        arrived(msg_in.at[0:63], msg_recv, "w_msg")

    @pl.when(is_l)
    def _():
        arrived(msg_in, msg_recv, "w_msg")

    rows = [msg_in[r] for r in range(64)]
    while len(rows) > 1:
        rows = [a + b for a, b in zip(rows[0::2], rows[1::2])]
    final = rows[0]
    scal_lane = lax.broadcasted_iota(jnp.int32, (1, 128), 1)
    scal = final[:, 256:384]
    kk, ll, kl = (jnp.sum(jnp.where(scal_lane == j, scal, 0.0), axis=1, keepdims=True) for j in range(3))
    norm = jnp.sqrt(kk * ll)
    sim_ref[...] = kl / norm
    half = jnp.where(core == 0, final[:, 0:128], final[:, 128:256])
    tokens = half
    for j in (1, 2, 3):
        tokens = jnp.where(z == j, pltpu.roll(half, 128 - 32 * j, 1), tokens)
    share_ref[...] = (4096.0 * tokens / norm)[:, 0:32]

    with jax.named_scope("end"):
        put_e.wait()
    put_l.wait()
    left(late.at[:, 0:6144], late_send)
    left(cen.at[0:15], early_send)
    left(blocks.at[1:6], gather_send)
    left(parts.at[:, 0:3], part_send)
    left(half_parts.at[:, 0:3], half_send)
    left(parts0.at[0:3], part0_send)

    @pl.when(is_k)
    def _():
        left(late.at[:, 0:2048], pair_send.at[0])
        left(early_pieces.at[0], pair_send.at[1])
        left(blocks.at[0, 0:192, :], rows_send)
        left(msg_in.at[0:63], msg_send.at[K_CORE])
        left(msg_in, msg_send.at[L_CORE])

    @pl.when(is_l)
    def _():
        left(cen.at[0], pair_send.at[0])
        left(mean_out, pair_send.at[1])
        left(parts0.at[0], pair_send.at[2])
        left(parts.at[:, 0], pair_send.at[3])
        left(half_parts.at[:, 0], pair_send.at[4])
        left(plane_sums.at[0:15], sums_send)
        left(plane_sums.at[0:6], mean_send)


def publish(share_in, sim_in, early_in, late_in, share, sim, early, late, bufs, share_buf, sim_buf, in_sem, out_sem):
    ways = (
        (early_in, bufs.at[0], early),
        (late_in, bufs.at[1], late),
        (share_in, share_buf, share),
        (sim_in, sim_buf, sim),
    )
    gets = [pltpu.make_async_copy(a, b, in_sem.at[n]) for n, (a, b, _) in enumerate(ways)]
    puts = [pltpu.make_async_copy(b, c, out_sem.at[n]) for n, (_, b, c) in enumerate(ways)]
    for get in gets:
        get.start()
    for get, put in zip(gets, puts):
        get.wait()
        put.start()
    for put in puts:
        put.wait()


def body(layer_early, layer_late):
    vm = pltpu.VMEM
    dma = pltpu.SemaphoreType.DMA
    hbm = pl.BlockSpec(memory_space=pltpu.HBM)
    whole = pl.BlockSpec(memory_space=pltpu.VMEM)
    share, sim, early_rows, late_rows = pl.pallas_call(
        kernel,
        out_shape=(
            jax.ShapeDtypeStruct((1, 32), F32),
            jax.ShapeDtypeStruct((1, 1), F32),
            jax.ShapeDtypeStruct((32, 8192), BF16),
            jax.ShapeDtypeStruct((32, 8192), BF16),
        ),
        in_specs=[hbm, hbm],
        out_specs=(whole, whole, hbm, hbm),
        scratch_shapes=[
            vm((64, 4096), BF16),
            vm((32, 8192), BF16),
            vm((16, 64, 256), BF16),
            vm((32, 64, 256), BF16),
            vm((12, 256, 2048), BF16),
            vm((10, 256, 256), F32),
            vm((6, 256, 256), BF16),
            vm((6, 7, 64, 256), BF16),
            vm((3, 128, 256), BF16),
            vm((3, 7, 32, 256), BF16),
            vm((7, 64, 256), F32),
            vm((1, 2048), F32),
            vm((16, 1, 2048), F32),
            vm((1, 2048), F32),
            vm((4, 1, 2048), F32),
            vm((4, 32, 2048), BF16),
            vm((32, 8192), BF16),
            vm((32, 8192), BF16),
            vm((3, 64, 256), F32),
            vm((64, 128), F32),
            vm((32, 128), F32),
            vm((8, 256), F32),
            vm((16, 1, 384), F32),
            vm((64, 1, 384), F32),
            dma((2,)),
            dma((2,)),
            dma,
            dma((8,)),
            dma,
            dma((4,)),
            dma((5,)),
            dma,
            dma,
            dma,
            dma,
            dma,
            dma((5, PIECES)),
            dma,
            dma,
            dma,
            dma((9,)),
            dma,
            dma,
            dma,
            dma((2,)),
            dma,
        ],
        compiler_params=pltpu.CompilerParams(collective_id=0, has_side_effects=True, vmem_limit_bytes=67043328),
    )(layer_early.T, layer_late)
    share, sim, early_rows, late_rows = pl.pallas_call(
        publish,
        out_shape=(
            jax.ShapeDtypeStruct((1, 32), F32),
            jax.ShapeDtypeStruct((1, 1), F32),
            jax.ShapeDtypeStruct((32, 8192), BF16),
            jax.ShapeDtypeStruct((32, 8192), BF16),
        ),
        in_specs=[hbm] * 4,
        out_specs=(hbm,) * 4,
        scratch_shapes=[
            vm((2, 32, 8192), BF16),
            vm((1, 32), F32),
            vm((1, 1), F32),
            dma((4,)),
            dma((4,)),
        ],
    )(share, sim, early_rows, late_rows)
    return sim.reshape(()), share.reshape(32), early_rows, late_rows


def solution(mesh):
    return jax.shard_map(
        body,
        mesh=mesh,
        in_specs=(P(None, ("gx", "gy")), P(("gx", "gy"), None)),
        out_specs=(P(), P(("gx", "gy")), P(("gx", "gy"), None), P(("gx", "gy"), None)),
        check_vma=False,
    )
```

```python
import jax
import jax.numpy as jnp
from jax import lax
from jax.experimental import pallas as pl
from jax.experimental.pallas import tpu as pltpu
from jax.sharding import PartitionSpec as P

MESH = pl.DeviceIdType.MESH
F32 = jnp.float32
BF16 = jnp.bfloat16

SLOTS = ((0, 0), (1, 0), (0, 1), (1, 1), (1, 3), (3, 1))
TILES = ((0, 0), (1, 0), (2, 0), (1, 2), (4, 2), (5, 1), (3, 0), (4, 5), (3, 5), (3, 4))
SHARED = 7
K_CORE = 1
L_CORE = 0
PIECES = 8
DETOUR = (2, 3)
ORDER = ((0, 0), (0, 1), (2, 0), (2, 1), (1, 0), (1, 1), (3, 0), (3, 1))
EVERYONE = sorted(
    [(dx, dy, dz) for dx in range(4) for dy in range(4) for dz in range(4)],
    key=lambda d: -sum(min(v, 4 - v) for v in d),
)
OTHERS = tuple((dx, dy) for dx in (2, 1, 3, 0) for dy in (2, 1, 3, 0) if dx or dy)


def send(src, dst, send_sem, recv_sem, gx, gy):
    pltpu.make_async_remote_copy(
        src_ref=src,
        dst_ref=dst,
        send_sem=send_sem,
        recv_sem=recv_sem,
        device_id=(gx, gy),
        device_id_type=MESH,
    ).start()


def kernel(
    xt_hbm,
    late_hbm,
    share_ref,
    sim_ref,
    eout_hbm,
    lout_hbm,
    xt,
    late,
    cen,
    rt,
    blocks,
    gram,
    stage,
    parts,
    halves,
    half_parts,
    parts0,
    own_sum,
    plane_sums,
    mean_out,
    means,
    early_pieces,
    early_out,
    late_out,
    acc,
    row_cols,
    half_cols,
    col_acc,
    msg,
    msg_in,
    load_sem,
    out_sem,
    late_send,
    late_recv,
    early_send,
    early_recv,
    pair_send,
    sums_send,
    sums_recv,
    mean_send,
    mean_recv,
    gather_send,
    gather_recv,
    rows_send,
    rows_recv,
    part_send,
    part_recv,
    half_send,
    part0_send,
    part0_recv,
    msg_send,
    msg_recv,
):
    gx = lax.axis_index("gx")
    z = lax.axis_index("gy")
    core = lax.rem(gx, 2)
    chip = gx // 2
    x = chip // 4
    y = lax.rem(chip, 4)
    partner = gx + 1 - 2 * core
    k_dev = 2 * chip + K_CORE
    l_dev = 2 * chip + L_CORE
    is_k = core == K_CORE
    is_l = core == L_CORE

    def arrived(ref, sem, name="wait"):
        with jax.named_scope(name):
            pltpu.make_async_remote_copy(
                src_ref=ref, dst_ref=ref, send_sem=sem, recv_sem=sem, device_id=(partner, z), device_id_type=MESH
            ).wait_recv()

    def left(ref, sem):
        pltpu.make_async_remote_copy(
            src_ref=ref, dst_ref=ref, send_sem=sem, recv_sem=sem, device_id=(partner, z), device_id_type=MESH
        ).wait_send()

    def chip_at(dx, dy):
        return lax.rem(x + dx, 4) * 4 + lax.rem(y + dy, 4)

    def level(dz):
        return lax.rem(z + dz, 4)

    load_x = pltpu.make_async_copy(xt_hbm, xt, load_sem.at[0])
    load_y = pltpu.make_async_copy(late_hbm, late, load_sem.at[1])
    load_x.start()
    load_y.start()
    barrier = pltpu.get_barrier_semaphore()

    for dx, dy in OTHERS:
        other = chip_at(dx, dy)
        pl.semaphore_signal(barrier, inc=1, device_id=(2 * other + core, z), device_id_type=MESH)

    @pl.when(is_k)
    def _():
        for dx, dy in OTHERS:
            other = chip_at(dx, dy)
            pl.semaphore_signal(barrier, inc=1, device_id=(2 * other + L_CORE, z), device_id_type=MESH)

    for dz in (1, 2, 3):
        pl.semaphore_signal(barrier, inc=1, device_id=(2 * chip, level(dz)), device_id_type=MESH)
        pl.semaphore_signal(barrier, inc=1, device_id=(2 * chip + 1, level(dz)), device_id_type=MESH)
    pl.semaphore_signal(barrier, inc=1, device_id=(partner, z), device_id_type=MESH)

    with jax.named_scope("load"):
        load_x.wait()

    sums = jnp.zeros((64, 256), F32)
    for u in range(16):
        sums = sums + xt[:, 256 * u : 256 * (u + 1)].astype(F32)
    col_mean = jnp.sum(sums, axis=1, keepdims=True) / 4096.0
    for u in range(16):
        cen[u] = (xt[:, 256 * u : 256 * (u + 1)].astype(F32) - col_mean).astype(BF16)
    load_y.wait()

    with jax.named_scope("barrier"):
        pl.semaphore_wait(barrier, 22 + 15 * (1 - core))

    def piece(j):
        dz, q = ORDER[j]
        return pl.ds(pl.multiple_of(32 * (4 * q + level(dz)), 32), 32)

    my_rows = pl.ds(pl.multiple_of(32 * (4 * core + z), 32), 32)
    for dz in (2, 1, 3):
        to = level(dz)
        send(
            late.at[:, pl.ds(pl.multiple_of(2048 * to, 2048), 2048)],
            blocks.at[0, my_rows, :],
            late_send,
            late_recv.at[2 * (4 - dz) + core],
            l_dev,
            to,
        )
    own_cols = pl.ds(pl.multiple_of(2048 * z, 2048), 2048)

    for dx, dy in OTHERS:
        other = chip_at(dx, dy)
        send(cen.at[other], rt.at[gx], early_send, early_recv.at[x], 2 * other + K_CORE, z)

    def forward(src, dst, j, ex, ey):
        to = 2 * chip_at(4 - ex, 4 - ey) + core
        rows = piece(j)
        send(blocks.at[src, rows, :], blocks.at[dst, rows, :], gather_send, gather_recv.at[dst - 1, j], to, z)

    def take(slot, j):
        arrived(blocks.at[slot, piece(j), :], gather_recv.at[slot - 1, j], f"g{slot}_{j}")

    @pl.when(is_k)
    def _():
        send(late.at[:, own_cols], blocks.at[0, my_rows, :], pair_send.at[0], late_recv.at[1], l_dev, z)
        rt[gx] = cen[chip]
        for dx in (2, 1, 3, 0):
            xs = lax.rem(x + dx, 4)
            arrived(rt.at[0 : 8 if dx else 7], early_recv.at[xs], f"w_early{dx}")

            @pl.loop(0, 4)
            def _(k):
                u = 4 * xs + k
                cols = jnp.concatenate([rt[2 * u].astype(F32), rt[2 * u + 1].astype(F32)], axis=0)
                at = pl.ds(pl.multiple_of(128 * u, 128), 128)
                blocks[0, :, at] = cols.T.astype(BF16)

        for j in range(PIECES):
            forward(0, 1, j, 1, 0)
            forward(0, 2, j, 0, 1)
        for dz in (1, 2, 3):
            for q in (0, 1):
                rows = pl.ds(pl.multiple_of(32 * (4 * q + level(dz)), 32), 32)
                send(blocks.at[0, rows, :], early_pieces.at[z], rows_send, rows_recv, 2 * chip + q, level(dz))
        rows = pl.ds(pl.multiple_of(32 * (4 * L_CORE + z), 32), 32)
        send(blocks.at[0, rows, :], early_pieces.at[z], pair_send.at[1], rows_recv, l_dev, z)
        early_pieces[z] = blocks[0, my_rows, :]

    def start(j):
        if j != DETOUR[1]:
            forward(0, 2, j, 0, 1)
        if j != DETOUR[0]:
            forward(0, 1, j, 1, 0)

    @pl.when(is_l)
    def _():
        send(cen.at[chip], rt.at[gx], pair_send.at[0], early_recv.at[x], k_dev, z)
        blocks[0, my_rows, :] = late[:, own_cols]
        for j in range(PIECES):
            if j:
                arrived(blocks.at[0, piece(j), :], late_recv.at[2 * ORDER[j][0] + ORDER[j][1]], f"w_late{j}")
            if j < 6:
                start(j)
        for c in range(4):
            at = slice(512 * c, 512 * (c + 1))
            part = jnp.zeros((32, 512), F32)
            for r in range(8):
                part = part + blocks[0, 32 * r : 32 * (r + 1), at].astype(F32)
            own_sum[:, at] = jnp.sum(part, axis=0, keepdims=True)
        plane_sums[chip] = own_sum[...]

        @pl.loop(1, 16)
        def _(r):
            other = lax.rem(chip + r, 16)
            send(own_sum, plane_sums.at[chip], sums_send, sums_recv, 2 * other + L_CORE, z)

        start(6)
        start(7)

    def center(slot):
        for c in range(4):
            at = slice(512 * c, 512 * (c + 1))
            m = mean_out[:, at]
            for r in range(8):
                rows = slice(32 * r, 32 * (r + 1))
                blocks[6 + slot, rows, at] = (blocks[slot, rows, at].astype(F32) - m).astype(BF16)

    def late_mean():
        arrived(plane_sums.at[0:15], sums_recv, "w_sums")
        mean = plane_sums[0]
        for u in range(1, 16):
            mean = mean + plane_sums[u]
        mean_out[...] = mean / 4096.0
        means[z] = mean_out[...]
        send(mean_out, means.at[z], pair_send.at[1], mean_recv, k_dev, z)
        for dz in (1, 2, 3):
            send(mean_out, means.at[z], mean_send, mean_recv, k_dev, level(dz))
            send(mean_out, means.at[z], mean_send, mean_recv, l_dev, level(dz))
        center(0)
        product(0)

    dims = (((1,), (1,)), ((), ()))

    ready = 6 * (1 - core)

    def sides(t):
        a, b = TILES[t]
        if t < SHARED:
            return a, b, 0
        half = (y if t == 9 else x) // 2
        return a + half * (b - a), b + half * (a - b), half

    def product(t):
        a, b, half = sides(t)
        with jax.named_scope(f"dot{t}"):
            if t < SHARED:
                gram[t] = lax.dot_general(blocks[a + ready], blocks[b + ready], dims, preferred_element_type=F32)
            else:
                top = pl.ds(pl.multiple_of(128 * half, 128), 128)
                gram[t, 0:128, :] = lax.dot_general(
                    blocks[a + ready, top, :], blocks[b + ready], dims, preferred_element_type=F32
                )
        if t == 0:
            src, dst, size, out, into, pair = gram.at[0], parts0, 64, part0_send, part0_recv, 2
        elif t < SHARED:
            src, dst, size, out, into, pair = stage.at[t - 1], parts.at[t - 1], 64, part_send, part_recv.at[t - 1], 3
            stage[t - 1] = gram[t].astype(BF16)
        else:
            n = t - SHARED
            src, dst, size, out, into, pair = halves.at[n], half_parts.at[n], 32, half_send, part_recv.at[t - 1], 4
            halves[n] = gram[t, 0:128, :].astype(BF16)
        for dz in (1, 2, 3):
            to = level(dz)
            rows = pl.ds(pl.multiple_of(size * to, size), size)
            send(src.at[rows, :], dst.at[dz - 1 + 4 * (1 - core)], out, into, k_dev, to)

        @pl.when(is_l)
        def _():
            rows = pl.ds(pl.multiple_of(size * z, size), size)
            send(src.at[rows, :], dst.at[3], pair_send.at[pair], into, k_dev, z)

    def settle(t):
        _, b, _ = sides(t)
        if t == 0:
            size, buf, sem = 64, parts0, part0_recv
        elif t < SHARED:
            size, buf, sem = 64, parts.at[t - 1], part_recv.at[t - 1]
        else:
            size, buf, sem = 32, half_parts.at[t - SHARED], part_recv.at[t - 1]
        arrived(buf, sem, f"wp{t}")
        part = [buf[n].astype(F32) for n in range(7)]
        rows = pl.ds(pl.multiple_of(size * z, size), size)
        k = gram[t, rows, :] + ((part[0] + part[1]) + part[2])
        l = (part[3] + part[4]) + (part[5] + part[6])
        h = k * l
        lane = lax.broadcasted_iota(jnp.int32, (size, 128), 1)
        own = jnp.where(lane == t, jnp.sum(h, axis=1, keepdims=True), 0.0)
        weight = 1.0
        if t:
            weight = 2.0
            across = jnp.sum(h, axis=0, keepdims=True)
            col_acc[...] += jnp.where(slot_row == b, across, 0.0)
        if t < SHARED:
            row_cols[...] += own
        else:
            half_cols[...] += own
        acc[0, 0:size] += weight * (k * k)
        acc[1, 0:size] += weight * (l * l)
        acc[2, 0:size] += weight * h

    slot_row = lax.broadcasted_iota(jnp.int32, (8, 256), 0)

    @pl.when(is_k)
    def _():
        acc[...] = jnp.zeros_like(acc)
        row_cols[...] = jnp.zeros_like(row_cols)
        half_cols[...] = jnp.zeros_like(half_cols)
        col_acc[...] = jnp.zeros_like(col_acc)
        product(0)
        for j in range(PIECES):
            take(1, j)
            forward(1, 4, j, 0, 3)
            if j % 2 == 0:
                forward(1, 3, j, 0, 1)
            take(2, j)
            forward(2, 5, j, 3, 0)
            if j % 2:
                forward(2, 3, j, 1, 0)

    @pl.when(is_l)
    def _():
        def from_1(j):
            take(1, j)
            forward(1, 4, j, 0, 3)
            if j == DETOUR[1]:
                forward(1, 3, j, 0, 1)

        def from_2(j):
            take(2, j)
            forward(2, 5, j, 3, 0)
            if j == DETOUR[0]:
                forward(2, 3, j, 1, 0)

        for near, far in ((0, 0), (1, 1), (3, 2), (4, 4), (5, 5), (6, 6), (7, 7)):
            from_1(near)
            from_2(far)
        for j in (0, 1, 4):
            forward(1, 3, j, 0, 1)
        for j in (5, 6, 7):
            forward(2, 3, j, 1, 0)
        late_mean()
        take(3, DETOUR[0])
        forward(3, 1, DETOUR[0], 0, 3)
        take(3, DETOUR[1])
        forward(3, 2, DETOUR[1], 3, 0)
        from_2(DETOUR[1])
        from_1(DETOUR[0])

    @pl.when(is_l)
    def _():
        center(1)
        center(2)

    for t in (1, 2, 3):
        product(t)

    @pl.when(is_k)
    def _():
        arrived(means, mean_recv, "w_mean")
        arrived(early_pieces.at[0:3], rows_recv, "w_rows")

    @pl.when(is_l)
    def _():
        arrived(means.at[0:3], mean_recv, "w_mean")
        arrived(early_pieces, rows_recv, "w_rows")

    for c in range(4):
        at = slice(2048 * c, 2048 * (c + 1))
        late_out[:, at] = (late[:, at].astype(F32) - means[c]).astype(BF16)
    low = lax.broadcasted_iota(jnp.int32, (32, 128), 1) < 64
    for u in range(16):
        p = [early_pieces[c, :, 128 * u : 128 * (u + 1)].astype(F32) for c in range(4)]
        turned = [pltpu.roll(v, 64, 1) for v in p]
        for j in range(2):
            first = jnp.where(low, p[2 * j], turned[2 * j + 1])
            second = jnp.where(low, turned[2 * j], p[2 * j + 1])
            early_out[:, 128 * (4 * u + j) : 128 * (4 * u + j + 1)] = first.astype(BF16)
            early_out[:, 128 * (4 * u + 2 + j) : 128 * (4 * u + 3 + j)] = second.astype(BF16)
    put_e = pltpu.make_async_copy(early_out, eout_hbm, out_sem.at[0])
    put_l = pltpu.make_async_copy(late_out, lout_hbm, out_sem.at[1])
    put_e.start()
    put_l.start()

    for slot in (4, 5):
        for j in range(PIECES):
            take(slot, j)
        pl.when(is_l)(lambda: center(slot))
        product(slot)
    product(7)

    for j in range(PIECES):
        if j in DETOUR:
            pl.when(is_k)(lambda: take(3, j))
        else:
            take(3, j)
    pl.when(is_l)(lambda: center(3))
    for t in (6, 8, 9):
        product(t)

    @pl.when(is_k)
    def _():
        for t in (0, 1, 2, 3, 4, 5, 7, 6, 8, 9):
            settle(t)
        turned = jnp.concatenate([row_cols[...]] * 4, axis=0).T
        half_turned = jnp.concatenate([half_cols[...]] * 8, axis=0).T
        col = lax.broadcasted_iota(jnp.int32, (1, 256), 1)
        both = col_acc[...]
        for t in range(len(TILES)):
            a, _, half = sides(t)
            if t < SHARED:
                row = jnp.where(col // 64 == z, turned[t : t + 1, :], 0.0)
            else:
                row = jnp.where(col // 32 == 4 * half + z, half_turned[t : t + 1, :], 0.0)
            both = both + jnp.where(slot_row == a, row, 0.0)
        scal_lane = lax.broadcasted_iota(jnp.int32, (1, 128), 1)
        scal = jnp.zeros((1, 128), F32)
        for j in range(3):
            s = jnp.sum(jnp.sum(acc[j], axis=0, keepdims=True), axis=1, keepdims=True)
            scal = jnp.where(scal_lane == j, s, scal)
        for dx in range(4):
            for dy in range(4):
                r = 4 * dx + dy
                if (dx, dy) in SLOTS:
                    slot = SLOTS.index((dx, dy))
                    msg[r, :, 0:256] = both[slot : slot + 1, :]
                else:
                    msg[r, :, 0:256] = jnp.zeros((1, 256), F32)
                msg[r, :, 256:384] = scal
        for dx, dy, dz in EVERYONE:
            r = 4 * dx + dy
            there = msg_in.at[16 * dz + r]
            chip_there = 2 * chip_at(dx, dy)
            if dx or dy or dz:
                send(msg.at[r], there, msg_send.at[K_CORE], msg_recv, chip_there + K_CORE, level(dz))
            send(msg.at[r], there, msg_send.at[L_CORE], msg_recv, chip_there + L_CORE, level(dz))
        msg_in[0] = msg[0]
        arrived(msg_in.at[0:63], msg_recv, "w_msg")

    @pl.when(is_l)
    def _():
        arrived(msg_in, msg_recv, "w_msg")

    rows = [msg_in[r] for r in range(64)]
    while len(rows) > 1:
        rows = [a + b for a, b in zip(rows[0::2], rows[1::2])]
    final = rows[0]
    scal_lane = lax.broadcasted_iota(jnp.int32, (1, 128), 1)
    scal = final[:, 256:384]
    kk, ll, kl = (jnp.sum(jnp.where(scal_lane == j, scal, 0.0), axis=1, keepdims=True) for j in range(3))
    norm = jnp.sqrt(kk * ll)
    sim_ref[...] = kl / norm
    half = jnp.where(core == 0, final[:, 0:128], final[:, 128:256])
    tokens = half
    for j in (1, 2, 3):
        tokens = jnp.where(z == j, pltpu.roll(half, 128 - 32 * j, 1), tokens)
    share_ref[...] = (4096.0 * tokens / norm)[:, 0:32]

    with jax.named_scope("end"):
        put_e.wait()
    put_l.wait()
    left(late.at[:, 0:6144], late_send)
    left(cen.at[0:15], early_send)
    left(blocks.at[1:6], gather_send)
    left(parts.at[:, 0:3], part_send)
    left(half_parts.at[:, 0:3], half_send)
    left(parts0.at[0:3], part0_send)

    @pl.when(is_k)
    def _():
        left(late.at[:, 0:2048], pair_send.at[0])
        left(early_pieces.at[0], pair_send.at[1])
        left(blocks.at[0, 0:192, :], rows_send)
        left(msg_in.at[0:63], msg_send.at[K_CORE])
        left(msg_in, msg_send.at[L_CORE])

    @pl.when(is_l)
    def _():
        left(cen.at[0], pair_send.at[0])
        left(mean_out, pair_send.at[1])
        left(parts0.at[0], pair_send.at[2])
        left(parts.at[:, 0], pair_send.at[3])
        left(half_parts.at[:, 0], pair_send.at[4])
        left(plane_sums.at[0:15], sums_send)
        left(plane_sums.at[0:6], mean_send)


def publish(share_in, sim_in, early_in, late_in, share, sim, early, late, bufs, share_buf, sim_buf, in_sem, out_sem):
    ways = (
        (early_in, bufs.at[0], early),
        (late_in, bufs.at[1], late),
        (share_in, share_buf, share),
        (sim_in, sim_buf, sim),
    )
    gets = [pltpu.make_async_copy(a, b, in_sem.at[n]) for n, (a, b, _) in enumerate(ways)]
    puts = [pltpu.make_async_copy(b, c, out_sem.at[n]) for n, (_, b, c) in enumerate(ways)]
    for get in gets:
        get.start()
    for get, put in zip(gets, puts):
        get.wait()
        put.start()
    for put in puts:
        put.wait()


def body(layer_early, layer_late):
    vm = pltpu.VMEM
    dma = pltpu.SemaphoreType.DMA
    hbm = pl.BlockSpec(memory_space=pltpu.HBM)
    whole = pl.BlockSpec(memory_space=pltpu.VMEM)
    share, sim, early_rows, late_rows = pl.pallas_call(
        kernel,
        out_shape=(
            jax.ShapeDtypeStruct((1, 32), F32),
            jax.ShapeDtypeStruct((1, 1), F32),
            jax.ShapeDtypeStruct((32, 8192), BF16),
            jax.ShapeDtypeStruct((32, 8192), BF16),
        ),
        in_specs=[hbm, hbm],
        out_specs=(whole, whole, hbm, hbm),
        scratch_shapes=[
            vm((64, 4096), BF16),
            vm((32, 8192), BF16),
            vm((16, 64, 256), BF16),
            vm((32, 64, 256), BF16),
            vm((12, 256, 2048), BF16),
            vm((10, 256, 256), F32),
            vm((6, 256, 256), BF16),
            vm((6, 7, 64, 256), BF16),
            vm((3, 128, 256), BF16),
            vm((3, 7, 32, 256), BF16),
            vm((7, 64, 256), F32),
            vm((1, 2048), F32),
            vm((16, 1, 2048), F32),
            vm((1, 2048), F32),
            vm((4, 1, 2048), F32),
            vm((4, 32, 2048), BF16),
            vm((32, 8192), BF16),
            vm((32, 8192), BF16),
            vm((3, 64, 256), F32),
            vm((64, 128), F32),
            vm((32, 128), F32),
            vm((8, 256), F32),
            vm((16, 1, 384), F32),
            vm((64, 1, 384), F32),
            dma((2,)),
            dma((2,)),
            dma,
            dma((8,)),
            dma,
            dma((4,)),
            dma((5,)),
            dma,
            dma,
            dma,
            dma,
            dma,
            dma((5, PIECES)),
            dma,
            dma,
            dma,
            dma((9,)),
            dma,
            dma,
            dma,
            dma((2,)),
            dma,
        ],
        compiler_params=pltpu.CompilerParams(collective_id=0, has_side_effects=True, vmem_limit_bytes=67043328),
    )(layer_early.T, layer_late)
    share, sim, early_rows, late_rows = pl.pallas_call(
        publish,
        out_shape=(
            jax.ShapeDtypeStruct((1, 32), F32),
            jax.ShapeDtypeStruct((1, 1), F32),
            jax.ShapeDtypeStruct((32, 8192), BF16),
            jax.ShapeDtypeStruct((32, 8192), BF16),
        ),
        in_specs=[hbm] * 4,
        out_specs=(hbm,) * 4,
        scratch_shapes=[
            vm((2, 32, 8192), BF16),
            vm((1, 32), F32),
            vm((1, 1), F32),
            dma((4,)),
            dma((4,)),
        ],
    )(share, sim, early_rows, late_rows)
    return sim.reshape(()), share.reshape(32), early_rows, late_rows


def solution(mesh):
    return jax.shard_map(
        body,
        mesh=mesh,
        in_specs=(P(None, ("gx", "gy")), P(("gx", "gy"), None)),
        out_specs=(P(), P(("gx", "gy")), P(("gx", "gy"), None), P(("gx", "gy"), None)),
        check_vma=False,
    )
```

```python
import jax
import jax.numpy as jnp
from jax import lax
from jax.experimental import pallas as pl
from jax.experimental.pallas import tpu as pltpu
from jax.sharding import PartitionSpec as P

MESH = pl.DeviceIdType.MESH
F32 = jnp.float32
BF16 = jnp.bfloat16

SLOTS = ((0, 0), (1, 0), (0, 1), (1, 1), (1, 3), (3, 1))
TILES = (
    (0, 0, None),
    (1, 2, None),
    (4, 2, None),
    (5, 1, None),
    (1, 0, 0),
    (1, 0, 1),
    (2, 0, 0),
    (2, 0, 1),
    (3, 0, 0),
    (3, 0, 1),
    (4, 5, "x"),
    (3, 5, "x"),
    (3, 4, "y"),
)
WHOLE = 4
K_CORE = 1
L_CORE = 0
PIECES = 8
DETOUR = (5, 6)
ORDER = ((0, 0), (2, 0), (1, 0), (3, 0), (0, 1), (2, 1), (1, 1), (3, 1))
EVERYONE = sorted(
    [(dx, dy, dz) for dx in range(4) for dy in range(4) for dz in range(4)],
    key=lambda d: -sum(min(v, 4 - v) for v in d),
)
OTHERS = tuple((dx, dy) for dx in (2, 1, 3, 0) for dy in (2, 1, 3, 0) if dx or dy)


def send(src, dst, send_sem, recv_sem, gx, gy):
    pltpu.make_async_remote_copy(
        src_ref=src,
        dst_ref=dst,
        send_sem=send_sem,
        recv_sem=recv_sem,
        device_id=(gx, gy),
        device_id_type=MESH,
    ).start()


def kernel(
    xt_hbm,
    late_hbm,
    share_ref,
    sim_ref,
    eout_hbm,
    lout_hbm,
    xt,
    late,
    cen,
    rt,
    blocks,
    gram,
    stage,
    parts,
    halves,
    half_parts,
    parts0,
    own_sum,
    plane_sums,
    mean_out,
    means,
    early_pieces,
    early_out,
    late_out,
    acc,
    row_cols,
    half_cols,
    col_acc,
    msg,
    msg_in,
    load_sem,
    out_sem,
    late_send,
    late_recv,
    early_send,
    early_recv,
    pair_send,
    sums_send,
    sums_recv,
    mean_send,
    mean_recv,
    gather_send,
    gather_recv,
    rows_send,
    rows_recv,
    part_send,
    part_recv,
    half_send,
    part0_send,
    part0_recv,
    msg_send,
    msg_recv,
):
    gx = lax.axis_index("gx")
    z = lax.axis_index("gy")
    core = lax.rem(gx, 2)
    chip = gx // 2
    x = chip // 4
    y = lax.rem(chip, 4)
    partner = gx + 1 - 2 * core
    k_dev = 2 * chip + K_CORE
    l_dev = 2 * chip + L_CORE
    is_k = core == K_CORE
    is_l = core == L_CORE

    def arrived(ref, sem, name="wait"):
        with jax.named_scope(name):
            pltpu.make_async_remote_copy(
                src_ref=ref, dst_ref=ref, send_sem=sem, recv_sem=sem, device_id=(partner, z), device_id_type=MESH
            ).wait_recv()

    def left(ref, sem):
        pltpu.make_async_remote_copy(
            src_ref=ref, dst_ref=ref, send_sem=sem, recv_sem=sem, device_id=(partner, z), device_id_type=MESH
        ).wait_send()

    def chip_at(dx, dy):
        return lax.rem(x + dx, 4) * 4 + lax.rem(y + dy, 4)

    def level(dz):
        return lax.rem(z + dz, 4)

    load_x = pltpu.make_async_copy(xt_hbm, xt, load_sem.at[0])
    load_y = pltpu.make_async_copy(late_hbm, late, load_sem.at[1])
    load_x.start()
    load_y.start()
    barrier = pltpu.get_barrier_semaphore()

    for dx, dy in OTHERS:
        other = chip_at(dx, dy)
        pl.semaphore_signal(barrier, inc=1, device_id=(2 * other + core, z), device_id_type=MESH)

    @pl.when(is_k)
    def _():
        for dx, dy in OTHERS:
            other = chip_at(dx, dy)
            pl.semaphore_signal(barrier, inc=1, device_id=(2 * other + L_CORE, z), device_id_type=MESH)

    for dz in (1, 2, 3):
        pl.semaphore_signal(barrier, inc=1, device_id=(2 * chip, level(dz)), device_id_type=MESH)
        pl.semaphore_signal(barrier, inc=1, device_id=(2 * chip + 1, level(dz)), device_id_type=MESH)
    pl.semaphore_signal(barrier, inc=1, device_id=(partner, z), device_id_type=MESH)

    with jax.named_scope("load"):
        load_x.wait()

    sums = jnp.zeros((64, 256), F32)
    for u in range(16):
        sums = sums + xt[:, 256 * u : 256 * (u + 1)].astype(F32)
    col_mean = jnp.sum(sums, axis=1, keepdims=True) / 4096.0
    for u in range(16):
        cen[u] = (xt[:, 256 * u : 256 * (u + 1)].astype(F32) - col_mean).astype(BF16)
    load_y.wait()

    with jax.named_scope("barrier"):
        pl.semaphore_wait(barrier, 22 + 15 * (1 - core))

    def piece(j):
        dz, q = ORDER[j]
        return pl.ds(pl.multiple_of(32 * (4 * q + level(dz)), 32), 32)

    my_rows = pl.ds(pl.multiple_of(32 * (4 * core + z), 32), 32)
    for dz in (2, 1, 3):
        to = level(dz)
        send(
            late.at[:, pl.ds(pl.multiple_of(2048 * to, 2048), 2048)],
            blocks.at[0, my_rows, :],
            late_send,
            late_recv.at[2 * (4 - dz) + core],
            l_dev,
            to,
        )
    own_cols = pl.ds(pl.multiple_of(2048 * z, 2048), 2048)

    for dx, dy in OTHERS:
        other = chip_at(dx, dy)
        send(cen.at[other], rt.at[gx], early_send, early_recv.at[x], 2 * other + K_CORE, z)

    def forward(src, dst, j, ex, ey):
        to = 2 * chip_at(4 - ex, 4 - ey) + core
        rows = piece(j)
        send(blocks.at[src, rows, :], blocks.at[dst, rows, :], gather_send, gather_recv.at[dst - 1, j], to, z)

    def take(slot, j):
        arrived(blocks.at[slot, piece(j), :], gather_recv.at[slot - 1, j], f"g{slot}_{j}")

    @pl.when(is_k)
    def _():
        send(late.at[:, own_cols], blocks.at[0, my_rows, :], pair_send.at[0], late_recv.at[1], l_dev, z)
        rt[gx] = cen[chip]
        for dx in (2, 1, 3, 0):
            xs = lax.rem(x + dx, 4)
            arrived(rt.at[0 : 8 if dx else 7], early_recv.at[xs], f"w_early{dx}")

            @pl.loop(0, 4)
            def _(k):
                u = 4 * xs + k
                cols = jnp.concatenate([rt[2 * u].astype(F32), rt[2 * u + 1].astype(F32)], axis=0)
                at = pl.ds(pl.multiple_of(128 * u, 128), 128)
                blocks[0, :, at] = cols.T.astype(BF16)

        for j in range(PIECES):
            forward(0, 1, j, 1, 0)
            forward(0, 2, j, 0, 1)
        for dz in (1, 2, 3):
            for q in (0, 1):
                rows = pl.ds(pl.multiple_of(32 * (4 * q + level(dz)), 32), 32)
                send(blocks.at[0, rows, :], early_pieces.at[z], rows_send, rows_recv, 2 * chip + q, level(dz))
        rows = pl.ds(pl.multiple_of(32 * (4 * L_CORE + z), 32), 32)
        send(blocks.at[0, rows, :], early_pieces.at[z], pair_send.at[1], rows_recv, l_dev, z)
        early_pieces[z] = blocks[0, my_rows, :]

    def start(j):
        if j != DETOUR[1]:
            forward(0, 2, j, 0, 1)
        if j != DETOUR[0]:
            forward(0, 1, j, 1, 0)

    @pl.when(is_l)
    def _():
        send(cen.at[chip], rt.at[gx], pair_send.at[0], early_recv.at[x], k_dev, z)
        blocks[0, my_rows, :] = late[:, own_cols]
        for n, j in enumerate((0, 4, 1, 5, 2, 6, 3, 7)):
            if j:
                arrived(blocks.at[0, piece(j), :], late_recv.at[2 * ORDER[j][0] + ORDER[j][1]], f"w_late{j}")
            if n < 6:
                start(j)
        for c in range(4):
            at = slice(512 * c, 512 * (c + 1))
            part = jnp.zeros((32, 512), F32)
            for r in range(8):
                part = part + blocks[0, 32 * r : 32 * (r + 1), at].astype(F32)
            own_sum[:, at] = jnp.sum(part, axis=0, keepdims=True)
        plane_sums[chip] = own_sum[...]

        @pl.loop(1, 16)
        def _(r):
            other = lax.rem(chip + r, 16)
            send(own_sum, plane_sums.at[chip], sums_send, sums_recv, 2 * other + L_CORE, z)

        start(3)
        start(7)

    def center(slot, half=None):
        for c in range(4):
            at = slice(512 * c, 512 * (c + 1))
            m = mean_out[:, at]
            for r in range(8) if half is None else range(4 * half, 4 * half + 4):
                rows = slice(32 * r, 32 * (r + 1))
                blocks[6 + slot, rows, at] = (blocks[slot, rows, at].astype(F32) - m).astype(BF16)

    def late_mean():
        arrived(plane_sums.at[0:15], sums_recv, "w_sums")
        mean = plane_sums[0]
        for u in range(1, 16):
            mean = mean + plane_sums[u]
        mean_out[...] = mean / 4096.0
        means[z] = mean_out[...]
        send(mean_out, means.at[z], pair_send.at[1], mean_recv, k_dev, z)
        for dz in (1, 2, 3):
            send(mean_out, means.at[z], mean_send, mean_recv, k_dev, level(dz))
            send(mean_out, means.at[z], mean_send, mean_recv, l_dev, level(dz))
        center(0)
        product(0)

    dims = (((1,), (1,)), ((), ()))

    ready = 6 * (1 - core)

    def sides(t):
        a, b, half = TILES[t]
        if half in ("x", "y"):
            half = (x if half == "x" else y) // 2
            return a + half * (b - a), b + half * (a - b), half
        return a, b, half

    def product(t):
        a, b, half = sides(t)
        with jax.named_scope(f"dot{t}"):
            if t < WHOLE:
                gram[t] = lax.dot_general(blocks[a + ready], blocks[b + ready], dims, preferred_element_type=F32)
            else:
                top = pl.ds(pl.multiple_of(128 * half, 128), 128)
                gram[t, 0:128, :] = lax.dot_general(
                    blocks[a + ready, top, :], blocks[b + ready], dims, preferred_element_type=F32
                )
        if t == 0:
            src, dst, size, out, into, pair = gram.at[0], parts0, 64, part0_send, part0_recv, 2
        elif t < WHOLE:
            src, dst, size, out, into, pair = stage.at[t - 1], parts.at[t - 1], 64, part_send, part_recv.at[t - 1], 3
            stage[t - 1] = gram[t].astype(BF16)
        else:
            n = t - WHOLE
            src, dst, size, out, into, pair = halves.at[n], half_parts.at[n], 32, half_send, part_recv.at[t - 1], 4
            halves[n] = gram[t, 0:128, :].astype(BF16)
        for dz in (1, 2, 3):
            to = level(dz)
            rows = pl.ds(pl.multiple_of(size * to, size), size)
            send(src.at[rows, :], dst.at[dz - 1 + 4 * (1 - core)], out, into, k_dev, to)

        @pl.when(is_l)
        def _():
            rows = pl.ds(pl.multiple_of(size * z, size), size)
            send(src.at[rows, :], dst.at[3], pair_send.at[pair], into, k_dev, z)

    def settle(t):
        _, b, _ = sides(t)
        if t == 0:
            size, buf, sem = 64, parts0, part0_recv
        elif t < WHOLE:
            size, buf, sem = 64, parts.at[t - 1], part_recv.at[t - 1]
        else:
            size, buf, sem = 32, half_parts.at[t - WHOLE], part_recv.at[t - 1]
        arrived(buf, sem, f"wp{t}")
        part = [buf[n].astype(F32) for n in range(7)]
        rows = pl.ds(pl.multiple_of(size * z, size), size)
        k = gram[t, rows, :] + ((part[0] + part[1]) + part[2])
        l = (part[3] + part[4]) + (part[5] + part[6])
        h = k * l
        lane = lax.broadcasted_iota(jnp.int32, (size, 128), 1)
        own = jnp.where(lane == t, jnp.sum(h, axis=1, keepdims=True), 0.0)
        weight = 1.0
        if t:
            weight = 2.0
            across = jnp.sum(h, axis=0, keepdims=True)
            col_acc[...] += jnp.where(slot_row == b, across, 0.0)
        if t < WHOLE:
            row_cols[...] += own
        else:
            half_cols[...] += own
        acc[0, 0:size] += weight * (k * k)
        acc[1, 0:size] += weight * (l * l)
        acc[2, 0:size] += weight * h

    slot_row = lax.broadcasted_iota(jnp.int32, (8, 256), 0)

    @pl.when(is_k)
    def _():
        acc[...] = jnp.zeros_like(acc)
        row_cols[...] = jnp.zeros_like(row_cols)
        half_cols[...] = jnp.zeros_like(half_cols)
        col_acc[...] = jnp.zeros_like(col_acc)
        product(0)
        for j in range(PIECES):
            take(1, j)
            forward(1, 4, j, 0, 3)
            if j % 2 == 0:
                forward(1, 3, j, 0, 1)
            take(2, j)
            forward(2, 5, j, 3, 0)
            if j % 2:
                forward(2, 3, j, 1, 0)
            if j == 3:
                product(4)
                product(6)

    @pl.when(is_l)
    def _():
        def from_1(j):
            take(1, j)
            forward(1, 4, j, 0, 3)
            if j == DETOUR[1]:
                forward(1, 3, j, 0, 1)

        def from_2(j):
            take(2, j)
            forward(2, 5, j, 3, 0)
            if j == DETOUR[0]:
                forward(2, 3, j, 1, 0)

        for near, far in ((0, 0), (4, 4), (1, 1), (2, 5), (6, 2), (3, 3), (7, 7)):
            from_1(near)
            from_2(far)
        late_mean()
        center(1, 0)
        product(4)
        center(2, 0)
        product(6)
        for j in (0, 1, 2, 3, 4, 7):
            if j % 2:
                forward(1, 3, j, 0, 1)
            else:
                forward(2, 3, j, 1, 0)
        take(3, DETOUR[0])
        forward(3, 1, DETOUR[0], 0, 3)
        take(3, DETOUR[1])
        forward(3, 2, DETOUR[1], 3, 0)
        from_2(DETOUR[1])
        from_1(DETOUR[0])
        center(1, 1)
        center(2, 1)

    for t in (5, 7, 1):
        product(t)

    @pl.when(is_k)
    def _():
        arrived(means, mean_recv, "w_mean")
        arrived(early_pieces.at[0:3], rows_recv, "w_rows")

    @pl.when(is_l)
    def _():
        arrived(means.at[0:3], mean_recv, "w_mean")
        arrived(early_pieces, rows_recv, "w_rows")

    for c in range(4):
        at = slice(2048 * c, 2048 * (c + 1))
        late_out[:, at] = (late[:, at].astype(F32) - means[c]).astype(BF16)
    low = lax.broadcasted_iota(jnp.int32, (32, 128), 1) < 64
    for u in range(16):
        p = [early_pieces[c, :, 128 * u : 128 * (u + 1)].astype(F32) for c in range(4)]
        turned = [pltpu.roll(v, 64, 1) for v in p]
        for j in range(2):
            first = jnp.where(low, p[2 * j], turned[2 * j + 1])
            second = jnp.where(low, turned[2 * j], p[2 * j + 1])
            early_out[:, 128 * (4 * u + j) : 128 * (4 * u + j + 1)] = first.astype(BF16)
            early_out[:, 128 * (4 * u + 2 + j) : 128 * (4 * u + 3 + j)] = second.astype(BF16)
    put_e = pltpu.make_async_copy(early_out, eout_hbm, out_sem.at[0])
    put_l = pltpu.make_async_copy(late_out, lout_hbm, out_sem.at[1])
    put_e.start()
    put_l.start()

    for j in range(4):
        take(3, j)
    pl.when(is_l)(lambda: center(3, 0))
    product(8)
    for slot, t in ((4, 2), (5, 3)):
        for j in range(PIECES):
            take(slot, j)
        pl.when(is_l)(lambda: center(slot))
        product(t)
    product(10)
    for j in range(4, PIECES):
        if j in DETOUR:
            pl.when(is_k)(lambda: take(3, j))
        else:
            take(3, j)
    pl.when(is_l)(lambda: center(3, 1))
    for t in (9, 11, 12):
        product(t)

    @pl.when(is_k)
    def _():
        for t in (0, 4, 6, 5, 7, 1, 8, 2, 3, 10, 9, 11, 12):
            settle(t)
        turned = jnp.concatenate([row_cols[...]] * 4, axis=0).T
        half_turned = jnp.concatenate([half_cols[...]] * 8, axis=0).T
        col = lax.broadcasted_iota(jnp.int32, (1, 256), 1)
        both = col_acc[...]
        for t in range(len(TILES)):
            a, _, half = sides(t)
            if t < WHOLE:
                row = jnp.where(col // 64 == z, turned[t : t + 1, :], 0.0)
            else:
                row = jnp.where(col // 32 == 4 * half + z, half_turned[t : t + 1, :], 0.0)
            both = both + jnp.where(slot_row == a, row, 0.0)
        scal_lane = lax.broadcasted_iota(jnp.int32, (1, 128), 1)
        scal = jnp.zeros((1, 128), F32)
        for j in range(3):
            s = jnp.sum(jnp.sum(acc[j], axis=0, keepdims=True), axis=1, keepdims=True)
            scal = jnp.where(scal_lane == j, s, scal)
        for dx in range(4):
            for dy in range(4):
                r = 4 * dx + dy
                if (dx, dy) in SLOTS:
                    slot = SLOTS.index((dx, dy))
                    msg[r, :, 0:256] = both[slot : slot + 1, :]
                else:
                    msg[r, :, 0:256] = jnp.zeros((1, 256), F32)
                msg[r, :, 256:384] = scal
        for dx, dy, dz in EVERYONE:
            r = 4 * dx + dy
            there = msg_in.at[16 * dz + r]
            chip_there = 2 * chip_at(dx, dy)
            if dx or dy or dz:
                send(msg.at[r], there, msg_send.at[K_CORE], msg_recv, chip_there + K_CORE, level(dz))
            send(msg.at[r], there, msg_send.at[L_CORE], msg_recv, chip_there + L_CORE, level(dz))
        msg_in[0] = msg[0]
        arrived(msg_in.at[0:63], msg_recv, "w_msg")

    @pl.when(is_l)
    def _():
        arrived(msg_in, msg_recv, "w_msg")

    rows = [msg_in[r] for r in range(64)]
    while len(rows) > 1:
        rows = [a + b for a, b in zip(rows[0::2], rows[1::2])]
    final = rows[0]
    scal_lane = lax.broadcasted_iota(jnp.int32, (1, 128), 1)
    scal = final[:, 256:384]
    kk, ll, kl = (jnp.sum(jnp.where(scal_lane == j, scal, 0.0), axis=1, keepdims=True) for j in range(3))
    norm = jnp.sqrt(kk * ll)
    sim_ref[...] = kl / norm
    half = jnp.where(core == 0, final[:, 0:128], final[:, 128:256])
    tokens = half
    for j in (1, 2, 3):
        tokens = jnp.where(z == j, pltpu.roll(half, 128 - 32 * j, 1), tokens)
    share_ref[...] = (4096.0 * tokens / norm)[:, 0:32]

    with jax.named_scope("end"):
        put_e.wait()
    put_l.wait()
    left(late.at[:, 0:6144], late_send)
    left(cen.at[0:15], early_send)
    left(blocks.at[1:6], gather_send)
    left(parts.at[:, 0:3], part_send)
    left(half_parts.at[:, 0:3], half_send)
    left(parts0.at[0:3], part0_send)

    @pl.when(is_k)
    def _():
        left(late.at[:, 0:2048], pair_send.at[0])
        left(early_pieces.at[0], pair_send.at[1])
        left(blocks.at[0, 0:192, :], rows_send)
        left(msg_in.at[0:63], msg_send.at[K_CORE])
        left(msg_in, msg_send.at[L_CORE])

    @pl.when(is_l)
    def _():
        left(cen.at[0], pair_send.at[0])
        left(mean_out, pair_send.at[1])
        left(parts0.at[0], pair_send.at[2])
        left(parts.at[:, 0], pair_send.at[3])
        left(half_parts.at[:, 0], pair_send.at[4])
        left(plane_sums.at[0:15], sums_send)
        left(plane_sums.at[0:6], mean_send)


def publish(share_in, sim_in, early_in, late_in, share, sim, early, late, bufs, share_buf, sim_buf, in_sem, out_sem):
    ways = (
        (early_in, bufs.at[0], early),
        (late_in, bufs.at[1], late),
        (share_in, share_buf, share),
        (sim_in, sim_buf, sim),
    )
    gets = [pltpu.make_async_copy(a, b, in_sem.at[n]) for n, (a, b, _) in enumerate(ways)]
    puts = [pltpu.make_async_copy(b, c, out_sem.at[n]) for n, (_, b, c) in enumerate(ways)]
    for get in gets:
        get.start()
    for get, put in zip(gets, puts):
        get.wait()
        put.start()
    for put in puts:
        put.wait()


def body(layer_early, layer_late):
    vm = pltpu.VMEM
    dma = pltpu.SemaphoreType.DMA
    hbm = pl.BlockSpec(memory_space=pltpu.HBM)
    whole = pl.BlockSpec(memory_space=pltpu.VMEM)
    share, sim, early_rows, late_rows = pl.pallas_call(
        kernel,
        out_shape=(
            jax.ShapeDtypeStruct((1, 32), F32),
            jax.ShapeDtypeStruct((1, 1), F32),
            jax.ShapeDtypeStruct((32, 8192), BF16),
            jax.ShapeDtypeStruct((32, 8192), BF16),
        ),
        in_specs=[hbm, hbm],
        out_specs=(whole, whole, hbm, hbm),
        scratch_shapes=[
            vm((64, 4096), BF16),
            vm((32, 8192), BF16),
            vm((16, 64, 256), BF16),
            vm((32, 64, 256), BF16),
            vm((12, 256, 2048), BF16),
            vm((13, 256, 256), F32),
            vm((3, 256, 256), BF16),
            vm((3, 7, 64, 256), BF16),
            vm((9, 128, 256), BF16),
            vm((9, 7, 32, 256), BF16),
            vm((7, 64, 256), F32),
            vm((1, 2048), F32),
            vm((16, 1, 2048), F32),
            vm((1, 2048), F32),
            vm((4, 1, 2048), F32),
            vm((4, 32, 2048), BF16),
            vm((32, 8192), BF16),
            vm((32, 8192), BF16),
            vm((3, 64, 256), F32),
            vm((64, 128), F32),
            vm((32, 128), F32),
            vm((8, 256), F32),
            vm((16, 1, 384), F32),
            vm((64, 1, 384), F32),
            dma((2,)),
            dma((2,)),
            dma,
            dma((8,)),
            dma,
            dma((4,)),
            dma((5,)),
            dma,
            dma,
            dma,
            dma,
            dma,
            dma((5, PIECES)),
            dma,
            dma,
            dma,
            dma((12,)),
            dma,
            dma,
            dma,
            dma((2,)),
            dma,
        ],
        compiler_params=pltpu.CompilerParams(collective_id=0, has_side_effects=True, vmem_limit_bytes=67043328),
    )(layer_early.T, layer_late)
    share, sim, early_rows, late_rows = pl.pallas_call(
        publish,
        out_shape=(
            jax.ShapeDtypeStruct((1, 32), F32),
            jax.ShapeDtypeStruct((1, 1), F32),
            jax.ShapeDtypeStruct((32, 8192), BF16),
            jax.ShapeDtypeStruct((32, 8192), BF16),
        ),
        in_specs=[hbm] * 4,
        out_specs=(hbm,) * 4,
        scratch_shapes=[
            vm((2, 32, 8192), BF16),
            vm((1, 32), F32),
            vm((1, 1), F32),
            dma((4,)),
            dma((4,)),
        ],
    )(share, sim, early_rows, late_rows)
    return sim.reshape(()), share.reshape(32), early_rows, late_rows


def solution(mesh):
    return jax.shard_map(
        body,
        mesh=mesh,
        in_specs=(P(None, ("gx", "gy")), P(("gx", "gy"), None)),
        out_specs=(P(), P(("gx", "gy")), P(("gx", "gy"), None), P(("gx", "gy"), None)),
        check_vma=False,
    )
```

```python
import jax
import jax.numpy as jnp
from jax import lax
from jax.experimental import pallas as pl
from jax.experimental.pallas import tpu as pltpu
from jax.sharding import PartitionSpec as P

MESH = pl.DeviceIdType.MESH
F32 = jnp.float32
BF16 = jnp.bfloat16

SLOTS = ((0, 0), (1, 0), (0, 1), (1, 1), (1, 3), (3, 1))
TILES = (
    (0, 0, None),
    (1, 2, None),
    (4, 2, None),
    (5, 1, None),
    (1, 0, 0),
    (1, 0, 1),
    (2, 0, 0),
    (2, 0, 1),
    (3, 0, 0),
    (3, 0, 1),
    (4, 5, "x"),
    (3, 5, "x"),
    (3, 4, "y"),
)
WHOLE = 4
K_CORE = 1
L_CORE = 0
PIECES = 8
DETOUR = (5, 6)
ORDER = ((0, 0), (2, 0), (1, 0), (3, 0), (0, 1), (2, 1), (1, 1), (3, 1))
EVERYONE = sorted(
    [(dx, dy, dz) for dx in range(4) for dy in range(4) for dz in range(4)],
    key=lambda d: -sum(min(v, 4 - v) for v in d),
)
OTHERS = tuple((dx, dy) for dx in (2, 1, 3, 0) for dy in (2, 1, 3, 0) if dx or dy)


def send(src, dst, send_sem, recv_sem, gx, gy):
    pltpu.make_async_remote_copy(
        src_ref=src,
        dst_ref=dst,
        send_sem=send_sem,
        recv_sem=recv_sem,
        device_id=(gx, gy),
        device_id_type=MESH,
    ).start()


def kernel(
    xt_hbm,
    late_hbm,
    share_ref,
    sim_ref,
    eout_hbm,
    lout_hbm,
    xt,
    late,
    cen,
    rt,
    blocks,
    gram,
    stage,
    parts,
    halves,
    half_parts,
    parts0,
    own_sum,
    plane_sums,
    mean_out,
    means,
    early_pieces,
    early_out,
    late_out,
    acc,
    row_cols,
    half_cols,
    col_acc,
    msg,
    msg_in,
    load_sem,
    out_sem,
    late_send,
    late_recv,
    early_send,
    early_recv,
    pair_send,
    sums_send,
    sums_recv,
    mean_send,
    mean_recv,
    gather_send,
    gather_recv,
    rows_send,
    rows_recv,
    part_send,
    part_recv,
    half_send,
    part0_send,
    part0_recv,
    msg_send,
    msg_recv,
):
    gx = lax.axis_index("gx")
    z = lax.axis_index("gy")
    core = lax.rem(gx, 2)
    chip = gx // 2
    x = chip // 4
    y = lax.rem(chip, 4)
    partner = gx + 1 - 2 * core
    k_dev = 2 * chip + K_CORE
    l_dev = 2 * chip + L_CORE
    is_k = core == K_CORE
    is_l = core == L_CORE

    def arrived(ref, sem, name="wait"):
        with jax.named_scope(name):
            pltpu.make_async_remote_copy(
                src_ref=ref, dst_ref=ref, send_sem=sem, recv_sem=sem, device_id=(partner, z), device_id_type=MESH
            ).wait_recv()

    def left(ref, sem):
        pltpu.make_async_remote_copy(
            src_ref=ref, dst_ref=ref, send_sem=sem, recv_sem=sem, device_id=(partner, z), device_id_type=MESH
        ).wait_send()

    def chip_at(dx, dy):
        return lax.rem(x + dx, 4) * 4 + lax.rem(y + dy, 4)

    def level(dz):
        return lax.rem(z + dz, 4)

    load_x = pltpu.make_async_copy(xt_hbm, xt, load_sem.at[0])
    load_y = pltpu.make_async_copy(late_hbm, late, load_sem.at[1])
    load_x.start()
    load_y.start()
    barrier = pltpu.get_barrier_semaphore()

    for dx, dy in OTHERS:
        other = chip_at(dx, dy)
        pl.semaphore_signal(barrier, inc=1, device_id=(2 * other + core, z), device_id_type=MESH)

    @pl.when(is_k)
    def _():
        for dx, dy in OTHERS:
            other = chip_at(dx, dy)
            pl.semaphore_signal(barrier, inc=1, device_id=(2 * other + L_CORE, z), device_id_type=MESH)

    for dz in (1, 2, 3):
        pl.semaphore_signal(barrier, inc=1, device_id=(2 * chip, level(dz)), device_id_type=MESH)
        pl.semaphore_signal(barrier, inc=1, device_id=(2 * chip + 1, level(dz)), device_id_type=MESH)
    pl.semaphore_signal(barrier, inc=1, device_id=(partner, z), device_id_type=MESH)

    with jax.named_scope("load"):
        load_x.wait()

    sums = jnp.zeros((64, 256), F32)
    for u in range(16):
        sums = sums + xt[:, 256 * u : 256 * (u + 1)].astype(F32)
    col_mean = jnp.sum(sums, axis=1, keepdims=True) / 4096.0
    for u in range(16):
        cen[u] = (xt[:, 256 * u : 256 * (u + 1)].astype(F32) - col_mean).astype(BF16)
    load_y.wait()

    with jax.named_scope("barrier"):
        pl.semaphore_wait(barrier, 22 + 15 * (1 - core))

    def piece(j):
        dz, q = ORDER[j]
        return pl.ds(pl.multiple_of(32 * (4 * q + level(dz)), 32), 32)

    my_rows = pl.ds(pl.multiple_of(32 * (4 * core + z), 32), 32)
    for dz in (2, 1, 3):
        to = level(dz)
        send(
            late.at[:, pl.ds(pl.multiple_of(2048 * to, 2048), 2048)],
            blocks.at[0, my_rows, :],
            late_send,
            late_recv.at[2 * (4 - dz) + core],
            l_dev,
            to,
        )
    own_cols = pl.ds(pl.multiple_of(2048 * z, 2048), 2048)

    for dx, dy in OTHERS:
        other = chip_at(dx, dy)
        send(cen.at[other], rt.at[gx], early_send, early_recv.at[x], 2 * other + K_CORE, z)

    def forward(src, dst, j, ex, ey):
        to = 2 * chip_at(4 - ex, 4 - ey) + core
        rows = piece(j)
        send(blocks.at[src, rows, :], blocks.at[dst, rows, :], gather_send, gather_recv.at[dst - 1, j], to, z)

    def take(slot, j):
        arrived(blocks.at[slot, piece(j), :], gather_recv.at[slot - 1, j], f"g{slot}_{j}")

    @pl.when(is_k)
    def _():
        send(late.at[:, own_cols], blocks.at[0, my_rows, :], pair_send.at[0], late_recv.at[1], l_dev, z)
        rt[gx] = cen[chip]
        for dx in (2, 1, 3, 0):
            xs = lax.rem(x + dx, 4)
            arrived(rt.at[0 : 8 if dx else 7], early_recv.at[xs], f"w_early{dx}")

            @pl.loop(0, 4)
            def _(k):
                u = 4 * xs + k
                cols = jnp.concatenate([rt[2 * u].astype(F32), rt[2 * u + 1].astype(F32)], axis=0)
                at = pl.ds(pl.multiple_of(128 * u, 128), 128)
                blocks[0, :, at] = cols.T.astype(BF16)

        for j in range(PIECES):
            forward(0, 1, j, 1, 0)
            forward(0, 2, j, 0, 1)
        for dz in (1, 2, 3):
            for q in (0, 1):
                rows = pl.ds(pl.multiple_of(32 * (4 * q + level(dz)), 32), 32)
                send(blocks.at[0, rows, :], early_pieces.at[z], rows_send, rows_recv, 2 * chip + q, level(dz))
        rows = pl.ds(pl.multiple_of(32 * (4 * L_CORE + z), 32), 32)
        send(blocks.at[0, rows, :], early_pieces.at[z], pair_send.at[1], rows_recv, l_dev, z)
        early_pieces[z] = blocks[0, my_rows, :]

    def start(j):
        if j != DETOUR[1]:
            forward(0, 2, j, 0, 1)
        if j != DETOUR[0]:
            forward(0, 1, j, 1, 0)

    @pl.when(is_l)
    def _():
        send(cen.at[chip], rt.at[gx], pair_send.at[0], early_recv.at[x], k_dev, z)
        blocks[0, my_rows, :] = late[:, own_cols]
        for n, j in enumerate((0, 4, 1, 5, 2, 6, 3, 7)):
            if j:
                arrived(blocks.at[0, piece(j), :], late_recv.at[2 * ORDER[j][0] + ORDER[j][1]], f"w_late{j}")
            if n < 6:
                start(j)
        for c in range(4):
            at = slice(512 * c, 512 * (c + 1))
            part = jnp.zeros((32, 512), F32)
            for r in range(8):
                part = part + blocks[0, 32 * r : 32 * (r + 1), at].astype(F32)
            own_sum[:, at] = jnp.sum(part, axis=0, keepdims=True)
        plane_sums[chip] = own_sum[...]

        @pl.loop(1, 16)
        def _(r):
            other = lax.rem(chip + r, 16)
            send(own_sum, plane_sums.at[chip], sums_send, sums_recv, 2 * other + L_CORE, z)

        start(3)
        start(7)

    def center(slot, half=None):
        for c in range(4):
            at = slice(512 * c, 512 * (c + 1))
            m = mean_out[:, at]
            for r in range(8) if half is None else range(4 * half, 4 * half + 4):
                rows = slice(32 * r, 32 * (r + 1))
                blocks[6 + slot, rows, at] = (blocks[slot, rows, at].astype(F32) - m).astype(BF16)

    def late_mean():
        arrived(plane_sums.at[0:15], sums_recv, "w_sums")
        mean = plane_sums[0]
        for u in range(1, 16):
            mean = mean + plane_sums[u]
        mean_out[...] = mean / 4096.0
        means[z] = mean_out[...]
        send(mean_out, means.at[z], pair_send.at[1], mean_recv, k_dev, z)
        for dz in (1, 2, 3):
            send(mean_out, means.at[z], mean_send, mean_recv, k_dev, level(dz))
            send(mean_out, means.at[z], mean_send, mean_recv, l_dev, level(dz))
        center(0)
        product(0)

    dims = (((1,), (1,)), ((), ()))

    ready = 6 * (1 - core)

    def sides(t):
        a, b, half = TILES[t]
        if half in ("x", "y"):
            half = (x if half == "x" else y) // 2
            return a + half * (b - a), b + half * (a - b), half
        return a, b, half

    def product(t):
        a, b, half = sides(t)
        with jax.named_scope(f"dot{t}"):
            if t < WHOLE:
                gram[t] = lax.dot_general(blocks[a + ready], blocks[b + ready], dims, preferred_element_type=F32)
            else:
                top = pl.ds(pl.multiple_of(128 * half, 128), 128)
                gram[t, 0:128, :] = lax.dot_general(
                    blocks[a + ready, top, :], blocks[b + ready], dims, preferred_element_type=F32
                )
        if t == 0:
            src, dst, size, out, into, pair = gram.at[0], parts0, 64, part0_send, part0_recv, 2
        elif t < WHOLE:
            src, dst, size, out, into, pair = stage.at[t - 1], parts.at[t - 1], 64, part_send, part_recv.at[t - 1], 3
            stage[t - 1] = gram[t].astype(BF16)
        else:
            n = t - WHOLE
            src, dst, size, out, into, pair = halves.at[n], half_parts.at[n], 32, half_send, part_recv.at[t - 1], 4
            halves[n] = gram[t, 0:128, :].astype(BF16)
        for dz in (2, 1, 3):
            to = level(dz)
            rows = pl.ds(pl.multiple_of(size * to, size), size)
            send(src.at[rows, :], dst.at[dz - 1 + 4 * (1 - core)], out, into, k_dev, to)

        @pl.when(is_l)
        def _():
            rows = pl.ds(pl.multiple_of(size * z, size), size)
            send(src.at[rows, :], dst.at[3], pair_send.at[pair], into, k_dev, z)

    def settle(t):
        _, b, _ = sides(t)
        if t == 0:
            size, buf, sem = 64, parts0, part0_recv
        elif t < WHOLE:
            size, buf, sem = 64, parts.at[t - 1], part_recv.at[t - 1]
        else:
            size, buf, sem = 32, half_parts.at[t - WHOLE], part_recv.at[t - 1]
        arrived(buf, sem, f"wp{t}")
        part = [buf[n].astype(F32) for n in range(7)]
        rows = pl.ds(pl.multiple_of(size * z, size), size)
        k = gram[t, rows, :] + ((part[0] + part[1]) + part[2])
        l = (part[3] + part[4]) + (part[5] + part[6])
        h = k * l
        lane = lax.broadcasted_iota(jnp.int32, (size, 128), 1)
        own = jnp.where(lane == t, jnp.sum(h, axis=1, keepdims=True), 0.0)
        weight = 1.0
        if t:
            weight = 2.0
            across = jnp.sum(h, axis=0, keepdims=True)
            col_acc[...] += jnp.where(slot_row == b, across, 0.0)
        if t < WHOLE:
            row_cols[...] += own
        else:
            half_cols[...] += own
        acc[0, 0:size] += weight * (k * k)
        acc[1, 0:size] += weight * (l * l)
        acc[2, 0:size] += weight * h

    slot_row = lax.broadcasted_iota(jnp.int32, (8, 256), 0)

    @pl.when(is_k)
    def _():
        acc[...] = jnp.zeros_like(acc)
        row_cols[...] = jnp.zeros_like(row_cols)
        half_cols[...] = jnp.zeros_like(half_cols)
        col_acc[...] = jnp.zeros_like(col_acc)
        product(0)
        for j in range(PIECES):
            take(1, j)
            forward(1, 4, j, 0, 3)
            if j % 2 == 0:
                forward(1, 3, j, 0, 1)
            take(2, j)
            forward(2, 5, j, 3, 0)
            if j % 2:
                forward(2, 3, j, 1, 0)
            if j == 3:
                product(4)
                product(6)

    @pl.when(is_l)
    def _():
        def from_1(j):
            take(1, j)
            forward(1, 4, j, 0, 3)
            if j == DETOUR[1]:
                forward(1, 3, j, 0, 1)

        def from_2(j):
            take(2, j)
            forward(2, 5, j, 3, 0)
            if j == DETOUR[0]:
                forward(2, 3, j, 1, 0)

        for near, far in ((0, 0), (4, 4), (1, 1), (2, 5), (6, 2), (3, 3), (7, 7)):
            from_1(near)
            from_2(far)
        late_mean()
        center(1, 0)
        product(4)
        center(2, 0)
        product(6)
        for j in (0, 1, 2, 3, 4, 7):
            if j % 2:
                forward(1, 3, j, 0, 1)
            else:
                forward(2, 3, j, 1, 0)
        take(3, DETOUR[0])
        forward(3, 1, DETOUR[0], 0, 3)
        take(3, DETOUR[1])
        forward(3, 2, DETOUR[1], 3, 0)
        from_2(DETOUR[1])
        from_1(DETOUR[0])
        center(1, 1)
        center(2, 1)

    for t in (5, 7, 1):
        product(t)

    @pl.when(is_k)
    def _():
        arrived(means, mean_recv, "w_mean")
        arrived(early_pieces.at[0:3], rows_recv, "w_rows")

    @pl.when(is_l)
    def _():
        arrived(means.at[0:3], mean_recv, "w_mean")
        arrived(early_pieces, rows_recv, "w_rows")

    for c in range(4):
        at = slice(2048 * c, 2048 * (c + 1))
        late_out[:, at] = (late[:, at].astype(F32) - means[c]).astype(BF16)
    low = lax.broadcasted_iota(jnp.int32, (32, 128), 1) < 64
    for u in range(16):
        p = [early_pieces[c, :, 128 * u : 128 * (u + 1)].astype(F32) for c in range(4)]
        turned = [pltpu.roll(v, 64, 1) for v in p]
        for j in range(2):
            first = jnp.where(low, p[2 * j], turned[2 * j + 1])
            second = jnp.where(low, turned[2 * j], p[2 * j + 1])
            early_out[:, 128 * (4 * u + j) : 128 * (4 * u + j + 1)] = first.astype(BF16)
            early_out[:, 128 * (4 * u + 2 + j) : 128 * (4 * u + 3 + j)] = second.astype(BF16)
    put_e = pltpu.make_async_copy(early_out, eout_hbm, out_sem.at[0])
    put_l = pltpu.make_async_copy(late_out, lout_hbm, out_sem.at[1])
    put_e.start()
    put_l.start()

    for j in range(4):
        take(3, j)
    pl.when(is_l)(lambda: center(3, 0))
    product(8)
    for slot, t in ((4, 2), (5, 3)):
        for j in range(PIECES):
            take(slot, j)
        pl.when(is_l)(lambda: center(slot))
        product(t)
    product(10)
    for j in range(4, PIECES):
        if j in DETOUR:
            pl.when(is_k)(lambda: take(3, j))
        else:
            take(3, j)
    pl.when(is_l)(lambda: center(3, 1))
    for t in (9, 11, 12):
        product(t)

    @pl.when(is_k)
    def _():
        for t in (0, 4, 6, 5, 7, 1, 8, 2, 3):
            settle(t)
        turned = jnp.concatenate([row_cols[...]] * 2, axis=0).T
        turned = jnp.concatenate([turned] * 2, axis=1)
        for t in (10, 9, 11, 12):
            settle(t)
        half_turned = jnp.concatenate([half_cols[...]] * 4, axis=0).T
        half_turned = jnp.concatenate([half_turned] * 2, axis=1)
        col = lax.broadcasted_iota(jnp.int32, (1, 256), 1)
        both = col_acc[...]
        for t in range(len(TILES)):
            a, _, half = sides(t)
            if t < WHOLE:
                row = jnp.where(col // 64 == z, turned[t : t + 1, :], 0.0)
            else:
                row = jnp.where(col // 32 == 4 * half + z, half_turned[t : t + 1, :], 0.0)
            both = both + jnp.where(slot_row == a, row, 0.0)
        scal_lane = lax.broadcasted_iota(jnp.int32, (1, 128), 1)
        scal = jnp.zeros((1, 128), F32)
        for j in range(3):
            s = jnp.sum(jnp.sum(acc[j], axis=0, keepdims=True), axis=1, keepdims=True)
            scal = jnp.where(scal_lane == j, s, scal)
        for dx in range(4):
            for dy in range(4):
                r = 4 * dx + dy
                if (dx, dy) in SLOTS:
                    slot = SLOTS.index((dx, dy))
                    msg[r, :, 0:256] = both[slot : slot + 1, :]
                else:
                    msg[r, :, 0:256] = jnp.zeros((1, 256), F32)
                msg[r, :, 256:384] = scal
        for dx, dy, dz in EVERYONE:
            r = 4 * dx + dy
            there = msg_in.at[16 * dz + r]
            chip_there = 2 * chip_at(dx, dy)
            if dx or dy or dz:
                send(msg.at[r], there, msg_send.at[K_CORE], msg_recv, chip_there + K_CORE, level(dz))
            send(msg.at[r], there, msg_send.at[L_CORE], msg_recv, chip_there + L_CORE, level(dz))
        msg_in[0] = msg[0]
        arrived(msg_in.at[0:63], msg_recv, "w_msg")

    @pl.when(is_l)
    def _():
        arrived(msg_in, msg_recv, "w_msg")

    rows = [msg_in[r] for r in range(64)]
    while len(rows) > 1:
        rows = [a + b for a, b in zip(rows[0::2], rows[1::2])]
    final = rows[0]
    scal_lane = lax.broadcasted_iota(jnp.int32, (1, 128), 1)
    scal = final[:, 256:384]
    kk, ll, kl = (jnp.sum(jnp.where(scal_lane == j, scal, 0.0), axis=1, keepdims=True) for j in range(3))
    norm = jnp.sqrt(kk * ll)
    sim_ref[...] = kl / norm
    half = jnp.where(core == 0, final[:, 0:128], final[:, 128:256])
    tokens = half
    for j in (1, 2, 3):
        tokens = jnp.where(z == j, pltpu.roll(half, 128 - 32 * j, 1), tokens)
    share_ref[...] = (4096.0 * tokens / norm)[:, 0:32]

    with jax.named_scope("end"):
        put_e.wait()
    put_l.wait()
    left(late.at[:, 0:6144], late_send)
    left(cen.at[0:15], early_send)
    left(blocks.at[1:6], gather_send)
    left(parts.at[:, 0:3], part_send)
    left(half_parts.at[:, 0:3], half_send)
    left(parts0.at[0:3], part0_send)

    @pl.when(is_k)
    def _():
        left(late.at[:, 0:2048], pair_send.at[0])
        left(early_pieces.at[0], pair_send.at[1])
        left(blocks.at[0, 0:192, :], rows_send)
        left(msg_in.at[0:63], msg_send.at[K_CORE])
        left(msg_in, msg_send.at[L_CORE])

    @pl.when(is_l)
    def _():
        left(cen.at[0], pair_send.at[0])
        left(mean_out, pair_send.at[1])
        left(parts0.at[0], pair_send.at[2])
        left(parts.at[:, 0], pair_send.at[3])
        left(half_parts.at[:, 0], pair_send.at[4])
        left(plane_sums.at[0:15], sums_send)
        left(plane_sums.at[0:6], mean_send)


def publish(share_in, sim_in, early_in, late_in, share, sim, early, late, bufs, share_buf, sim_buf, in_sem, out_sem):
    ways = (
        (early_in, bufs.at[0], early),
        (late_in, bufs.at[1], late),
        (share_in, share_buf, share),
        (sim_in, sim_buf, sim),
    )
    gets = [pltpu.make_async_copy(a, b, in_sem.at[n]) for n, (a, b, _) in enumerate(ways)]
    puts = [pltpu.make_async_copy(b, c, out_sem.at[n]) for n, (_, b, c) in enumerate(ways)]
    for get in gets:
        get.start()
    for get, put in zip(gets, puts):
        get.wait()
        put.start()
    for put in puts:
        put.wait()


def body(layer_early, layer_late):
    vm = pltpu.VMEM
    dma = pltpu.SemaphoreType.DMA
    hbm = pl.BlockSpec(memory_space=pltpu.HBM)
    whole = pl.BlockSpec(memory_space=pltpu.VMEM)
    share, sim, early_rows, late_rows = pl.pallas_call(
        kernel,
        out_shape=(
            jax.ShapeDtypeStruct((1, 32), F32),
            jax.ShapeDtypeStruct((1, 1), F32),
            jax.ShapeDtypeStruct((32, 8192), BF16),
            jax.ShapeDtypeStruct((32, 8192), BF16),
        ),
        in_specs=[hbm, hbm],
        out_specs=(whole, whole, hbm, hbm),
        scratch_shapes=[
            vm((64, 4096), BF16),
            vm((32, 8192), BF16),
            vm((16, 64, 256), BF16),
            vm((32, 64, 256), BF16),
            vm((12, 256, 2048), BF16),
            vm((13, 256, 256), F32),
            vm((3, 256, 256), BF16),
            vm((3, 7, 64, 256), BF16),
            vm((9, 128, 256), BF16),
            vm((9, 7, 32, 256), BF16),
            vm((7, 64, 256), F32),
            vm((1, 2048), F32),
            vm((16, 1, 2048), F32),
            vm((1, 2048), F32),
            vm((4, 1, 2048), F32),
            vm((4, 32, 2048), BF16),
            vm((32, 8192), BF16),
            vm((32, 8192), BF16),
            vm((3, 64, 256), F32),
            vm((64, 128), F32),
            vm((32, 128), F32),
            vm((8, 256), F32),
            vm((16, 1, 384), F32),
            vm((64, 1, 384), F32),
            dma((2,)),
            dma((2,)),
            dma,
            dma((8,)),
            dma,
            dma((4,)),
            dma((5,)),
            dma,
            dma,
            dma,
            dma,
            dma,
            dma((5, PIECES)),
            dma,
            dma,
            dma,
            dma((12,)),
            dma,
            dma,
            dma,
            dma((2,)),
            dma,
        ],
        compiler_params=pltpu.CompilerParams(collective_id=0, has_side_effects=True, vmem_limit_bytes=67043328),
    )(layer_early.T, layer_late)
    share, sim, early_rows, late_rows = pl.pallas_call(
        publish,
        out_shape=(
            jax.ShapeDtypeStruct((1, 32), F32),
            jax.ShapeDtypeStruct((1, 1), F32),
            jax.ShapeDtypeStruct((32, 8192), BF16),
            jax.ShapeDtypeStruct((32, 8192), BF16),
        ),
        in_specs=[hbm] * 4,
        out_specs=(hbm,) * 4,
        scratch_shapes=[
            vm((2, 32, 8192), BF16),
            vm((1, 32), F32),
            vm((1, 1), F32),
            dma((4,)),
            dma((4,)),
        ],
    )(share, sim, early_rows, late_rows)
    return sim.reshape(()), share.reshape(32), early_rows, late_rows


def solution(mesh):
    return jax.shard_map(
        body,
        mesh=mesh,
        in_specs=(P(None, ("gx", "gy")), P(("gx", "gy"), None)),
        out_specs=(P(), P(("gx", "gy")), P(("gx", "gy"), None), P(("gx", "gy"), None)),
        check_vma=False,
    )
```

```python
import jax
import jax.numpy as jnp
from jax import lax
from jax.experimental import pallas as pl
from jax.experimental.pallas import tpu as pltpu
from jax.sharding import PartitionSpec as P

MESH = pl.DeviceIdType.MESH
F32 = jnp.float32
BF16 = jnp.bfloat16

SLOTS = ((0, 0), (1, 0), (0, 1), (1, 1), (1, 3), (3, 1))
TILES = (
    (0, 0, None),
    (1, 2, None),
    (4, 2, None),
    (5, 1, None),
    (1, 0, 0),
    (1, 0, 1),
    (2, 0, 0),
    (2, 0, 1),
    (3, 0, 0),
    (3, 0, 1),
    (4, 5, "x"),
    (3, 5, "x"),
    (3, 4, "y"),
)
WHOLE = 4
K_CORE = 1
L_CORE = 0
PIECES = 8
DETOUR = (5, 6)
ORDER = ((0, 0), (2, 0), (1, 0), (3, 0), (0, 1), (2, 1), (1, 1), (3, 1))
EVERYONE = sorted(
    [(dx, dy, dz) for dx in range(4) for dy in range(4) for dz in range(4)],
    key=lambda d: -sum(min(v, 4 - v) for v in d),
)
OTHERS = tuple((dx, dy) for dx in (2, 1, 3, 0) for dy in (2, 1, 3, 0) if dx or dy)


def send(src, dst, send_sem, recv_sem, gx, gy):
    pltpu.make_async_remote_copy(
        src_ref=src,
        dst_ref=dst,
        send_sem=send_sem,
        recv_sem=recv_sem,
        device_id=(gx, gy),
        device_id_type=MESH,
    ).start()


def kernel(
    xt_hbm,
    late_hbm,
    share_ref,
    sim_ref,
    eout_hbm,
    lout_hbm,
    xt,
    late,
    cen,
    rt,
    blocks,
    gram,
    stage,
    parts,
    halves,
    half_parts,
    parts0,
    own_sum,
    plane_sums,
    mean_out,
    means,
    early_pieces,
    early_out,
    late_out,
    acc,
    row_cols,
    col_acc,
    msg,
    msg_in,
    load_sem,
    out_sem,
    late_send,
    late_recv,
    early_send,
    early_recv,
    pair_send,
    sums_send,
    sums_recv,
    mean_send,
    mean_recv,
    gather_send,
    gather_recv,
    rows_send,
    rows_recv,
    part_send,
    part_recv,
    half_send,
    part0_send,
    part0_recv,
    msg_send,
    msg_recv,
):
    gx = lax.axis_index("gx")
    z = lax.axis_index("gy")
    core = lax.rem(gx, 2)
    chip = gx // 2
    x = chip // 4
    y = lax.rem(chip, 4)
    partner = gx + 1 - 2 * core
    k_dev = 2 * chip + K_CORE
    l_dev = 2 * chip + L_CORE
    is_k = core == K_CORE
    is_l = core == L_CORE

    def arrived(ref, sem, name="wait"):
        with jax.named_scope(name):
            pltpu.make_async_remote_copy(
                src_ref=ref, dst_ref=ref, send_sem=sem, recv_sem=sem, device_id=(partner, z), device_id_type=MESH
            ).wait_recv()

    def left(ref, sem):
        pltpu.make_async_remote_copy(
            src_ref=ref, dst_ref=ref, send_sem=sem, recv_sem=sem, device_id=(partner, z), device_id_type=MESH
        ).wait_send()

    def chip_at(dx, dy):
        return lax.rem(x + dx, 4) * 4 + lax.rem(y + dy, 4)

    def level(dz):
        return lax.rem(z + dz, 4)

    load_x = pltpu.make_async_copy(xt_hbm, xt, load_sem.at[0])
    load_y = pltpu.make_async_copy(late_hbm, late, load_sem.at[1])
    load_x.start()
    load_y.start()
    barrier = pltpu.get_barrier_semaphore()

    for dx, dy in OTHERS:
        other = chip_at(dx, dy)
        pl.semaphore_signal(barrier, inc=1, device_id=(2 * other + core, z), device_id_type=MESH)

    @pl.when(is_k)
    def _():
        for dx, dy in OTHERS:
            other = chip_at(dx, dy)
            pl.semaphore_signal(barrier, inc=1, device_id=(2 * other + L_CORE, z), device_id_type=MESH)

    for dz in (1, 2, 3):
        pl.semaphore_signal(barrier, inc=1, device_id=(2 * chip, level(dz)), device_id_type=MESH)
        pl.semaphore_signal(barrier, inc=1, device_id=(2 * chip + 1, level(dz)), device_id_type=MESH)
    pl.semaphore_signal(barrier, inc=1, device_id=(partner, z), device_id_type=MESH)

    with jax.named_scope("load"):
        load_x.wait()

    sums = jnp.zeros((64, 256), F32)
    for u in range(16):
        sums = sums + xt[:, 256 * u : 256 * (u + 1)].astype(F32)
    col_mean = jnp.sum(sums, axis=1, keepdims=True) / 4096.0
    for u in range(16):
        cen[u] = (xt[:, 256 * u : 256 * (u + 1)].astype(F32) - col_mean).astype(BF16)
    load_y.wait()

    with jax.named_scope("barrier"):
        pl.semaphore_wait(barrier, 22 + 15 * (1 - core))

    def piece(j):
        dz, q = ORDER[j]
        return pl.ds(pl.multiple_of(32 * (4 * q + level(dz)), 32), 32)

    my_rows = pl.ds(pl.multiple_of(32 * (4 * core + z), 32), 32)
    for dz in (2, 1, 3):
        to = level(dz)
        send(
            late.at[:, pl.ds(pl.multiple_of(2048 * to, 2048), 2048)],
            blocks.at[0, my_rows, :],
            late_send,
            late_recv.at[2 * (4 - dz) + core],
            l_dev,
            to,
        )
    own_cols = pl.ds(pl.multiple_of(2048 * z, 2048), 2048)

    for dx, dy in OTHERS:
        other = chip_at(dx, dy)
        send(cen.at[other], rt.at[gx], early_send, early_recv.at[x], 2 * other + K_CORE, z)

    def forward(src, dst, j, ex, ey):
        to = 2 * chip_at(4 - ex, 4 - ey) + core
        rows = piece(j)
        send(blocks.at[src, rows, :], blocks.at[dst, rows, :], gather_send, gather_recv.at[dst - 1, j], to, z)

    def take(slot, j):
        arrived(blocks.at[slot, piece(j), :], gather_recv.at[slot - 1, j], f"g{slot}_{j}")

    @pl.when(is_k)
    def _():
        send(late.at[:, own_cols], blocks.at[0, my_rows, :], pair_send.at[0], late_recv.at[1], l_dev, z)
        rt[gx] = cen[chip]
        for dx in (2, 1, 3, 0):
            xs = lax.rem(x + dx, 4)
            arrived(rt.at[0 : 8 if dx else 7], early_recv.at[xs], f"w_early{dx}")

            @pl.loop(0, 4)
            def _(k):
                u = 4 * xs + k
                cols = jnp.concatenate([rt[2 * u].astype(F32), rt[2 * u + 1].astype(F32)], axis=0)
                at = pl.ds(pl.multiple_of(128 * u, 128), 128)
                blocks[0, :, at] = cols.T.astype(BF16)

        for j in range(PIECES):
            forward(0, 1, j, 1, 0)
            forward(0, 2, j, 0, 1)
        for dz in (1, 2, 3):
            for q in (0, 1):
                rows = pl.ds(pl.multiple_of(32 * (4 * q + level(dz)), 32), 32)
                send(blocks.at[0, rows, :], early_pieces.at[z], rows_send, rows_recv, 2 * chip + q, level(dz))
        rows = pl.ds(pl.multiple_of(32 * (4 * L_CORE + z), 32), 32)
        send(blocks.at[0, rows, :], early_pieces.at[z], pair_send.at[1], rows_recv, l_dev, z)
        early_pieces[z] = blocks[0, my_rows, :]

    def start(j):
        if j != DETOUR[1]:
            forward(0, 2, j, 0, 1)
        if j != DETOUR[0]:
            forward(0, 1, j, 1, 0)

    @pl.when(is_l)
    def _():
        send(cen.at[chip], rt.at[gx], pair_send.at[0], early_recv.at[x], k_dev, z)
        blocks[0, my_rows, :] = late[:, own_cols]
        for n, j in enumerate((0, 4, 1, 5, 2, 6, 3, 7)):
            if j:
                arrived(blocks.at[0, piece(j), :], late_recv.at[2 * ORDER[j][0] + ORDER[j][1]], f"w_late{j}")
            if n < 6:
                start(j)
        for c in range(4):
            at = slice(512 * c, 512 * (c + 1))
            part = jnp.zeros((32, 512), F32)
            for r in range(8):
                part = part + blocks[0, 32 * r : 32 * (r + 1), at].astype(F32)
            own_sum[:, at] = jnp.sum(part, axis=0, keepdims=True)
        plane_sums[chip] = own_sum[...]

        @pl.loop(1, 16)
        def _(r):
            other = lax.rem(chip + r, 16)
            send(own_sum, plane_sums.at[chip], sums_send, sums_recv, 2 * other + L_CORE, z)

        start(3)
        start(7)

    def center(slot, half=None):
        for c in range(4):
            at = slice(512 * c, 512 * (c + 1))
            m = mean_out[:, at]
            for r in range(8) if half is None else range(4 * half, 4 * half + 4):
                rows = slice(32 * r, 32 * (r + 1))
                blocks[6 + slot, rows, at] = (blocks[slot, rows, at].astype(F32) - m).astype(BF16)

    def late_mean():
        arrived(plane_sums.at[0:15], sums_recv, "w_sums")
        mean = plane_sums[0]
        for u in range(1, 16):
            mean = mean + plane_sums[u]
        mean_out[...] = mean / 4096.0
        means[z] = mean_out[...]
        send(mean_out, means.at[z], pair_send.at[1], mean_recv, k_dev, z)
        for dz in (1, 2, 3):
            send(mean_out, means.at[z], mean_send, mean_recv, k_dev, level(dz))
            send(mean_out, means.at[z], mean_send, mean_recv, l_dev, level(dz))
        center(0)
        product(0)

    dims = (((1,), (1,)), ((), ()))

    ready = 6 * (1 - core)

    def sides(t):
        a, b, half = TILES[t]
        if half in ("x", "y"):
            half = (x if half == "x" else y) // 2
            return a + half * (b - a), b + half * (a - b), half
        return a, b, half

    def product(t):
        a, b, half = sides(t)
        with jax.named_scope(f"dot{t}"):
            if t < WHOLE:
                gram[t] = lax.dot_general(blocks[a + ready], blocks[b + ready], dims, preferred_element_type=F32)
            else:
                top = pl.ds(pl.multiple_of(128 * half, 128), 128)
                gram[t, :, 0:128] = lax.dot_general(
                    blocks[b + ready], blocks[a + ready, top, :], dims, preferred_element_type=F32
                )
        if t == 0:
            src, dst, out, into, pair = gram.at[0], parts0, part0_send, part0_recv, 2
        elif t < WHOLE:
            src, dst, out, into, pair = stage.at[t - 1], parts.at[t - 1], part_send, part_recv.at[t - 1], 3
            stage[t - 1] = gram[t].astype(BF16)
        else:
            n = t - WHOLE
            src, dst, out, into, pair = halves.at[n], half_parts.at[n], half_send, part_recv.at[t - 1], 4
            halves[n] = gram[t, :, 0:128].astype(BF16)
        for dz in (2, 1, 3):
            to = level(dz)
            rows = pl.ds(pl.multiple_of(64 * to, 64), 64)
            send(src.at[rows, :], dst.at[dz - 1 + 4 * (1 - core)], out, into, k_dev, to)

        @pl.when(is_l)
        def _():
            rows = pl.ds(pl.multiple_of(64 * z, 64), 64)
            send(src.at[rows, :], dst.at[3], pair_send.at[pair], into, k_dev, z)

    def settle(t):
        a, b, half = sides(t)
        wide = 256 if t < WHOLE else 128
        if t == 0:
            buf, sem = parts0, part0_recv
        elif t < WHOLE:
            buf, sem = parts.at[t - 1], part_recv.at[t - 1]
        else:
            buf, sem = half_parts.at[t - WHOLE], part_recv.at[t - 1]
        arrived(buf, sem, f"wp{t}")
        part = [buf[n].astype(F32) for n in range(7)]
        rows = pl.ds(pl.multiple_of(64 * z, 64), 64)
        k = gram[t, rows, 0:wide] + ((part[0] + part[1]) + part[2])
        l = (part[3] + part[4]) + (part[5] + part[6])
        h = k * l
        lane = lax.broadcasted_iota(jnp.int32, (64, 128), 1)
        row_cols[...] += jnp.where(lane == t, jnp.sum(h, axis=1, keepdims=True), 0.0)
        weight = 1.0
        if t:
            weight = 2.0
            across = jnp.sum(h, axis=0, keepdims=True)
            to = b
            if t >= WHOLE:
                side = lax.broadcasted_iota(jnp.int32, (1, 256), 1) // 128
                across = jnp.where(side == half, jnp.concatenate([across] * 2, axis=1), 0.0)
                to = a
            col_acc[...] += jnp.where(slot_row == to, across, 0.0)
        acc[0, :, 0:wide] += weight * (k * k)
        acc[1, :, 0:wide] += weight * (l * l)
        acc[2, :, 0:wide] += weight * h

    slot_row = lax.broadcasted_iota(jnp.int32, (8, 256), 0)

    @pl.when(is_k)
    def _():
        acc[...] = jnp.zeros_like(acc)
        row_cols[...] = jnp.zeros_like(row_cols)
        col_acc[...] = jnp.zeros_like(col_acc)
        product(0)
        for j in range(PIECES):
            take(1, j)
            forward(1, 4, j, 0, 3)
            if j % 2 == 0:
                forward(1, 3, j, 0, 1)
            take(2, j)
            forward(2, 5, j, 3, 0)
            if j % 2:
                forward(2, 3, j, 1, 0)
            if j == 3:
                product(4)
                product(6)

    @pl.when(is_l)
    def _():
        def from_1(j):
            take(1, j)
            forward(1, 4, j, 0, 3)
            if j == DETOUR[1]:
                forward(1, 3, j, 0, 1)

        def from_2(j):
            take(2, j)
            forward(2, 5, j, 3, 0)
            if j == DETOUR[0]:
                forward(2, 3, j, 1, 0)

        for near, far in ((0, 0), (4, 4), (1, 1), (2, 5), (6, 2), (3, 3), (7, 7)):
            from_1(near)
            from_2(far)
        late_mean()
        center(1, 0)
        product(4)
        center(2, 0)
        product(6)
        for j in (0, 1, 2, 3, 4, 7):
            if j % 2:
                forward(1, 3, j, 0, 1)
            else:
                forward(2, 3, j, 1, 0)
        take(3, DETOUR[0])
        forward(3, 1, DETOUR[0], 0, 3)
        take(3, DETOUR[1])
        forward(3, 2, DETOUR[1], 3, 0)
        from_2(DETOUR[1])
        from_1(DETOUR[0])
        center(1, 1)
        center(2, 1)

    for t in (5, 7, 1):
        product(t)

    @pl.when(is_k)
    def _():
        arrived(means, mean_recv, "w_mean")
        arrived(early_pieces.at[0:3], rows_recv, "w_rows")

    @pl.when(is_l)
    def _():
        arrived(means.at[0:3], mean_recv, "w_mean")
        arrived(early_pieces, rows_recv, "w_rows")

    for c in range(4):
        at = slice(2048 * c, 2048 * (c + 1))
        late_out[:, at] = (late[:, at].astype(F32) - means[c]).astype(BF16)
    low = lax.broadcasted_iota(jnp.int32, (32, 128), 1) < 64
    for u in range(16):
        p = [early_pieces[c, :, 128 * u : 128 * (u + 1)].astype(F32) for c in range(4)]
        turned = [pltpu.roll(v, 64, 1) for v in p]
        for j in range(2):
            first = jnp.where(low, p[2 * j], turned[2 * j + 1])
            second = jnp.where(low, turned[2 * j], p[2 * j + 1])
            early_out[:, 128 * (4 * u + j) : 128 * (4 * u + j + 1)] = first.astype(BF16)
            early_out[:, 128 * (4 * u + 2 + j) : 128 * (4 * u + 3 + j)] = second.astype(BF16)
    put_e = pltpu.make_async_copy(early_out, eout_hbm, out_sem.at[0])
    put_l = pltpu.make_async_copy(late_out, lout_hbm, out_sem.at[1])
    put_e.start()
    put_l.start()

    for j in range(4):
        take(3, j)
    pl.when(is_l)(lambda: center(3, 0))
    product(8)
    for slot, t in ((4, 2), (5, 3)):
        for j in range(PIECES):
            take(slot, j)
        pl.when(is_l)(lambda: center(slot))
        product(t)
    product(10)
    for j in range(4, PIECES):
        if j in DETOUR:
            pl.when(is_k)(lambda: take(3, j))
        else:
            take(3, j)
    pl.when(is_l)(lambda: center(3, 1))
    for t in (9, 11, 12):
        product(t)

    @pl.when(is_k)
    def _():
        for t in (0, 4, 6, 5, 7, 1, 8, 2, 3, 10, 9, 11, 12):
            settle(t)
        turned = jnp.concatenate([row_cols[...]] * 2, axis=0).T
        turned = jnp.concatenate([turned] * 2, axis=1)
        mine = lax.broadcasted_iota(jnp.int32, (1, 256), 1) // 64 == z
        both = col_acc[...]
        for t in range(len(TILES)):
            a, b, _ = sides(t)
            row = jnp.where(mine, turned[t : t + 1, :], 0.0)
            both = both + jnp.where(slot_row == (a if t < WHOLE else b), row, 0.0)
        scal_lane = lax.broadcasted_iota(jnp.int32, (1, 128), 1)
        scal = jnp.zeros((1, 128), F32)
        for j in range(3):
            s = jnp.sum(jnp.sum(acc[j], axis=0, keepdims=True), axis=1, keepdims=True)
            scal = jnp.where(scal_lane == j, s, scal)
        for dx in range(4):
            for dy in range(4):
                r = 4 * dx + dy
                if (dx, dy) in SLOTS:
                    slot = SLOTS.index((dx, dy))
                    msg[r, :, 0:256] = both[slot : slot + 1, :]
                else:
                    msg[r, :, 0:256] = jnp.zeros((1, 256), F32)
                msg[r, :, 256:384] = scal
        for dx, dy, dz in EVERYONE:
            r = 4 * dx + dy
            there = msg_in.at[16 * dz + r]
            chip_there = 2 * chip_at(dx, dy)
            if dx or dy or dz:
                send(msg.at[r], there, msg_send.at[K_CORE], msg_recv, chip_there + K_CORE, level(dz))
            send(msg.at[r], there, msg_send.at[L_CORE], msg_recv, chip_there + L_CORE, level(dz))
        msg_in[0] = msg[0]
        arrived(msg_in.at[0:63], msg_recv, "w_msg")

    @pl.when(is_l)
    def _():
        arrived(msg_in, msg_recv, "w_msg")

    rows = [msg_in[r] for r in range(64)]
    while len(rows) > 1:
        rows = [a + b for a, b in zip(rows[0::2], rows[1::2])]
    final = rows[0]
    scal_lane = lax.broadcasted_iota(jnp.int32, (1, 128), 1)
    scal = final[:, 256:384]
    kk, ll, kl = (jnp.sum(jnp.where(scal_lane == j, scal, 0.0), axis=1, keepdims=True) for j in range(3))
    norm = jnp.sqrt(kk * ll)
    sim_ref[...] = kl / norm
    half = jnp.where(core == 0, final[:, 0:128], final[:, 128:256])
    tokens = half
    for j in (1, 2, 3):
        tokens = jnp.where(z == j, pltpu.roll(half, 128 - 32 * j, 1), tokens)
    share_ref[...] = (4096.0 * tokens / norm)[:, 0:32]

    with jax.named_scope("end"):
        put_e.wait()
    put_l.wait()
    left(late.at[:, 0:6144], late_send)
    left(cen.at[0:15], early_send)
    left(blocks.at[1:6], gather_send)
    left(parts.at[:, 0:3], part_send)
    left(half_parts.at[:, 0:3], half_send)
    left(parts0.at[0:3], part0_send)

    @pl.when(is_k)
    def _():
        left(late.at[:, 0:2048], pair_send.at[0])
        left(early_pieces.at[0], pair_send.at[1])
        left(blocks.at[0, 0:192, :], rows_send)
        left(msg_in.at[0:63], msg_send.at[K_CORE])
        left(msg_in, msg_send.at[L_CORE])

    @pl.when(is_l)
    def _():
        left(cen.at[0], pair_send.at[0])
        left(mean_out, pair_send.at[1])
        left(parts0.at[0], pair_send.at[2])
        left(parts.at[:, 0], pair_send.at[3])
        left(half_parts.at[:, 0], pair_send.at[4])
        left(plane_sums.at[0:15], sums_send)
        left(plane_sums.at[0:6], mean_send)


def publish(share_in, sim_in, early_in, late_in, share, sim, early, late, bufs, share_buf, sim_buf, in_sem, out_sem):
    ways = (
        (early_in, bufs.at[0], early),
        (late_in, bufs.at[1], late),
        (share_in, share_buf, share),
        (sim_in, sim_buf, sim),
    )
    gets = [pltpu.make_async_copy(a, b, in_sem.at[n]) for n, (a, b, _) in enumerate(ways)]
    puts = [pltpu.make_async_copy(b, c, out_sem.at[n]) for n, (_, b, c) in enumerate(ways)]
    for get in gets:
        get.start()
    for get, put in zip(gets, puts):
        get.wait()
        put.start()
    for put in puts:
        put.wait()


def body(layer_early, layer_late):
    vm = pltpu.VMEM
    dma = pltpu.SemaphoreType.DMA
    hbm = pl.BlockSpec(memory_space=pltpu.HBM)
    whole = pl.BlockSpec(memory_space=pltpu.VMEM)
    share, sim, early_rows, late_rows = pl.pallas_call(
        kernel,
        out_shape=(
            jax.ShapeDtypeStruct((1, 32), F32),
            jax.ShapeDtypeStruct((1, 1), F32),
            jax.ShapeDtypeStruct((32, 8192), BF16),
            jax.ShapeDtypeStruct((32, 8192), BF16),
        ),
        in_specs=[hbm, hbm],
        out_specs=(whole, whole, hbm, hbm),
        scratch_shapes=[
            vm((64, 4096), BF16),
            vm((32, 8192), BF16),
            vm((16, 64, 256), BF16),
            vm((32, 64, 256), BF16),
            vm((12, 256, 2048), BF16),
            vm((13, 256, 256), F32),
            vm((3, 256, 256), BF16),
            vm((3, 7, 64, 256), BF16),
            vm((9, 256, 128), BF16),
            vm((9, 7, 64, 128), BF16),
            vm((7, 64, 256), F32),
            vm((1, 2048), F32),
            vm((16, 1, 2048), F32),
            vm((1, 2048), F32),
            vm((4, 1, 2048), F32),
            vm((4, 32, 2048), BF16),
            vm((32, 8192), BF16),
            vm((32, 8192), BF16),
            vm((3, 64, 256), F32),
            vm((64, 128), F32),
            vm((8, 256), F32),
            vm((16, 1, 384), F32),
            vm((64, 1, 384), F32),
            dma((2,)),
            dma((2,)),
            dma,
            dma((8,)),
            dma,
            dma((4,)),
            dma((5,)),
            dma,
            dma,
            dma,
            dma,
            dma,
            dma((5, PIECES)),
            dma,
            dma,
            dma,
            dma((12,)),
            dma,
            dma,
            dma,
            dma((2,)),
            dma,
        ],
        compiler_params=pltpu.CompilerParams(collective_id=0, has_side_effects=True, vmem_limit_bytes=67043328),
    )(layer_early.T, layer_late)
    share, sim, early_rows, late_rows = pl.pallas_call(
        publish,
        out_shape=(
            jax.ShapeDtypeStruct((1, 32), F32),
            jax.ShapeDtypeStruct((1, 1), F32),
            jax.ShapeDtypeStruct((32, 8192), BF16),
            jax.ShapeDtypeStruct((32, 8192), BF16),
        ),
        in_specs=[hbm] * 4,
        out_specs=(hbm,) * 4,
        scratch_shapes=[
            vm((2, 32, 8192), BF16),
            vm((1, 32), F32),
            vm((1, 1), F32),
            dma((4,)),
            dma((4,)),
        ],
    )(share, sim, early_rows, late_rows)
    return sim.reshape(()), share.reshape(32), early_rows, late_rows


def solution(mesh):
    return jax.shard_map(
        body,
        mesh=mesh,
        in_specs=(P(None, ("gx", "gy")), P(("gx", "gy"), None)),
        out_specs=(P(), P(("gx", "gy")), P(("gx", "gy"), None), P(("gx", "gy"), None)),
        check_vma=False,
    )
```

```python
import jax
import jax.numpy as jnp
from jax import lax
from jax.experimental import pallas as pl
from jax.experimental.pallas import tpu as pltpu
from jax.sharding import PartitionSpec as P

MESH = pl.DeviceIdType.MESH
F32 = jnp.float32
BF16 = jnp.bfloat16

SLOTS = ((0, 0), (1, 0), (0, 1), (1, 1), (1, 3), (3, 1))
TILES = (
    (0, 0, None),
    (1, 2, None),
    (4, 2, None),
    (5, 1, None),
    (1, 0, 0),
    (1, 0, 1),
    (2, 0, 0),
    (2, 0, 1),
    (3, 0, 0),
    (3, 0, 1),
    (4, 5, "x"),
    (3, 5, "x"),
    (3, 4, "y"),
)
WHOLE = 4
K_CORE = 1
L_CORE = 0
PIECES = 8
DETOUR = (5, 6)
ORDER = ((0, 0), (2, 0), (1, 0), (3, 0), (0, 1), (2, 1), (1, 1), (3, 1))
EVERYONE = sorted(
    [(dx, dy, dz) for dx in range(4) for dy in range(4) for dz in range(4)],
    key=lambda d: -sum(min(v, 4 - v) for v in d),
)
OTHERS = tuple((dx, dy) for dx in (2, 1, 3, 0) for dy in (2, 1, 3, 0) if dx or dy)


def send(src, dst, send_sem, recv_sem, gx, gy):
    pltpu.make_async_remote_copy(
        src_ref=src,
        dst_ref=dst,
        send_sem=send_sem,
        recv_sem=recv_sem,
        device_id=(gx, gy),
        device_id_type=MESH,
    ).start()


def kernel(
    xt_hbm,
    late_hbm,
    share_ref,
    sim_ref,
    eout_hbm,
    lout_hbm,
    xt,
    late,
    cen,
    rt,
    blocks,
    gram,
    stage,
    parts,
    halves,
    half_parts,
    parts0,
    own_sum,
    plane_sums,
    mean_out,
    means,
    early_pieces,
    early_out,
    late_out,
    acc,
    row_cols,
    half_cols,
    col_acc,
    msg,
    msg_in,
    load_sem,
    out_sem,
    late_send,
    late_recv,
    early_send,
    early_recv,
    pair_send,
    sums_send,
    sums_recv,
    mean_send,
    mean_recv,
    gather_send,
    gather_recv,
    rows_send,
    rows_recv,
    part_send,
    part_recv,
    half_send,
    part0_send,
    part0_recv,
    msg_send,
    msg_recv,
):
    gx = lax.axis_index("gx")
    z = lax.axis_index("gy")
    core = lax.rem(gx, 2)
    chip = gx // 2
    x = chip // 4
    y = lax.rem(chip, 4)
    partner = gx + 1 - 2 * core
    k_dev = 2 * chip + K_CORE
    l_dev = 2 * chip + L_CORE
    is_k = core == K_CORE
    is_l = core == L_CORE

    def arrived(ref, sem, name="wait"):
        with jax.named_scope(name):
            pltpu.make_async_remote_copy(
                src_ref=ref, dst_ref=ref, send_sem=sem, recv_sem=sem, device_id=(partner, z), device_id_type=MESH
            ).wait_recv()

    def left(ref, sem):
        pltpu.make_async_remote_copy(
            src_ref=ref, dst_ref=ref, send_sem=sem, recv_sem=sem, device_id=(partner, z), device_id_type=MESH
        ).wait_send()

    def chip_at(dx, dy):
        return lax.rem(x + dx, 4) * 4 + lax.rem(y + dy, 4)

    def level(dz):
        return lax.rem(z + dz, 4)

    load_x = pltpu.make_async_copy(xt_hbm, xt, load_sem.at[0])
    load_y = pltpu.make_async_copy(late_hbm, late, load_sem.at[1])
    load_x.start()
    load_y.start()
    barrier = pltpu.get_barrier_semaphore()

    for dx, dy in OTHERS:
        other = chip_at(dx, dy)
        pl.semaphore_signal(barrier, inc=1, device_id=(2 * other + core, z), device_id_type=MESH)

    @pl.when(is_k)
    def _():
        for dx, dy in OTHERS:
            other = chip_at(dx, dy)
            pl.semaphore_signal(barrier, inc=1, device_id=(2 * other + L_CORE, z), device_id_type=MESH)

    for dz in (1, 2, 3):
        pl.semaphore_signal(barrier, inc=1, device_id=(2 * chip, level(dz)), device_id_type=MESH)
        pl.semaphore_signal(barrier, inc=1, device_id=(2 * chip + 1, level(dz)), device_id_type=MESH)
    pl.semaphore_signal(barrier, inc=1, device_id=(partner, z), device_id_type=MESH)

    with jax.named_scope("load"):
        load_x.wait()

    sums = jnp.zeros((64, 256), F32)
    for u in range(16):
        sums = sums + xt[:, 256 * u : 256 * (u + 1)].astype(F32)
    col_mean = jnp.sum(sums, axis=1, keepdims=True) / 4096.0
    for u in range(16):
        cen[u] = (xt[:, 256 * u : 256 * (u + 1)].astype(F32) - col_mean).astype(BF16)
    load_y.wait()

    with jax.named_scope("barrier"):
        pl.semaphore_wait(barrier, 22 + 15 * (1 - core))

    def piece(j):
        dz, q = ORDER[j]
        return pl.ds(pl.multiple_of(32 * (4 * q + level(dz)), 32), 32)

    my_rows = pl.ds(pl.multiple_of(32 * (4 * core + z), 32), 32)
    for dz in (2, 1, 3):
        to = level(dz)
        send(
            late.at[:, pl.ds(pl.multiple_of(2048 * to, 2048), 2048)],
            blocks.at[0, my_rows, :],
            late_send,
            late_recv.at[2 * (4 - dz) + core],
            l_dev,
            to,
        )
    own_cols = pl.ds(pl.multiple_of(2048 * z, 2048), 2048)

    for dx, dy in OTHERS:
        other = chip_at(dx, dy)
        send(cen.at[other], rt.at[gx], early_send, early_recv.at[x], 2 * other + K_CORE, z)

    def forward(src, dst, j, ex, ey):
        to = 2 * chip_at(4 - ex, 4 - ey) + core
        rows = piece(j)
        send(blocks.at[src, rows, :], blocks.at[dst, rows, :], gather_send, gather_recv.at[dst - 1, j], to, z)

    def take(slot, j):
        arrived(blocks.at[slot, piece(j), :], gather_recv.at[slot - 1, j], f"g{slot}_{j}")

    @pl.when(is_k)
    def _():
        send(late.at[:, own_cols], blocks.at[0, my_rows, :], pair_send.at[0], late_recv.at[1], l_dev, z)
        rt[gx] = cen[chip]
        for dx in (2, 1, 3, 0):
            xs = lax.rem(x + dx, 4)
            arrived(rt.at[0 : 8 if dx else 7], early_recv.at[xs], f"w_early{dx}")

            @pl.loop(0, 4)
            def _(k):
                u = 4 * xs + k
                cols = jnp.concatenate([rt[2 * u].astype(F32), rt[2 * u + 1].astype(F32)], axis=0)
                at = pl.ds(pl.multiple_of(128 * u, 128), 128)
                blocks[0, :, at] = cols.T.astype(BF16)

        for j in range(PIECES):
            forward(0, 1, j, 1, 0)
            forward(0, 2, j, 0, 1)
        for dz in (1, 2, 3):
            for q in (0, 1):
                rows = pl.ds(pl.multiple_of(32 * (4 * q + level(dz)), 32), 32)
                send(blocks.at[0, rows, :], early_pieces.at[z], rows_send, rows_recv, 2 * chip + q, level(dz))
        rows = pl.ds(pl.multiple_of(32 * (4 * L_CORE + z), 32), 32)
        send(blocks.at[0, rows, :], early_pieces.at[z], pair_send.at[1], rows_recv, l_dev, z)
        early_pieces[z] = blocks[0, my_rows, :]

    def start(j):
        if j != DETOUR[1]:
            forward(0, 2, j, 0, 1)
        if j != DETOUR[0]:
            forward(0, 1, j, 1, 0)

    @pl.when(is_l)
    def _():
        send(cen.at[chip], rt.at[gx], pair_send.at[0], early_recv.at[x], k_dev, z)
        blocks[0, my_rows, :] = late[:, own_cols]
        for n, j in enumerate((0, 4, 1, 5, 2, 6, 3, 7)):
            if j:
                arrived(blocks.at[0, piece(j), :], late_recv.at[2 * ORDER[j][0] + ORDER[j][1]], f"w_late{j}")
            if n < 6:
                start(j)
        for c in range(4):
            at = slice(512 * c, 512 * (c + 1))
            part = jnp.zeros((32, 512), F32)
            for r in range(8):
                part = part + blocks[0, 32 * r : 32 * (r + 1), at].astype(F32)
            own_sum[:, at] = jnp.sum(part, axis=0, keepdims=True)
        plane_sums[chip] = own_sum[...]

        @pl.loop(1, 16)
        def _(r):
            other = lax.rem(chip + r, 16)
            send(own_sum, plane_sums.at[chip], sums_send, sums_recv, 2 * other + L_CORE, z)

        start(3)
        start(7)

    def center(slot, half=None):
        for c in range(4):
            at = slice(512 * c, 512 * (c + 1))
            m = mean_out[:, at]
            for r in range(8) if half is None else range(4 * half, 4 * half + 4):
                rows = slice(32 * r, 32 * (r + 1))
                blocks[6 + slot, rows, at] = (blocks[slot, rows, at].astype(F32) - m).astype(BF16)

    def late_mean():
        arrived(plane_sums.at[0:15], sums_recv, "w_sums")
        mean = plane_sums[0]
        for u in range(1, 16):
            mean = mean + plane_sums[u]
        mean_out[...] = mean / 4096.0
        means[z] = mean_out[...]
        send(mean_out, means.at[z], pair_send.at[1], mean_recv, k_dev, z)
        for dz in (1, 2, 3):
            send(mean_out, means.at[z], mean_send, mean_recv, k_dev, level(dz))
            send(mean_out, means.at[z], mean_send, mean_recv, l_dev, level(dz))
        center(0)
        product(0)

    dims = (((1,), (1,)), ((), ()))

    ready = 6 * (1 - core)

    def sides(t):
        a, b, half = TILES[t]
        if half in ("x", "y"):
            half = (x if half == "x" else y) // 2
            return a + half * (b - a), b + half * (a - b), half
        return a, b, half

    def product(t):
        a, b, half = sides(t)
        with jax.named_scope(f"dot{t}"):
            if t < WHOLE:
                gram[t] = lax.dot_general(blocks[a + ready], blocks[b + ready], dims, preferred_element_type=F32)
            else:
                top = pl.ds(pl.multiple_of(128 * half, 128), 128)
                gram[t, 0:128, :] = lax.dot_general(
                    blocks[a + ready, top, :], blocks[b + ready], dims, preferred_element_type=F32
                )
        if t == 0:
            src, dst, size, out, into, pair = gram.at[0], parts0, 64, part0_send, part0_recv, 2
        elif t < WHOLE:
            src, dst, size, out, into, pair = stage.at[t - 1], parts.at[t - 1], 64, part_send, part_recv.at[t - 1], 3
            stage[t - 1] = gram[t].astype(BF16)
        else:
            n = t - WHOLE
            src, dst, size, out, into, pair = halves.at[n], half_parts.at[n], 32, half_send, part_recv.at[t - 1], 4
            halves[n] = gram[t, 0:128, :].astype(BF16)
        for dz in (2, 1, 3):
            to = level(dz)
            rows = pl.ds(pl.multiple_of(size * to, size), size)
            send(src.at[rows, :], dst.at[dz - 1 + 4 * (1 - core)], out, into, k_dev, to)

        @pl.when(is_l)
        def _():
            rows = pl.ds(pl.multiple_of(size * z, size), size)
            send(src.at[rows, :], dst.at[3], pair_send.at[pair], into, k_dev, z)

    def settle(t):
        _, b, _ = sides(t)
        if t == 0:
            size, buf, sem = 64, parts0, part0_recv
        elif t < WHOLE:
            size, buf, sem = 64, parts.at[t - 1], part_recv.at[t - 1]
        else:
            size, buf, sem = 32, half_parts.at[t - WHOLE], part_recv.at[t - 1]
        arrived(buf, sem, f"wp{t}")
        part = [buf[n].astype(F32) for n in range(7)]
        rows = pl.ds(pl.multiple_of(size * z, size), size)
        k = gram[t, rows, :] + ((part[0] + part[1]) + part[2])
        l = (part[3] + part[4]) + (part[5] + part[6])
        h = k * l
        lane = lax.broadcasted_iota(jnp.int32, (size, 128), 1)
        own = jnp.where(lane == t, jnp.sum(h, axis=1, keepdims=True), 0.0)
        weight = 1.0
        if t:
            weight = 2.0
            across = jnp.sum(h, axis=0, keepdims=True)
            col_acc[...] += jnp.where(slot_row == b, across, 0.0)
        if t < WHOLE:
            row_cols[...] += own
        else:
            half_cols[...] += own
        acc[0, 0:size] += weight * (k * k)
        acc[1, 0:size] += weight * (l * l)
        acc[2, 0:size] += weight * h

    slot_row = lax.broadcasted_iota(jnp.int32, (8, 256), 0)

    @pl.when(is_k)
    def _():
        acc[...] = jnp.zeros_like(acc)
        row_cols[...] = jnp.zeros_like(row_cols)
        half_cols[...] = jnp.zeros_like(half_cols)
        col_acc[...] = jnp.zeros_like(col_acc)
        product(0)
        for j in range(PIECES):
            take(1, j)
            forward(1, 4, j, 0, 3)
            if j % 2 == 0:
                forward(1, 3, j, 0, 1)
            take(2, j)
            forward(2, 5, j, 3, 0)
            if j % 2:
                forward(2, 3, j, 1, 0)
            if j == 3:
                product(4)
                product(6)

    @pl.when(is_l)
    def _():
        def from_1(j):
            take(1, j)
            forward(1, 4, j, 0, 3)
            if j == DETOUR[1]:
                forward(1, 3, j, 0, 1)

        def from_2(j):
            take(2, j)
            forward(2, 5, j, 3, 0)
            if j == DETOUR[0]:
                forward(2, 3, j, 1, 0)

        for near, far in ((0, 0), (4, 4), (1, 1), (2, 5), (6, 2), (3, 3), (7, 7)):
            from_1(near)
            from_2(far)
        late_mean()
        take(3, DETOUR[0])
        forward(3, 1, DETOUR[0], 0, 3)
        take(3, DETOUR[1])
        forward(3, 2, DETOUR[1], 3, 0)
        for j in (0, 1, 2, 3, 4, 7):
            if j % 2:
                forward(1, 3, j, 0, 1)
            else:
                forward(2, 3, j, 1, 0)
        center(1, 0)
        product(4)
        center(2, 0)
        product(6)
        from_2(DETOUR[1])
        from_1(DETOUR[0])
        center(1, 1)
        center(2, 1)

    for t in (5, 7, 1):
        product(t)

    @pl.when(is_k)
    def _():
        arrived(means, mean_recv, "w_mean")
        arrived(early_pieces.at[0:3], rows_recv, "w_rows")

    @pl.when(is_l)
    def _():
        arrived(means.at[0:3], mean_recv, "w_mean")
        arrived(early_pieces, rows_recv, "w_rows")

    for c in range(4):
        at = slice(2048 * c, 2048 * (c + 1))
        late_out[:, at] = (late[:, at].astype(F32) - means[c]).astype(BF16)
    low = lax.broadcasted_iota(jnp.int32, (32, 128), 1) < 64
    for u in range(16):
        p = [early_pieces[c, :, 128 * u : 128 * (u + 1)].astype(F32) for c in range(4)]
        turned = [pltpu.roll(v, 64, 1) for v in p]
        for j in range(2):
            first = jnp.where(low, p[2 * j], turned[2 * j + 1])
            second = jnp.where(low, turned[2 * j], p[2 * j + 1])
            early_out[:, 128 * (4 * u + j) : 128 * (4 * u + j + 1)] = first.astype(BF16)
            early_out[:, 128 * (4 * u + 2 + j) : 128 * (4 * u + 3 + j)] = second.astype(BF16)
    put_e = pltpu.make_async_copy(early_out, eout_hbm, out_sem.at[0])
    put_l = pltpu.make_async_copy(late_out, lout_hbm, out_sem.at[1])
    put_e.start()
    put_l.start()

    for j in range(4):
        take(3, j)
    pl.when(is_l)(lambda: center(3, 0))
    product(8)
    for slot, t in ((4, 2), (5, 3)):
        for j in range(PIECES):
            take(slot, j)
        pl.when(is_l)(lambda: center(slot))
        product(t)
    product(10)
    for j in range(4, PIECES):
        if j in DETOUR:
            pl.when(is_k)(lambda: take(3, j))
        else:
            take(3, j)
    pl.when(is_l)(lambda: center(3, 1))
    for t in (9, 11, 12):
        product(t)

    @pl.when(is_k)
    def _():
        for t in (0, 4, 6, 5, 7, 1, 8, 2, 3):
            settle(t)
        turned = jnp.concatenate([row_cols[...]] * 2, axis=0).T
        turned = jnp.concatenate([turned] * 2, axis=1)
        for t in (10, 9, 11, 12):
            settle(t)
        half_turned = jnp.concatenate([half_cols[...]] * 4, axis=0).T
        half_turned = jnp.concatenate([half_turned] * 2, axis=1)
        col = lax.broadcasted_iota(jnp.int32, (1, 256), 1)
        both = col_acc[...]
        for t in range(len(TILES)):
            a, _, half = sides(t)
            if t < WHOLE:
                row = jnp.where(col // 64 == z, turned[t : t + 1, :], 0.0)
            else:
                row = jnp.where(col // 32 == 4 * half + z, half_turned[t : t + 1, :], 0.0)
            both = both + jnp.where(slot_row == a, row, 0.0)
        scal_lane = lax.broadcasted_iota(jnp.int32, (1, 128), 1)
        scal = jnp.zeros((1, 128), F32)
        for j in range(3):
            s = jnp.sum(jnp.sum(acc[j], axis=0, keepdims=True), axis=1, keepdims=True)
            scal = jnp.where(scal_lane == j, s, scal)
        for dx in range(4):
            for dy in range(4):
                r = 4 * dx + dy
                if (dx, dy) in SLOTS:
                    slot = SLOTS.index((dx, dy))
                    msg[r, :, 0:256] = both[slot : slot + 1, :]
                else:
                    msg[r, :, 0:256] = jnp.zeros((1, 256), F32)
                msg[r, :, 256:384] = scal
        for dx, dy, dz in EVERYONE:
            r = 4 * dx + dy
            there = msg_in.at[16 * dz + r]
            chip_there = 2 * chip_at(dx, dy)
            if dx or dy or dz:
                send(msg.at[r], there, msg_send.at[K_CORE], msg_recv, chip_there + K_CORE, level(dz))
            send(msg.at[r], there, msg_send.at[L_CORE], msg_recv, chip_there + L_CORE, level(dz))
        msg_in[0] = msg[0]
        arrived(msg_in.at[0:63], msg_recv, "w_msg")

    @pl.when(is_l)
    def _():
        arrived(msg_in, msg_recv, "w_msg")

    rows = [msg_in[r] for r in range(64)]
    while len(rows) > 1:
        rows = [a + b for a, b in zip(rows[0::2], rows[1::2])]
    final = rows[0]
    scal_lane = lax.broadcasted_iota(jnp.int32, (1, 128), 1)
    scal = final[:, 256:384]
    kk, ll, kl = (jnp.sum(jnp.where(scal_lane == j, scal, 0.0), axis=1, keepdims=True) for j in range(3))
    norm = jnp.sqrt(kk * ll)
    sim_ref[...] = kl / norm
    half = jnp.where(core == 0, final[:, 0:128], final[:, 128:256])
    tokens = half
    for j in (1, 2, 3):
        tokens = jnp.where(z == j, pltpu.roll(half, 128 - 32 * j, 1), tokens)
    share_ref[...] = (4096.0 * tokens / norm)[:, 0:32]

    with jax.named_scope("end"):
        put_e.wait()
    put_l.wait()
    left(late.at[:, 0:6144], late_send)
    left(cen.at[0:15], early_send)
    left(blocks.at[1:6], gather_send)
    left(parts.at[:, 0:3], part_send)
    left(half_parts.at[:, 0:3], half_send)
    left(parts0.at[0:3], part0_send)

    @pl.when(is_k)
    def _():
        left(late.at[:, 0:2048], pair_send.at[0])
        left(early_pieces.at[0], pair_send.at[1])
        left(blocks.at[0, 0:192, :], rows_send)
        left(msg_in.at[0:63], msg_send.at[K_CORE])
        left(msg_in, msg_send.at[L_CORE])

    @pl.when(is_l)
    def _():
        left(cen.at[0], pair_send.at[0])
        left(mean_out, pair_send.at[1])
        left(parts0.at[0], pair_send.at[2])
        left(parts.at[:, 0], pair_send.at[3])
        left(half_parts.at[:, 0], pair_send.at[4])
        left(plane_sums.at[0:15], sums_send)
        left(plane_sums.at[0:6], mean_send)


def publish(share_in, sim_in, early_in, late_in, share, sim, early, late, bufs, share_buf, sim_buf, in_sem, out_sem):
    ways = (
        (early_in, bufs.at[0], early),
        (late_in, bufs.at[1], late),
        (share_in, share_buf, share),
        (sim_in, sim_buf, sim),
    )
    gets = [pltpu.make_async_copy(a, b, in_sem.at[n]) for n, (a, b, _) in enumerate(ways)]
    puts = [pltpu.make_async_copy(b, c, out_sem.at[n]) for n, (_, b, c) in enumerate(ways)]
    for get in gets:
        get.start()
    for get, put in zip(gets, puts):
        get.wait()
        put.start()
    for put in puts:
        put.wait()


def body(layer_early, layer_late):
    vm = pltpu.VMEM
    dma = pltpu.SemaphoreType.DMA
    hbm = pl.BlockSpec(memory_space=pltpu.HBM)
    whole = pl.BlockSpec(memory_space=pltpu.VMEM)
    share, sim, early_rows, late_rows = pl.pallas_call(
        kernel,
        out_shape=(
            jax.ShapeDtypeStruct((1, 32), F32),
            jax.ShapeDtypeStruct((1, 1), F32),
            jax.ShapeDtypeStruct((32, 8192), BF16),
            jax.ShapeDtypeStruct((32, 8192), BF16),
        ),
        in_specs=[hbm, hbm],
        out_specs=(whole, whole, hbm, hbm),
        scratch_shapes=[
            vm((64, 4096), BF16),
            vm((32, 8192), BF16),
            vm((16, 64, 256), BF16),
            vm((32, 64, 256), BF16),
            vm((12, 256, 2048), BF16),
            vm((13, 256, 256), F32),
            vm((3, 256, 256), BF16),
            vm((3, 7, 64, 256), BF16),
            vm((9, 128, 256), BF16),
            vm((9, 7, 32, 256), BF16),
            vm((7, 64, 256), F32),
            vm((1, 2048), F32),
            vm((16, 1, 2048), F32),
            vm((1, 2048), F32),
            vm((4, 1, 2048), F32),
            vm((4, 32, 2048), BF16),
            vm((32, 8192), BF16),
            vm((32, 8192), BF16),
            vm((3, 64, 256), F32),
            vm((64, 128), F32),
            vm((32, 128), F32),
            vm((8, 256), F32),
            vm((16, 1, 384), F32),
            vm((64, 1, 384), F32),
            dma((2,)),
            dma((2,)),
            dma,
            dma((8,)),
            dma,
            dma((4,)),
            dma((5,)),
            dma,
            dma,
            dma,
            dma,
            dma,
            dma((5, PIECES)),
            dma,
            dma,
            dma,
            dma((12,)),
            dma,
            dma,
            dma,
            dma((2,)),
            dma,
        ],
        compiler_params=pltpu.CompilerParams(collective_id=0, has_side_effects=True, vmem_limit_bytes=67043328),
    )(layer_early.T, layer_late)
    share, sim, early_rows, late_rows = pl.pallas_call(
        publish,
        out_shape=(
            jax.ShapeDtypeStruct((1, 32), F32),
            jax.ShapeDtypeStruct((1, 1), F32),
            jax.ShapeDtypeStruct((32, 8192), BF16),
            jax.ShapeDtypeStruct((32, 8192), BF16),
        ),
        in_specs=[hbm] * 4,
        out_specs=(hbm,) * 4,
        scratch_shapes=[
            vm((2, 32, 8192), BF16),
            vm((1, 32), F32),
            vm((1, 1), F32),
            dma((4,)),
            dma((4,)),
        ],
    )(share, sim, early_rows, late_rows)
    return sim.reshape(()), share.reshape(32), early_rows, late_rows


def solution(mesh):
    return jax.shard_map(
        body,
        mesh=mesh,
        in_specs=(P(None, ("gx", "gy")), P(("gx", "gy"), None)),
        out_specs=(P(), P(("gx", "gy")), P(("gx", "gy"), None), P(("gx", "gy"), None)),
        check_vma=False,
    )
```

```python
import jax
import jax.numpy as jnp
from jax import lax
from jax.experimental import pallas as pl
from jax.experimental.pallas import tpu as pltpu
from jax.sharding import PartitionSpec as P

MESH = pl.DeviceIdType.MESH
F32 = jnp.float32
BF16 = jnp.bfloat16

SLOTS = ((0, 0), (1, 0), (0, 1), (1, 1), (1, 3), (3, 1))
TILES = (
    (0, 0, None),
    (1, 2, None),
    (4, 2, None),
    (5, 1, None),
    (1, 0, 0),
    (1, 0, 1),
    (2, 0, 0),
    (2, 0, 1),
    (3, 0, 0),
    (3, 0, 1),
    (4, 5, "x"),
    (3, 5, "x"),
    (3, 4, "y"),
)
WHOLE = 4
K_CORE = 1
L_CORE = 0
PIECES = 8
DETOUR = (5, 6)
ORDER = ((0, 0), (2, 0), (1, 0), (3, 0), (0, 1), (2, 1), (1, 1), (3, 1))
EVERYONE = sorted(
    [(dx, dy, dz) for dx in range(4) for dy in range(4) for dz in range(4)],
    key=lambda d: -sum(min(v, 4 - v) for v in d),
)
OTHERS = tuple((dx, dy) for dx in (2, 1, 3, 0) for dy in (2, 1, 3, 0) if dx or dy)


def send(src, dst, send_sem, recv_sem, gx, gy):
    pltpu.make_async_remote_copy(
        src_ref=src,
        dst_ref=dst,
        send_sem=send_sem,
        recv_sem=recv_sem,
        device_id=(gx, gy),
        device_id_type=MESH,
    ).start()


def kernel(
    xt_hbm,
    late_hbm,
    share_ref,
    sim_ref,
    eout_hbm,
    lout_hbm,
    xt,
    late,
    cen,
    rt,
    blocks,
    gram,
    stage,
    parts,
    halves,
    half_parts,
    parts0,
    own_sum,
    plane_sums,
    mean_out,
    means,
    early_pieces,
    early_out,
    late_out,
    acc,
    row_cols,
    half_cols,
    col_acc,
    msg,
    msg_in,
    load_sem,
    out_sem,
    late_send,
    late_recv,
    early_send,
    early_recv,
    pair_send,
    sums_send,
    sums_recv,
    mean_send,
    mean_recv,
    gather_send,
    gather_recv,
    rows_send,
    rows_recv,
    part_send,
    part_recv,
    half_send,
    part0_send,
    part0_recv,
    msg_send,
    msg_recv,
):
    gx = lax.axis_index("gx")
    z = lax.axis_index("gy")
    core = lax.rem(gx, 2)
    chip = gx // 2
    x = chip // 4
    y = lax.rem(chip, 4)
    partner = gx + 1 - 2 * core
    k_dev = 2 * chip + K_CORE
    l_dev = 2 * chip + L_CORE
    is_k = core == K_CORE
    is_l = core == L_CORE

    def arrived(ref, sem, name="wait"):
        with jax.named_scope(name):
            pltpu.make_async_remote_copy(
                src_ref=ref, dst_ref=ref, send_sem=sem, recv_sem=sem, device_id=(partner, z), device_id_type=MESH
            ).wait_recv()

    def left(ref, sem):
        pltpu.make_async_remote_copy(
            src_ref=ref, dst_ref=ref, send_sem=sem, recv_sem=sem, device_id=(partner, z), device_id_type=MESH
        ).wait_send()

    def chip_at(dx, dy):
        return lax.rem(x + dx, 4) * 4 + lax.rem(y + dy, 4)

    def level(dz):
        return lax.rem(z + dz, 4)

    load_x = pltpu.make_async_copy(xt_hbm, xt, load_sem.at[0])
    load_y = pltpu.make_async_copy(late_hbm, late, load_sem.at[1])
    load_x.start()
    load_y.start()
    barrier = pltpu.get_barrier_semaphore()

    for dx, dy in OTHERS:
        other = chip_at(dx, dy)
        pl.semaphore_signal(barrier, inc=1, device_id=(2 * other + core, z), device_id_type=MESH)

    @pl.when(is_k)
    def _():
        for dx, dy in OTHERS:
            other = chip_at(dx, dy)
            pl.semaphore_signal(barrier, inc=1, device_id=(2 * other + L_CORE, z), device_id_type=MESH)

    for dz in (1, 2, 3):
        pl.semaphore_signal(barrier, inc=1, device_id=(2 * chip, level(dz)), device_id_type=MESH)
        pl.semaphore_signal(barrier, inc=1, device_id=(2 * chip + 1, level(dz)), device_id_type=MESH)
    pl.semaphore_signal(barrier, inc=1, device_id=(partner, z), device_id_type=MESH)

    with jax.named_scope("load"):
        load_x.wait()

    sums = jnp.zeros((64, 256), F32)
    for u in range(16):
        sums = sums + xt[:, 256 * u : 256 * (u + 1)].astype(F32)
    col_mean = jnp.sum(sums, axis=1, keepdims=True) / 4096.0
    for u in range(16):
        cen[u] = (xt[:, 256 * u : 256 * (u + 1)].astype(F32) - col_mean).astype(BF16)
    load_y.wait()

    with jax.named_scope("barrier"):
        pl.semaphore_wait(barrier, 22 + 15 * (1 - core))

    def piece(j):
        dz, q = ORDER[j]
        return pl.ds(pl.multiple_of(32 * (4 * q + level(dz)), 32), 32)

    my_rows = pl.ds(pl.multiple_of(32 * (4 * core + z), 32), 32)
    for dz in (2, 1, 3):
        to = level(dz)
        send(
            late.at[:, pl.ds(pl.multiple_of(2048 * to, 2048), 2048)],
            blocks.at[0, my_rows, :],
            late_send,
            late_recv.at[2 * (4 - dz) + core],
            l_dev,
            to,
        )
    own_cols = pl.ds(pl.multiple_of(2048 * z, 2048), 2048)

    for dx, dy in OTHERS:
        other = chip_at(dx, dy)
        send(cen.at[other], rt.at[gx], early_send, early_recv.at[x], 2 * other + K_CORE, z)

    def forward(src, dst, j, ex, ey):
        to = 2 * chip_at(4 - ex, 4 - ey) + core
        rows = piece(j)
        send(blocks.at[src, rows, :], blocks.at[dst, rows, :], gather_send, gather_recv.at[dst - 1, j], to, z)

    def take(slot, j):
        arrived(blocks.at[slot, piece(j), :], gather_recv.at[slot - 1, j], f"g{slot}_{j}")

    @pl.when(is_k)
    def _():
        send(late.at[:, own_cols], blocks.at[0, my_rows, :], pair_send.at[0], late_recv.at[1], l_dev, z)
        rt[gx] = cen[chip]
        for dx in (2, 1, 3, 0):
            xs = lax.rem(x + dx, 4)
            arrived(rt.at[0 : 8 if dx else 7], early_recv.at[xs], f"w_early{dx}")

            @pl.loop(0, 4)
            def _(k):
                u = 4 * xs + k
                cols = jnp.concatenate([rt[2 * u].astype(F32), rt[2 * u + 1].astype(F32)], axis=0)
                at = pl.ds(pl.multiple_of(128 * u, 128), 128)
                blocks[0, :, at] = cols.T.astype(BF16)

        for j in range(PIECES):
            forward(0, 1, j, 1, 0)
            forward(0, 2, j, 0, 1)
        for dz in (1, 2, 3):
            for q in (0, 1):
                rows = pl.ds(pl.multiple_of(32 * (4 * q + level(dz)), 32), 32)
                send(blocks.at[0, rows, :], early_pieces.at[z], rows_send, rows_recv, 2 * chip + q, level(dz))
        rows = pl.ds(pl.multiple_of(32 * (4 * L_CORE + z), 32), 32)
        send(blocks.at[0, rows, :], early_pieces.at[z], pair_send.at[1], rows_recv, l_dev, z)
        early_pieces[z] = blocks[0, my_rows, :]

    def start(j):
        if j != DETOUR[1]:
            forward(0, 2, j, 0, 1)
        if j != DETOUR[0]:
            forward(0, 1, j, 1, 0)

    @pl.when(is_l)
    def _():
        send(cen.at[chip], rt.at[gx], pair_send.at[0], early_recv.at[x], k_dev, z)
        blocks[0, my_rows, :] = late[:, own_cols]
        for n, j in enumerate((0, 4, 1, 5, 2, 6, 3, 7)):
            if j:
                arrived(blocks.at[0, piece(j), :], late_recv.at[2 * ORDER[j][0] + ORDER[j][1]], f"w_late{j}")
            if n < 6:
                start(j)
        for c in range(4):
            at = slice(512 * c, 512 * (c + 1))
            part = jnp.zeros((32, 512), F32)
            for r in range(8):
                part = part + blocks[0, 32 * r : 32 * (r + 1), at].astype(F32)
            own_sum[:, at] = jnp.sum(part, axis=0, keepdims=True)
        plane_sums[chip] = own_sum[...]

        @pl.loop(1, 16)
        def _(r):
            other = lax.rem(chip + r, 16)
            send(own_sum, plane_sums.at[chip], sums_send, sums_recv, 2 * other + L_CORE, z)

        start(3)
        start(7)

    def center(slot, half=None):
        for c in range(4):
            at = slice(512 * c, 512 * (c + 1))
            m = mean_out[:, at]
            for r in range(8) if half is None else range(4 * half, 4 * half + 4):
                rows = slice(32 * r, 32 * (r + 1))
                blocks[6 + slot, rows, at] = (blocks[slot, rows, at].astype(F32) - m).astype(BF16)

    def late_mean():
        arrived(plane_sums.at[0:15], sums_recv, "w_sums")
        mean = plane_sums[0]
        for u in range(1, 16):
            mean = mean + plane_sums[u]
        mean_out[...] = mean / 4096.0
        means[z] = mean_out[...]
        send(mean_out, means.at[z], pair_send.at[1], mean_recv, k_dev, z)
        for dz in (1, 2, 3):
            send(mean_out, means.at[z], mean_send, mean_recv, k_dev, level(dz))
            send(mean_out, means.at[z], mean_send, mean_recv, l_dev, level(dz))
        center(0)
        product(0)

    dims = (((1,), (1,)), ((), ()))

    ready = 6 * (1 - core)

    def sides(t):
        a, b, half = TILES[t]
        if half in ("x", "y"):
            half = (x if half == "x" else y) // 2
            return a + half * (b - a), b + half * (a - b), half
        return a, b, half

    def product(t):
        a, b, half = sides(t)
        with jax.named_scope(f"dot{t}"):
            if t < WHOLE:
                gram[t] = lax.dot_general(blocks[a + ready], blocks[b + ready], dims, preferred_element_type=F32)
            else:
                top = pl.ds(pl.multiple_of(128 * half, 128), 128)
                gram[t, 0:128, :] = lax.dot_general(
                    blocks[a + ready, top, :], blocks[b + ready], dims, preferred_element_type=F32
                )
        if t == 0:
            src, dst, size, out, into, pair = gram.at[0], parts0, 64, part0_send, part0_recv, 2
        elif t < WHOLE:
            src, dst, size, out, into, pair = stage.at[t - 1], parts.at[t - 1], 64, part_send, part_recv.at[t - 1], 3
            stage[t - 1] = gram[t].astype(BF16)
        else:
            n = t - WHOLE
            src, dst, size, out, into, pair = halves.at[n], half_parts.at[n], 32, half_send, part_recv.at[t - 1], 4
            halves[n] = gram[t, 0:128, :].astype(BF16)
        for dz in (2, 1, 3):
            to = level(dz)
            rows = pl.ds(pl.multiple_of(size * to, size), size)
            send(src.at[rows, :], dst.at[dz - 1 + 4 * (1 - core)], out, into, k_dev, to)

        @pl.when(is_l)
        def _():
            rows = pl.ds(pl.multiple_of(size * z, size), size)
            send(src.at[rows, :], dst.at[3], pair_send.at[pair], into, k_dev, z)

    def settle(t):
        _, b, _ = sides(t)
        if t == 0:
            size, buf, sem = 64, parts0, part0_recv
        elif t < WHOLE:
            size, buf, sem = 64, parts.at[t - 1], part_recv.at[t - 1]
        else:
            size, buf, sem = 32, half_parts.at[t - WHOLE], part_recv.at[t - 1]
        arrived(buf, sem, f"wp{t}")
        part = [buf[n].astype(F32) for n in range(7)]
        rows = pl.ds(pl.multiple_of(size * z, size), size)
        k = gram[t, rows, :] + ((part[0] + part[1]) + part[2])
        l = (part[3] + part[4]) + (part[5] + part[6])
        h = k * l
        lane = lax.broadcasted_iota(jnp.int32, (size, 128), 1)
        own = jnp.where(lane == t, jnp.sum(h, axis=1, keepdims=True), 0.0)
        weight = 1.0
        if t:
            weight = 2.0
            across = jnp.sum(h, axis=0, keepdims=True)
            col_acc[...] += jnp.where(slot_row == b, across, 0.0)
        if t < WHOLE:
            row_cols[...] += own
        else:
            half_cols[...] += own
        acc[0, 0:size] += weight * (k * k)
        acc[1, 0:size] += weight * (l * l)
        acc[2, 0:size] += weight * h

    slot_row = lax.broadcasted_iota(jnp.int32, (8, 256), 0)

    @pl.when(is_k)
    def _():
        acc[...] = jnp.zeros_like(acc)
        row_cols[...] = jnp.zeros_like(row_cols)
        half_cols[...] = jnp.zeros_like(half_cols)
        col_acc[...] = jnp.zeros_like(col_acc)
        product(0)
        for j in range(PIECES):
            take(1, j)
            forward(1, 4, j, 0, 3)
            if j % 2 == 0:
                forward(1, 3, j, 0, 1)
            take(2, j)
            forward(2, 5, j, 3, 0)
            if j % 2:
                forward(2, 3, j, 1, 0)
            if j == 3:
                product(4)
                product(6)

    @pl.when(is_l)
    def _():
        def from_1(j):
            take(1, j)
            forward(1, 4, j, 0, 3)
            if j == DETOUR[1]:
                forward(1, 3, j, 0, 1)

        def from_2(j):
            take(2, j)
            forward(2, 5, j, 3, 0)
            if j == DETOUR[0]:
                forward(2, 3, j, 1, 0)

        for near, far in ((0, 0), (4, 4), (1, 1), (2, 5), (6, 2), (3, 3), (7, 7)):
            from_1(near)
            from_2(far)
        late_mean()
        take(3, DETOUR[0])
        forward(3, 1, DETOUR[0], 0, 3)
        take(3, DETOUR[1])
        forward(3, 2, DETOUR[1], 3, 0)
        center(1, 0)
        product(4)
        center(2, 0)
        product(6)
        for j in (0, 1, 2, 3, 4, 7):
            if j % 2:
                forward(1, 3, j, 0, 1)
            else:
                forward(2, 3, j, 1, 0)
        from_2(DETOUR[1])
        from_1(DETOUR[0])
        center(1, 1)
        center(2, 1)

    for t in (5, 7, 1):
        product(t)

    @pl.when(is_k)
    def _():
        arrived(means, mean_recv, "w_mean")
        arrived(early_pieces.at[0:3], rows_recv, "w_rows")

    @pl.when(is_l)
    def _():
        arrived(means.at[0:3], mean_recv, "w_mean")
        arrived(early_pieces, rows_recv, "w_rows")

    for c in range(4):
        at = slice(2048 * c, 2048 * (c + 1))
        late_out[:, at] = (late[:, at].astype(F32) - means[c]).astype(BF16)
    low = lax.broadcasted_iota(jnp.int32, (32, 128), 1) < 64
    for u in range(16):
        p = [early_pieces[c, :, 128 * u : 128 * (u + 1)].astype(F32) for c in range(4)]
        turned = [pltpu.roll(v, 64, 1) for v in p]
        for j in range(2):
            first = jnp.where(low, p[2 * j], turned[2 * j + 1])
            second = jnp.where(low, turned[2 * j], p[2 * j + 1])
            early_out[:, 128 * (4 * u + j) : 128 * (4 * u + j + 1)] = first.astype(BF16)
            early_out[:, 128 * (4 * u + 2 + j) : 128 * (4 * u + 3 + j)] = second.astype(BF16)
    put_e = pltpu.make_async_copy(early_out, eout_hbm, out_sem.at[0])
    put_l = pltpu.make_async_copy(late_out, lout_hbm, out_sem.at[1])
    put_e.start()
    put_l.start()

    for j in range(4):
        take(3, j)
    pl.when(is_l)(lambda: center(3, 0))
    product(8)
    for slot, t in ((4, 2), (5, 3)):
        for j in range(PIECES):
            take(slot, j)
        pl.when(is_l)(lambda: center(slot))
        product(t)
    product(10)
    for j in range(4, PIECES):
        if j in DETOUR:
            pl.when(is_k)(lambda: take(3, j))
        else:
            take(3, j)
    pl.when(is_l)(lambda: center(3, 1))
    for t in (9, 11, 12):
        product(t)

    @pl.when(is_k)
    def _():
        for t in (0, 4, 6, 5, 7, 1, 8, 2, 3):
            settle(t)
        turned = jnp.concatenate([row_cols[...]] * 2, axis=0).T
        turned = jnp.concatenate([turned] * 2, axis=1)
        for t in (10, 9, 11, 12):
            settle(t)
        half_turned = jnp.concatenate([half_cols[...]] * 4, axis=0).T
        half_turned = jnp.concatenate([half_turned] * 2, axis=1)
        col = lax.broadcasted_iota(jnp.int32, (1, 256), 1)
        both = col_acc[...]
        for t in range(len(TILES)):
            a, _, half = sides(t)
            if t < WHOLE:
                row = jnp.where(col // 64 == z, turned[t : t + 1, :], 0.0)
            else:
                row = jnp.where(col // 32 == 4 * half + z, half_turned[t : t + 1, :], 0.0)
            both = both + jnp.where(slot_row == a, row, 0.0)
        scal_lane = lax.broadcasted_iota(jnp.int32, (1, 128), 1)
        scal = jnp.zeros((1, 128), F32)
        for j in range(3):
            s = jnp.sum(jnp.sum(acc[j], axis=0, keepdims=True), axis=1, keepdims=True)
            scal = jnp.where(scal_lane == j, s, scal)
        for dx in range(4):
            for dy in range(4):
                r = 4 * dx + dy
                if (dx, dy) in SLOTS:
                    slot = SLOTS.index((dx, dy))
                    msg[r, :, 0:256] = both[slot : slot + 1, :]
                else:
                    msg[r, :, 0:256] = jnp.zeros((1, 256), F32)
                msg[r, :, 256:384] = scal
        for dx, dy, dz in EVERYONE:
            r = 4 * dx + dy
            there = msg_in.at[16 * dz + r]
            chip_there = 2 * chip_at(dx, dy)
            if dx or dy or dz:
                send(msg.at[r], there, msg_send.at[K_CORE], msg_recv, chip_there + K_CORE, level(dz))
            send(msg.at[r], there, msg_send.at[L_CORE], msg_recv, chip_there + L_CORE, level(dz))
        msg_in[0] = msg[0]
        arrived(msg_in.at[0:63], msg_recv, "w_msg")

    @pl.when(is_l)
    def _():
        arrived(msg_in, msg_recv, "w_msg")

    rows = [msg_in[r] for r in range(64)]
    while len(rows) > 1:
        rows = [a + b for a, b in zip(rows[0::2], rows[1::2])]
    final = rows[0]
    scal_lane = lax.broadcasted_iota(jnp.int32, (1, 128), 1)
    scal = final[:, 256:384]
    kk, ll, kl = (jnp.sum(jnp.where(scal_lane == j, scal, 0.0), axis=1, keepdims=True) for j in range(3))
    norm = jnp.sqrt(kk * ll)
    sim_ref[...] = kl / norm
    half = jnp.where(core == 0, final[:, 0:128], final[:, 128:256])
    tokens = half
    for j in (1, 2, 3):
        tokens = jnp.where(z == j, pltpu.roll(half, 128 - 32 * j, 1), tokens)
    share_ref[...] = (4096.0 * tokens / norm)[:, 0:32]

    with jax.named_scope("end"):
        put_e.wait()
    put_l.wait()
    left(late.at[:, 0:6144], late_send)
    left(cen.at[0:15], early_send)
    left(blocks.at[1:6], gather_send)
    left(parts.at[:, 0:3], part_send)
    left(half_parts.at[:, 0:3], half_send)
    left(parts0.at[0:3], part0_send)

    @pl.when(is_k)
    def _():
        left(late.at[:, 0:2048], pair_send.at[0])
        left(early_pieces.at[0], pair_send.at[1])
        left(blocks.at[0, 0:192, :], rows_send)
        left(msg_in.at[0:63], msg_send.at[K_CORE])
        left(msg_in, msg_send.at[L_CORE])

    @pl.when(is_l)
    def _():
        left(cen.at[0], pair_send.at[0])
        left(mean_out, pair_send.at[1])
        left(parts0.at[0], pair_send.at[2])
        left(parts.at[:, 0], pair_send.at[3])
        left(half_parts.at[:, 0], pair_send.at[4])
        left(plane_sums.at[0:15], sums_send)
        left(plane_sums.at[0:6], mean_send)


def publish(share_in, sim_in, early_in, late_in, share, sim, early, late, bufs, share_buf, sim_buf, in_sem, out_sem):
    ways = (
        (early_in, bufs.at[0], early),
        (late_in, bufs.at[1], late),
        (share_in, share_buf, share),
        (sim_in, sim_buf, sim),
    )
    gets = [pltpu.make_async_copy(a, b, in_sem.at[n]) for n, (a, b, _) in enumerate(ways)]
    puts = [pltpu.make_async_copy(b, c, out_sem.at[n]) for n, (_, b, c) in enumerate(ways)]
    for get in gets:
        get.start()
    for get, put in zip(gets, puts):
        get.wait()
        put.start()
    for put in puts:
        put.wait()


def body(layer_early, layer_late):
    vm = pltpu.VMEM
    dma = pltpu.SemaphoreType.DMA
    hbm = pl.BlockSpec(memory_space=pltpu.HBM)
    whole = pl.BlockSpec(memory_space=pltpu.VMEM)
    share, sim, early_rows, late_rows = pl.pallas_call(
        kernel,
        out_shape=(
            jax.ShapeDtypeStruct((1, 32), F32),
            jax.ShapeDtypeStruct((1, 1), F32),
            jax.ShapeDtypeStruct((32, 8192), BF16),
            jax.ShapeDtypeStruct((32, 8192), BF16),
        ),
        in_specs=[hbm, hbm],
        out_specs=(whole, whole, hbm, hbm),
        scratch_shapes=[
            vm((64, 4096), BF16),
            vm((32, 8192), BF16),
            vm((16, 64, 256), BF16),
            vm((32, 64, 256), BF16),
            vm((12, 256, 2048), BF16),
            vm((13, 256, 256), F32),
            vm((3, 256, 256), BF16),
            vm((3, 7, 64, 256), BF16),
            vm((9, 128, 256), BF16),
            vm((9, 7, 32, 256), BF16),
            vm((7, 64, 256), F32),
            vm((1, 2048), F32),
            vm((16, 1, 2048), F32),
            vm((1, 2048), F32),
            vm((4, 1, 2048), F32),
            vm((4, 32, 2048), BF16),
            vm((32, 8192), BF16),
            vm((32, 8192), BF16),
            vm((3, 64, 256), F32),
            vm((64, 128), F32),
            vm((32, 128), F32),
            vm((8, 256), F32),
            vm((16, 1, 384), F32),
            vm((64, 1, 384), F32),
            dma((2,)),
            dma((2,)),
            dma,
            dma((8,)),
            dma,
            dma((4,)),
            dma((5,)),
            dma,
            dma,
            dma,
            dma,
            dma,
            dma((5, PIECES)),
            dma,
            dma,
            dma,
            dma((12,)),
            dma,
            dma,
            dma,
            dma((2,)),
            dma,
        ],
        compiler_params=pltpu.CompilerParams(collective_id=0, has_side_effects=True, vmem_limit_bytes=67043328),
    )(layer_early.T, layer_late)
    share, sim, early_rows, late_rows = pl.pallas_call(
        publish,
        out_shape=(
            jax.ShapeDtypeStruct((1, 32), F32),
            jax.ShapeDtypeStruct((1, 1), F32),
            jax.ShapeDtypeStruct((32, 8192), BF16),
            jax.ShapeDtypeStruct((32, 8192), BF16),
        ),
        in_specs=[hbm] * 4,
        out_specs=(hbm,) * 4,
        scratch_shapes=[
            vm((2, 32, 8192), BF16),
            vm((1, 32), F32),
            vm((1, 1), F32),
            dma((4,)),
            dma((4,)),
        ],
    )(share, sim, early_rows, late_rows)
    return sim.reshape(()), share.reshape(32), early_rows, late_rows


def solution(mesh):
    return jax.shard_map(
        body,
        mesh=mesh,
        in_specs=(P(None, ("gx", "gy")), P(("gx", "gy"), None)),
        out_specs=(P(), P(("gx", "gy")), P(("gx", "gy"), None), P(("gx", "gy"), None)),
        check_vma=False,
    )
```
